8 devices in a mesh: model: 4 (over z, y, x), data: 2 (over core).
Axes of the slice: x: 2, y: 2, z: 1, core: 2. Of those that a mesh axis runs over, the one named last changes fastest.
Arguments:
- x_in: bfloat16 [4, 1024, 1536], P('data')
- cot_out: bfloat16 [4, 1024, 1536], P('data')
- step_emb: bfloat16 [4, 1536], replicated
- w_q: bfloat16 [1536, 1536], P(None, 'model')
- w_k: bfloat16 [1536, 1536], P(None, 'model')
- w_v: bfloat16 [1536, 1536], P(None, 'model')
- w_o: bfloat16 [1536, 1536], P('model')
- w_1: bfloat16 [1536, 6144], P(None, 'model')
- w_2: bfloat16 [6144, 1536], P('model')
Outputs:
- output 1: float32 [1536, 1536], P(None, 'model')
- output 2: float32 [1536, 1536], P(None, 'model')
- output 3: float32 [1536, 1536], P(None, 'model')
- output 4: float32 [1536, 1536], P('model')
- output 5: float32 [1536, 6144], P(None, 'model')
- output 6: float32 [6144, 1536], P('model')
- output 7: bfloat16 [4, 1024, 1536], P('data')
All inputs are finite; a program needn't handle non-finite values.
Results may differ from the reference program's by a relative error of at most 0.0181743.
Values are sent between devices in bfloat16 or wider.
A program may use at most 1 GiB of HBM per device.

```python
import jax
import jax.numpy as jnp
from jax import lax

BATCH = 4
SEQ = 1024
D = 1536
HEADS = 24
FF = 6144
LAYERS = 4


def normal_weight(key, rows, cols):
    return (jax.random.normal(key, (rows, cols), jnp.float32) * rows ** -0.5).astype(jnp.bfloat16)


def setup_inputs(seed: int = 0) -> dict:
    key_list = jax.random.split(jax.random.key(seed), 9)
    x_in = jax.random.normal(key_list[0], (BATCH, SEQ, D), jnp.float32).astype(jnp.bfloat16)
    cot_out = jax.random.normal(key_list[1], (BATCH, SEQ, D), jnp.float32).astype(jnp.bfloat16)
    step_emb = (0.5 * jax.random.normal(key_list[2], (LAYERS, D), jnp.float32)).astype(jnp.bfloat16)
    return dict(x_in=x_in, cot_out=cot_out, step_emb=step_emb,
                w_q=normal_weight(key_list[3], D, D), w_k=normal_weight(key_list[4], D, D),
                w_v=normal_weight(key_list[5], D, D), w_o=normal_weight(key_list[6], D, D),
                w_1=normal_weight(key_list[7], D, FF), w_2=normal_weight(key_list[8], FF, D))


def rms_norm(values):
    return values * lax.rsqrt(jnp.mean(values * values, axis=-1, keepdims=True) + 1e-6)


def attend_one(qkv_seq):
    q_seq, k_seq, v_seq = qkv_seq
    head_dim = q_seq.shape[-1]
    scores = jnp.einsum('qhe,khe->hqk', q_seq, k_seq) * (head_dim ** -0.5)
    prob_mat = jax.nn.softmax(scores, axis=-1).astype(jnp.bfloat16).astype(jnp.float32)
    return jnp.einsum('hqk,khe->qhe', prob_mat, v_seq).astype(jnp.bfloat16)


def shared_block(x_cur, step_vec, weights32):
    w_q, w_k, w_v, w_o, w_1, w_2 = weights32
    batch_size, seq_len, width_model = x_cur.shape
    head_shape = (batch_size, seq_len, HEADS, width_model // HEADS)
    x_f = x_cur.astype(jnp.float32) + step_vec.astype(jnp.float32)
    u_f = rms_norm(x_f).astype(jnp.bfloat16).astype(jnp.float32)
    q_all = jnp.einsum('bsd,de->bse', u_f, w_q).astype(jnp.bfloat16).astype(jnp.float32).reshape(head_shape)
    k_all = jnp.einsum('bsd,de->bse', u_f, w_k).astype(jnp.bfloat16).astype(jnp.float32).reshape(head_shape)
    v_all = jnp.einsum('bsd,de->bse', u_f, w_v).astype(jnp.bfloat16).astype(jnp.float32).reshape(head_shape)
    context = lax.map(jax.checkpoint(attend_one), (q_all, k_all, v_all))
    context_f = context.reshape(batch_size, seq_len, width_model).astype(jnp.float32)
    h_f = (x_f + jnp.einsum('bse,ed->bsd', context_f, w_o)).astype(jnp.bfloat16).astype(jnp.float32)
    m_f = rms_norm(h_f).astype(jnp.bfloat16).astype(jnp.float32)
    z_b = jnp.einsum('bsd,df->bsf', m_f, w_1).astype(jnp.bfloat16)
    g_f = jax.nn.gelu(z_b.astype(jnp.float32)).astype(jnp.bfloat16).astype(jnp.float32)
    return (h_f + jnp.einsum('bsf,fd->bsd', g_f, w_2)).astype(jnp.bfloat16)


def reference(x_in, cot_out, step_emb, w_q, w_k, w_v, w_o, w_1, w_2):
    weights32 = tuple(weight.astype(jnp.float32) for weight in (w_q, w_k, w_v, w_o, w_1, w_2))

    def forward(x_start, weight_set):
        def scan_body(x_cur, step_vec):
            return jax.checkpoint(shared_block)(x_cur, step_vec, weight_set), None
        x_last, _ = lax.scan(scan_body, x_start, step_emb)
        return x_last

    _, pull_back = jax.vjp(forward, x_in, weights32)
    d_x, d_w = pull_back(cot_out)
    return (d_w[0], d_w[1], d_w[2], d_w[3], d_w[4], d_w[5], d_x)
```

```python
import functools

import jax
import jax.numpy as jnp
from jax import lax
from jax.experimental import pallas as pl
from jax.experimental.pallas import tpu as pltpu
from jax.sharding import PartitionSpec as P

HEAD_DIM = 64
EPS_NORM = 1e-6
F32 = jnp.float32
BF16 = jnp.bfloat16
LOG2E = 1.4426950408889634
SCALE = HEAD_DIM ** -0.5

SWAP_D = [(0, 1), (1, 0)]
SWAP_X = [(0, 1), (1, 0), (2, 3), (3, 2)]
SWAP_Y = [(0, 2), (2, 0), (1, 3), (3, 1)]


def pp_d(v):
    return lax.ppermute(v, 'data', SWAP_D)


def pp_x(v):
    return lax.ppermute(v, 'model', SWAP_X)


def pp_y(v):
    return lax.ppermute(v, 'model', SWAP_Y)


def rms_norm(values):
    return values * lax.rsqrt(jnp.mean(values * values, axis=-1, keepdims=True) + EPS_NORM)


def dot(a, b, dims):
    return lax.dot_general(a, b, (dims, ((), ())), preferred_element_type=F32)


def nn(a, b):
    return dot(a, b, ((1,), (0,)))


def nt(a, b):
    return dot(a, b, ((1,), (1,)))


def tn(a, b):
    return dot(a, b, ((0,), (0,)))


def pair_masks(rows):
    lane = lax.broadcasted_iota(jnp.int32, (rows, 128), 1)
    return lane < HEAD_DIM


def attn_fwd_body(q_ref, ko_ref, ks_ref, vo_ref, vs_ref, ctx_ref, lse_ref):
    k = jnp.concatenate([ko_ref[...], ks_ref[...]], axis=0)
    v = jnp.concatenate([vo_ref[...], vs_ref[...]], axis=0)
    tq = q_ref.shape[0]
    chunk = 256
    low = pair_masks(chunk)
    scores = []
    for i in range(tq // chunk):
        q = q_ref[i * chunk:(i + 1) * chunk, :]
        zero = jnp.zeros_like(q)
        both = jnp.concatenate([jnp.where(low, q, zero), jnp.where(low, zero, q)], axis=0)
        scores.append(nt(k, both))
    for i, s in enumerate(scores):
        rows = slice(i * chunk, (i + 1) * chunk)
        m = jnp.max(s, axis=0, keepdims=True)
        p = jnp.exp2((s - m) * (SCALE * LOG2E))
        l = jnp.sum(p, axis=0, keepdims=True)
        pb = (p * (1.0 / l)).astype(BF16)
        lse = m * (SCALE * LOG2E) + jnp.log2(l)
        lse_ref[0, 0:1, rows] = lse[:, :chunk]
        lse_ref[0, 1:2, rows] = lse[:, chunk:]
        ctx_t = tn(v, pb)
        ctx_t = jnp.concatenate([ctx_t[:HEAD_DIM, :chunk], ctx_t[HEAD_DIM:, chunk:]], axis=0)
        ctx_ref[rows, :] = ctx_t.T.astype(BF16)


def attn_fwd(q, kv, kv_s):
    tq, width = q.shape
    tk = kv.shape[0]
    pairs = width // 128
    def col(off):
        return lambda j: (0, j + off)
    flops = 2 * 2 * tq * (2 * tk) * 256 * (width // HEAD_DIM)
    return pl.pallas_call(
        attn_fwd_body,
        grid=(pairs,),
        in_specs=[pl.BlockSpec((tq, 128), col(0)),
                  pl.BlockSpec((tk, 128), col(0)), pl.BlockSpec((tk, 128), col(0)),
                  pl.BlockSpec((tk, 128), col(pairs)), pl.BlockSpec((tk, 128), col(pairs))],
        out_specs=[pl.BlockSpec((tq, 128), col(0)),
                   pl.BlockSpec((1, 2, tq), lambda j: (j, 0, 0))],
        out_shape=[jax.ShapeDtypeStruct((tq, width), BF16),
                   jax.ShapeDtypeStruct((pairs, 2, tq), F32)],
        compiler_params=pltpu.CompilerParams(dimension_semantics=('arbitrary',),
                                             vmem_limit_bytes=48 * 1024 * 1024),
        cost_estimate=pl.CostEstimate(flops=flops, bytes_accessed=2 * (tq * width * 2 + 4 * tk * width),
                                      transcendentals=tq * 2 * tk * (width // HEAD_DIM)),
        name='attn_fwd',
    )(q, kv, kv_s, kv, kv_s)


def attn_bwd_body(q_ref, ko_ref, ks_ref, vo_ref, vs_ref, do_ref, lse_ref,
                  dq_ref, dko_ref, dks_ref, dvo_ref, dvs_ref):
    tk = ko_ref.shape[0]
    k = jnp.concatenate([ko_ref[...], ks_ref[...]], axis=0)
    v = jnp.concatenate([vo_ref[...], vs_ref[...]], axis=0)
    tq = q_ref.shape[0]
    chunk = 256
    low = pair_masks(chunk)
    for ref in (dko_ref, dks_ref, dvo_ref, dvs_ref):
        ref[...] = jnp.zeros_like(ref)

    def step(i, carry):
        rows = pl.ds(pl.multiple_of(i * chunk, chunk), chunk)
        q = q_ref[rows, :]
        do = do_ref[rows, :]
        lse = lse_ref[0, :, rows]
        dqs = []
        for h in range(2):
            sel = low if h == 0 else ~low
            qm = jnp.where(sel, q, jnp.zeros_like(q))
            dom = jnp.where(sel, do, jnp.zeros_like(do))
            s = nt(k, qm)
            p = jnp.exp2(s * (SCALE * LOG2E) - lse[h:h + 1, :])
            dp = nt(v, dom).astype(BF16).astype(F32)
            delta = jnp.sum(p * dp, axis=0, keepdims=True)
            ds = (p * (dp - delta)).astype(BF16)
            dv = nn(p.astype(BF16), dom)
            dk = nn(ds, qm) * SCALE
            dvo_ref[...] += dv[:tk]
            dvs_ref[...] += dv[tk:]
            dko_ref[...] += dk[:tk]
            dks_ref[...] += dk[tk:]
            dqs.append(tn(k, ds)[h * HEAD_DIM:(h + 1) * HEAD_DIM, :] * SCALE)
        dq_ref[rows, :] = jnp.concatenate(dqs, axis=0).T.astype(BF16)
        return carry

    lax.fori_loop(0, tq // chunk, step, 0)


def attn_bwd(q, kv, kv_s, d_ctx, lse):
    tq, width = q.shape
    tk = kv.shape[0]
    pairs = width // 128
    def col(off):
        return lambda j: (0, j + off)
    flops = 5 * 2 * tq * (2 * tk) * 256 * (width // HEAD_DIM)
    kblk = pl.BlockSpec((tk, 128), col(0))
    return pl.pallas_call(
        attn_bwd_body,
        grid=(pairs,),
        in_specs=[pl.BlockSpec((tq, 128), col(0)),
                  kblk, kblk,
                  pl.BlockSpec((tk, 128), col(pairs)), pl.BlockSpec((tk, 128), col(pairs)),
                  pl.BlockSpec((tq, 128), col(0)),
                  pl.BlockSpec((1, 2, tq), lambda j: (j, 0, 0))],
        out_specs=[pl.BlockSpec((tq, 128), col(0)), kblk, kblk, kblk, kblk],
        out_shape=[jax.ShapeDtypeStruct((tq, width), BF16)]
        + [jax.ShapeDtypeStruct((tk, width), F32)] * 4,
        compiler_params=pltpu.CompilerParams(dimension_semantics=('arbitrary',),
                                             vmem_limit_bytes=48 * 1024 * 1024),
        cost_estimate=pl.CostEstimate(flops=flops, bytes_accessed=2 * (2 * tq * width * 2 + 4 * tk * width) + 16 * tk * width,
                                      transcendentals=tq * 2 * tk * (width // HEAD_DIM)),
        name='attn_bwd',
    )(q, kv, kv_s, kv, kv_s, d_ctx, lse)


def gather_pieces(part_a, part_b):
    xa, xb = pp_x(part_a), pp_x(part_b)
    ya, yb = pp_y(part_a), pp_y(part_b)
    da, db = pp_y(xa), pp_x(yb)
    own = [(part_a, part_b), (xa, xb), (ya, yb), (da, db)]
    sib = [None] + [(pp_d(a), pp_d(b)) for a, b in own[1:]]
    return own, sib


def reduce_pieces(piece):
    total = {}
    for r in (3, 1, 2, 0):
        for part in (0, 1):
            total[r, part] = piece(r, 0, part) + pp_d(piece(r, 1, part))
    a0 = total[0, 0] + pp_x(total[1, 0])
    a2 = total[2, 0] + pp_x(total[3, 0])
    b0 = total[0, 1] + pp_y(total[2, 1])
    b1 = total[1, 1] + pp_y(total[3, 1])
    own = (a0 + pp_y(a2), b0 + pp_x(b1))
    return own, (pp_d(own[0]), pp_d(own[1]))


def solution(mesh):
    spec_col = P(None, 'model')
    spec_row = P('model', None)
    spec_act = P('data', None, None)
    spec_rep = P(None, None)

    def device_step(x_in, cot_out, step_emb, w_q, w_k, w_v, w_o, w_1, w_2):
        layer_count, dim = step_emb.shape
        core = lax.axis_index('data')
        chip = lax.axis_index('model')
        chip_x = lax.rem(chip, 2)
        chip_y = lax.div(chip, 2)
        half_d = dim // 2
        seq = x_in.shape[1]
        half_t = seq // 2

        def ordered(own, sib, axis):
            size = own.shape[axis]
            shape = own.shape[:axis] + (2 * size,) + own.shape[axis + 1:]
            out = lax.dynamic_update_slice_in_dim(jnp.zeros(shape, own.dtype), own, core * size, axis)
            return lax.dynamic_update_slice_in_dim(out, sib, (1 - core) * size, axis)

        def take(v, which, axis, parts=2):
            size = v.shape[axis] // parts
            return lax.dynamic_slice_in_dim(v, which * size, size, axis)

        def my_tokens(v):
            mine = lax.dynamic_index_in_dim(v, chip_x, 0, keepdims=False)
            recv = pp_d(take(mine, 1 - core, 0))
            return jnp.where(core == chip_y, take(mine, core, 0), recv)

        x_cur = my_tokens(x_in)
        d_cur = my_tokens(cot_out)

        w_qkv = jnp.concatenate([w_q, w_k, w_v], axis=1)
        hid = w_q.shape[1]
        own_qkv = take(w_qkv, core, 0)
        quart = half_d // 2
        qkv_own, qkv_sib = gather_pieces(own_qkv[:quart], own_qkv[quart:])
        wqkv = [w_qkv] + [ordered(jnp.concatenate(qkv_own[r], 0), jnp.concatenate(qkv_sib[r], 0), 0) for r in (1, 2, 3)]
        wq = jnp.concatenate([w[:, :hid] for w in wqkv], axis=1)
        wkv = jnp.concatenate([w[:, hid:2 * hid] for w in wqkv] + [w[:, 2 * hid:] for w in wqkv], axis=1)
        own_o = take(w_o, core, 1)
        o_own, o_sib = gather_pieces(own_o[:, :quart], own_o[:, quart:])
        wo = jnp.concatenate([w_o] + [ordered(jnp.concatenate(o_own[r], 1), jnp.concatenate(o_sib[r], 1), 1) for r in (1, 2, 3)], axis=0)

        own_1, sib_1 = take(w_1, core, 1), take(w_1, 1 - core, 1)
        p1_own, p1_sib = gather_pieces(own_1[:half_d], own_1[half_d:])
        w1_list = [own_1, sib_1]
        for r in (1, 2, 3):
            w1_list += [jnp.concatenate(p1_own[r], 0), jnp.concatenate(p1_sib[r], 0)]
        w1 = jnp.concatenate(w1_list, axis=1)
        own_2, sib_2 = take(w_2, core, 0), take(w_2, 1 - core, 0)
        p2_own, p2_sib = gather_pieces(own_2[:, :half_d], own_2[:, half_d:])
        w2_list = [own_2, sib_2]
        for r in (1, 2, 3):
            w2_list += [jnp.concatenate(p2_own[r], 1), jnp.concatenate(p2_sib[r], 1)]
        w2 = jnp.concatenate(w2_list, axis=0)

        saved = []
        for layer in range(layer_count):
            s = x_cur.astype(F32) + step_emb[layer].astype(F32)
            u = rms_norm(s).astype(BF16)
            kv = nn(u, wkv).astype(BF16)
            kv_s = pp_d(kv)
            q = nn(u, wq).astype(BF16)
            ctx, lse = attn_fwd(q, kv, kv_s)
            h = (s + nn(ctx, wo)).astype(BF16)
            m = rms_norm(h.astype(F32)).astype(BF16)
            z = nn(m, w1).astype(BF16)
            g = jax.nn.gelu(z.astype(F32)).astype(BF16)
            x_next = (h.astype(F32) + nn(g, w2)).astype(BF16)
            saved.append((x_cur, u, q, kv, kv_s, ctx, lse, h, m, z, g))
            x_cur = x_next

        hist = []
        for layer in reversed(range(layer_count)):
            x_l, u, q, kv, kv_s, ctx, lse, h, m, z, g = saved[layer]
            d_next = d_cur
            d_act = nt(d_next, w2).astype(BF16)
            gelu_pull = jax.vjp(jax.nn.gelu, z.astype(F32))[1]
            d_up = gelu_pull(d_act.astype(F32))[0].astype(BF16)
            d_norm2 = nt(d_up, w1).astype(BF16)
            norm_pull = jax.vjp(rms_norm, h.astype(F32))[1]
            d_mid = (d_next.astype(F32) + norm_pull(d_norm2.astype(F32))[0]).astype(BF16)
            d_ctx = nt(d_mid, wo).astype(BF16)
            dq, dko, dks, dvo, dvs = attn_bwd(q, kv, kv_s, d_ctx, lse)
            dk = (dko + pp_d(dks)).astype(BF16)
            dv = (dvo + pp_d(dvs)).astype(BF16)
            dkv = jnp.concatenate([dk, dv], axis=1)
            d_norm1 = (nt(dq, wq) + nt(dkv, wkv)).astype(BF16)
            s = x_l.astype(F32) + step_emb[layer].astype(F32)
            norm_pull_x = jax.vjp(rms_norm, s)[1]
            d_cur = (d_mid.astype(F32) + norm_pull_x(d_norm1.astype(F32))[0]).astype(BF16)
            hist.append((u, dq, dkv, ctx, d_mid, m, d_up, g, d_next))

        u_h, dq_h, dkv_h, ctx_h, mid_h, m_h, up_h, g_h, next_h = [jnp.concatenate(v, axis=0) for v in zip(*hist)]
        ff = w_1.shape[1] // 2

        def piece_2(r, half, part):
            col = (2 * r + half) * ff
            return tn(g_h[:, col:col + ff], next_h[:, part * half_d:(part + 1) * half_d])

        def piece_1(r, half, part):
            col = (2 * r + half) * ff
            return tn(m_h[:, part * half_d:(part + 1) * half_d], up_h[:, col:col + ff])

        mid_half = tuple(lax.optimization_barrier(take(mid_h, w, 1)) for w in (core, 1 - core))
        u_half = tuple(lax.optimization_barrier(take(u_h, w, 1)) for w in (core, 1 - core))

        def piece_o(r, half, part):
            return tn(ctx_h[:, r * hid:(r + 1) * hid], mid_half[half][:, part * quart:(part + 1) * quart])

        dqkv_r = [lax.optimization_barrier(jnp.concatenate([dq_h[:, r * hid:(r + 1) * hid], dkv_h[:, r * hid:(r + 1) * hid],
                                   dkv_h[:, (4 + r) * hid:(5 + r) * hid]], axis=1)) for r in range(4)]

        def piece_qkv(r, half, part):
            return tn(u_half[half][:, part * quart:(part + 1) * quart], dqkv_r[r])

        own, sib = reduce_pieces(piece_2)
        grad_2 = ordered(jnp.concatenate(own, 1), jnp.concatenate(sib, 1), 0)
        own, sib = reduce_pieces(piece_1)
        grad_1 = ordered(jnp.concatenate(own, 0), jnp.concatenate(sib, 0), 1)
        own, sib = reduce_pieces(piece_o)
        grad_o = ordered(jnp.concatenate(own, 1), jnp.concatenate(sib, 1), 1)
        own, sib = reduce_pieces(piece_qkv)
        grad_qkv = ordered(jnp.concatenate(own, 0), jnp.concatenate(sib, 0), 0)

        whole = ordered(d_cur, pp_d(d_cur), 0)
        to_row = [(2 * c + d, 2 * (c ^ 2) + d) for c in range(4) for d in range(2) if c // 2 == d]
        from_y = lax.ppermute(whole, ('model', 'data'), to_row)
        row_seq = jnp.where(chip_y == core, whole, from_y)
        other = pp_x(row_seq)
        d_x = jnp.where(chip_x == 0, jnp.stack([row_seq, other]), jnp.stack([other, row_seq]))
        return (grad_qkv[:, :hid], grad_qkv[:, hid:2 * hid], grad_qkv[:, 2 * hid:], grad_o, grad_1, grad_2, d_x)

    return jax.shard_map(device_step, mesh=mesh,
                         in_specs=(spec_act, spec_act, spec_rep, spec_col, spec_col, spec_col, spec_row, spec_col, spec_row),
                         out_specs=(spec_col, spec_col, spec_col, spec_row, spec_col, spec_row, spec_act),
                         check_vma=False)
```

```python
import jax
import jax.numpy as jnp
from jax import lax
from jax.experimental import pallas as pl
from jax.experimental.pallas import tpu as pltpu
from jax.sharding import PartitionSpec as P


HEAD_DIM = 64
EPS_NORM = 1e-6
F32 = jnp.float32
BF16 = jnp.bfloat16
LOG2E = 1.4426950408889634
SCALE = HEAD_DIM ** -0.5

SWAP_D = [(0, 1), (1, 0)]


def pp_d(v):
    return lax.ppermute(v, 'data', SWAP_D)


def rms_norm(values):
    return values * lax.rsqrt(jnp.mean(values * values, axis=-1, keepdims=True) + EPS_NORM)


def dot(a, b, dims):
    return lax.dot_general(a, b, (dims, ((), ())), preferred_element_type=F32)


def nn(a, b):
    return dot(a, b, ((1,), (0,)))


def nt(a, b):
    return dot(a, b, ((1,), (1,)))


def tn(a, b):
    return dot(a, b, ((0,), (0,)))


def pair_masks(rows):
    lane = lax.broadcasted_iota(jnp.int32, (rows, 128), 1)
    return lane < HEAD_DIM


def attn_fwd_body(q_ref, ko_ref, ks_ref, vo_ref, vs_ref, ctx_ref, lse_ref):
    k = jnp.concatenate([ko_ref[...], ks_ref[...]], axis=0)
    v = jnp.concatenate([vo_ref[...], vs_ref[...]], axis=0)
    tq = q_ref.shape[0]
    chunk = 256
    low = pair_masks(chunk)
    scores = []
    for i in range(tq // chunk):
        q = q_ref[i * chunk:(i + 1) * chunk, :]
        zero = jnp.zeros_like(q)
        both = jnp.concatenate([jnp.where(low, q, zero), jnp.where(low, zero, q)], axis=0)
        scores.append(nt(k, both))
    for i, s in enumerate(scores):
        rows = slice(i * chunk, (i + 1) * chunk)
        m = jnp.max(s, axis=0, keepdims=True)
        p = jnp.exp2((s - m) * (SCALE * LOG2E))
        l = jnp.sum(p, axis=0, keepdims=True)
        pb = (p * (1.0 / l)).astype(BF16)
        lse = m * (SCALE * LOG2E) + jnp.log2(l)
        lse_ref[0, 0:1, rows] = lse[:, :chunk]
        lse_ref[0, 1:2, rows] = lse[:, chunk:]
        ctx_t = tn(v, pb)
        ctx_t = jnp.concatenate([ctx_t[:HEAD_DIM, :chunk], ctx_t[HEAD_DIM:, chunk:]], axis=0)
        ctx_ref[rows, :] = ctx_t.T.astype(BF16)


def attn_fwd(q, kv, kv_s):
    tq, width = q.shape
    tk = kv.shape[0]
    pairs = width // 128

    def col(off):
        return lambda j: (0, j + off)

    flops = 2 * 2 * tq * (2 * tk) * 256 * (width // HEAD_DIM)
    return pl.pallas_call(
        attn_fwd_body,
        grid=(pairs,),
        in_specs=[pl.BlockSpec((tq, 128), col(0)),
                  pl.BlockSpec((tk, 128), col(0)), pl.BlockSpec((tk, 128), col(0)),
                  pl.BlockSpec((tk, 128), col(pairs)), pl.BlockSpec((tk, 128), col(pairs))],
        out_specs=[pl.BlockSpec((tq, 128), col(0)),
                   pl.BlockSpec((1, 2, tq), lambda j: (j, 0, 0))],
        out_shape=[jax.ShapeDtypeStruct((tq, width), BF16),
                   jax.ShapeDtypeStruct((pairs, 2, tq), F32)],
        compiler_params=pltpu.CompilerParams(dimension_semantics=('arbitrary',),
                                             vmem_limit_bytes=48 * 1024 * 1024),
        cost_estimate=pl.CostEstimate(flops=flops, bytes_accessed=2 * (tq * width * 2 + 4 * tk * width),
                                      transcendentals=tq * 2 * tk * (width // HEAD_DIM)),
        name='attn_fwd',
    )(q, kv, kv_s, kv, kv_s)


def attn_bwd_body(q_ref, ko_ref, ks_ref, vo_ref, vs_ref, do_ref, lse_ref,
                  dq_ref, dko_ref, dks_ref, dvo_ref, dvs_ref):
    tk = ko_ref.shape[0]
    k = jnp.concatenate([ko_ref[...], ks_ref[...]], axis=0)
    v = jnp.concatenate([vo_ref[...], vs_ref[...]], axis=0)
    tq = q_ref.shape[0]
    chunk = 256
    low = pair_masks(chunk)
    for ref in (dko_ref, dks_ref, dvo_ref, dvs_ref):
        ref[...] = jnp.zeros_like(ref)

    def step(i, carry):
        rows = pl.ds(pl.multiple_of(i * chunk, chunk), chunk)
        q = q_ref[rows, :]
        do = do_ref[rows, :]
        lse = lse_ref[0, :, rows]
        dqs = []
        for h in range(2):
            sel = low if h == 0 else ~low
            qm = jnp.where(sel, q, jnp.zeros_like(q))
            dom = jnp.where(sel, do, jnp.zeros_like(do))
            s = nt(k, qm)
            p = jnp.exp2(s * (SCALE * LOG2E) - lse[h:h + 1, :])
            dp = nt(v, dom).astype(BF16).astype(F32)
            delta = jnp.sum(p * dp, axis=0, keepdims=True)
            ds = (p * (dp - delta)).astype(BF16)
            dv = nn(p.astype(BF16), dom)
            dk = nn(ds, qm) * SCALE
            dvo_ref[...] += dv[:tk]
            dvs_ref[...] += dv[tk:]
            dko_ref[...] += dk[:tk]
            dks_ref[...] += dk[tk:]
            dqs.append(tn(k, ds)[h * HEAD_DIM:(h + 1) * HEAD_DIM, :] * SCALE)
        dq_ref[rows, :] = jnp.concatenate(dqs, axis=0).T.astype(BF16)
        return carry

    lax.fori_loop(0, tq // chunk, step, 0)


def attn_bwd(q, kv, kv_s, d_ctx, lse):
    tq, width = q.shape
    tk = kv.shape[0]
    pairs = width // 128

    def col(off):
        return lambda j: (0, j + off)

    flops = 5 * 2 * tq * (2 * tk) * 256 * (width // HEAD_DIM)
    kblk = pl.BlockSpec((tk, 128), col(0))
    return pl.pallas_call(
        attn_bwd_body,
        grid=(pairs,),
        in_specs=[pl.BlockSpec((tq, 128), col(0)),
                  kblk, kblk,
                  pl.BlockSpec((tk, 128), col(pairs)), pl.BlockSpec((tk, 128), col(pairs)),
                  pl.BlockSpec((tq, 128), col(0)),
                  pl.BlockSpec((1, 2, tq), lambda j: (j, 0, 0))],
        out_specs=[pl.BlockSpec((tq, 128), col(0)), kblk, kblk, kblk, kblk],
        out_shape=[jax.ShapeDtypeStruct((tq, width), BF16)]
        + [jax.ShapeDtypeStruct((tk, width), F32)] * 4,
        compiler_params=pltpu.CompilerParams(dimension_semantics=('arbitrary',),
                                             vmem_limit_bytes=48 * 1024 * 1024),
        cost_estimate=pl.CostEstimate(flops=flops, bytes_accessed=2 * (2 * tq * width * 2 + 4 * tk * width) + 16 * tk * width,
                                      transcendentals=tq * 2 * tk * (width // HEAD_DIM)),
        name='attn_bwd',
    )(q, kv, kv_s, kv, kv_s, d_ctx, lse)


GELU_C = 0.7978845608028654
GELU_A = 0.044715
BLOCK_F = 1024
SUB_F = 512
ROWS = (slice(0, 256), slice(256, 512))


def mlp_fwd_body(*refs):
    m_ref, h_ref, w1_ref, w2_ref = refs[:4]
    z_ref, g_ref, x_ref, acc_ref = refs[-4:]
    j = pl.program_id(0)

    @pl.when(j == 0)
    def _():
        acc_ref[...] = h_ref[...].astype(F32)

    for i in range(0, BLOCK_F, SUB_F):
        cols = slice(i, i + SUB_F)
        for rows in ROWS:
            z = nt(m_ref[rows, :], w1_ref[cols, :]).astype(BF16)
            z_ref[rows, cols] = z
            zf = z.astype(F32)
            t = jnp.tanh(zf * (GELU_C + (GELU_A * GELU_C) * (zf * zf)))
            half = 0.5 * zf
            g_ref[0, rows, cols] = (half + half * t).astype(BF16)
    for rows in ROWS:
        acc_ref[rows, :] += nn(g_ref[0, rows, :], w2_ref[...])

    @pl.when(j == pl.num_programs(0) - 1)
    def _():
        x_ref[...] = acc_ref[...].astype(BF16)


def mlp_fwd(m, h, w1t, w2, layer, layers, hist):
    t, dim = m.shape
    hidden = w2.shape[0]
    whole = pl.BlockSpec((t, dim), lambda j: (0, 0))
    wblk = pl.BlockSpec((BLOCK_F, dim), lambda j: (j, 0))
    hspec = pl.BlockSpec((1, t, BLOCK_F), lambda j: (layer, 0, j))
    extra = [] if hist is None else [hist]
    return pl.pallas_call(
        mlp_fwd_body,
        grid=(hidden // BLOCK_F,),
        in_specs=[whole, whole, wblk, wblk] + [pl.BlockSpec(memory_space=pl.ANY)] * len(extra),
        out_specs=[pl.BlockSpec((t, BLOCK_F), lambda j: (0, j)), hspec, whole],
        out_shape=[jax.ShapeDtypeStruct((t, hidden), BF16),
                   jax.ShapeDtypeStruct((layers, t, hidden), BF16),
                   jax.ShapeDtypeStruct((t, dim), BF16)],
        scratch_shapes=[pltpu.VMEM((t, dim), F32)],
        input_output_aliases={4: 1} if extra else {},
        compiler_params=pltpu.CompilerParams(dimension_semantics=('arbitrary',), vmem_limit_bytes=48 * 1024 * 1024),
        cost_estimate=pl.CostEstimate(flops=4 * t * dim * hidden, bytes_accessed=4 * dim * hidden + 4 * t * hidden,
                                      transcendentals=t * hidden),
        name='mlp_fwd',
    )(m, h, w1t, w2, *extra)


def mlp_bwd_body(*refs):
    d_ref, h_ref, z_ref, w1_ref, w2_ref = refs[:5]
    up_ref, mid_ref, acc_ref = refs[-3:]
    j = pl.program_id(0)

    @pl.when(j == 0)
    def _():
        acc_ref[...] = jnp.zeros_like(acc_ref)

    for i in range(0, BLOCK_F, SUB_F):
        cols = slice(i, i + SUB_F)
        for rows in ROWS:
            da = nt(d_ref[rows, :], w2_ref[cols, :]).astype(BF16).astype(F32)
            zf = z_ref[rows, cols].astype(F32)
            z2 = zf * zf
            t = jnp.tanh(zf * (GELU_C + (GELU_A * GELU_C) * z2))
            slope = (1.0 + t) * (0.5 + (1.0 - t) * (zf * (0.5 * GELU_C + (1.5 * GELU_A * GELU_C) * z2)))
            up_ref[0, rows, cols] = (da * slope).astype(BF16)
    for rows in ROWS:
        acc_ref[rows, :] += nn(up_ref[0, rows, :], w1_ref[...])

    @pl.when(j == pl.num_programs(0) - 1)
    def _():
        dn = acc_ref[...].astype(BF16).astype(F32)
        hf = h_ref[...].astype(F32)
        inv = lax.rsqrt(jnp.mean(hf * hf, axis=-1, keepdims=True) + EPS_NORM)
        proj = jnp.mean(hf * dn, axis=-1, keepdims=True)
        mid_ref[...] = (d_ref[...].astype(F32) + inv * dn - hf * (inv * inv * inv * proj)).astype(BF16)


def mlp_bwd(d_next, h, z, w1t, w2, layer, layers, hist):
    t, dim = h.shape
    hidden = w2.shape[0]
    whole = pl.BlockSpec((t, dim), lambda j: (0, 0))
    wblk = pl.BlockSpec((BLOCK_F, dim), lambda j: (j, 0))
    hspec = pl.BlockSpec((1, t, BLOCK_F), lambda j: (layer, 0, j))
    extra = [] if hist is None else [hist]
    return pl.pallas_call(
        mlp_bwd_body,
        grid=(hidden // BLOCK_F,),
        in_specs=[whole, whole, pl.BlockSpec((t, BLOCK_F), lambda j: (0, j)), wblk, wblk]
        + [pl.BlockSpec(memory_space=pl.ANY)] * len(extra),
        out_specs=[hspec, whole],
        out_shape=[jax.ShapeDtypeStruct((layers, t, hidden), BF16), jax.ShapeDtypeStruct((t, dim), BF16)],
        scratch_shapes=[pltpu.VMEM((t, dim), F32)],
        input_output_aliases={5: 0} if extra else {},
        compiler_params=pltpu.CompilerParams(dimension_semantics=('arbitrary',), vmem_limit_bytes=48 * 1024 * 1024),
        cost_estimate=pl.CostEstimate(flops=4 * t * dim * hidden, bytes_accessed=4 * dim * hidden + 4 * t * hidden,
                                      transcendentals=t * hidden),
        name='mlp_bwd',
    )(d_next, h, z, w1t, w2, *extra)


BOTH = ('model', 'data')


def solution(mesh):
    spec_col = P(None, 'model')
    spec_row = P('model', None)
    spec_act = P('data', None, None)
    spec_rep = P(None, None)

    def device_step(x_in, cot_out, step_emb, w_q, w_k, w_v, w_o, w_1, w_2):
        layer_count, dim = step_emb.shape
        core = lax.axis_index('data')
        chip = lax.axis_index('model')
        chip_x = lax.rem(chip, 2)
        chip_y = lax.div(chip, 2)

        def take(v, which, axis, parts=2):
            size = v.shape[axis] // parts
            return lax.dynamic_slice_in_dim(v, which * size, size, axis)

        def gather(v):
            return lax.all_gather(v, BOTH, axis=0, tiled=True)

        def scatter(v):
            return lax.psum_scatter(v, BOTH, scatter_dimension=0, tiled=True)

        def my_tokens(v):
            mine = lax.dynamic_index_in_dim(v, chip_x, 0, keepdims=False)
            recv = pp_d(take(mine, 1 - core, 0))
            return jnp.where(core == chip_y, take(mine, core, 0), recv)

        wk = gather(take(w_k, core, 1).T)
        wv = gather(take(w_v, core, 1).T)
        wq = gather(take(w_q, core, 1).T)
        wo = gather(take(w_o, core, 0))
        w1 = gather(take(w_1, core, 1).T)
        w2 = gather(take(w_2, core, 0))

        x_cur = my_tokens(x_in)
        d_cur = my_tokens(cot_out)

        saved = []
        g_hist = None
        for layer in range(layer_count):
            s = x_cur.astype(F32) + step_emb[layer].astype(F32)
            u = rms_norm(s).astype(BF16)
            kv = jnp.concatenate([nt(u, wk).astype(BF16), nt(u, wv).astype(BF16)], axis=1)
            kv_s = pp_d(kv)
            q = nt(u, wq).astype(BF16)
            ctx, lse = attn_fwd(q, kv, kv_s)
            h = (s + nn(ctx, wo)).astype(BF16)
            m = rms_norm(h.astype(F32)).astype(BF16)
            z, g_hist, x_next = mlp_fwd(m, h, w1, w2, layer, layer_count, g_hist)
            saved.append((x_cur, u, q, kv, kv_s, ctx, lse, h, m, z))
            x_cur = x_next

        hist = []
        up_hist = None
        for layer in reversed(range(layer_count)):
            x_l, u, q, kv, kv_s, ctx, lse, h, m, z = saved[layer]
            d_next = d_cur
            if layer == 0:
                next_h = jnp.concatenate([d_next] + [e[0] for e in reversed(hist)], axis=0)
                term_2, d_next = lax.optimization_barrier((tn(g_hist.reshape(-1, g_hist.shape[-1]), next_h), d_next))
                grad_2 = scatter(term_2)
            up_hist, d_mid = mlp_bwd(d_next, h, z, w1, w2, layer, layer_count, up_hist)
            if layer == 0:
                m_h = jnp.concatenate([m] + [e[1] for e in reversed(hist)], axis=0)
                term_1, d_mid = lax.optimization_barrier((tn(up_hist.reshape(-1, up_hist.shape[-1]), m_h), d_mid))
                grad_1 = scatter(term_1)
                mid_h = jnp.concatenate([d_mid] + [e[2] for e in reversed(hist)], axis=0)
                ctx_h = jnp.concatenate([ctx] + [e[3] for e in reversed(hist)], axis=0)
                term_o, d_mid = lax.optimization_barrier((tn(ctx_h, mid_h), d_mid))
                grad_o = scatter(term_o)
            d_ctx = nt(d_mid, wo).astype(BF16)
            dq, dko, dks, dvo, dvs = attn_bwd(q, kv, kv_s, d_ctx, lse)
            dk = (dko + pp_d(dks)).astype(BF16)
            dv = (dvo + pp_d(dvs)).astype(BF16)
            d_norm1 = (nn(dq, wq) + nn(dk, wk) + nn(dv, wv)).astype(BF16)
            s = x_l.astype(F32) + step_emb[layer].astype(F32)
            norm_pull_x = jax.vjp(rms_norm, s)[1]
            d_cur = (d_mid.astype(F32) + norm_pull_x(d_norm1.astype(F32))[0]).astype(BF16)
            hist.append((d_next, m, d_mid, ctx, u, dq, dk, dv))

        u_h, dq_h, dk_h, dv_h = [jnp.concatenate([e[i] for e in reversed(hist)], axis=0) for i in (4, 5, 6, 7)]
        grad_q = scatter(tn(dq_h, u_h))
        grad_k = scatter(tn(dk_h, u_h))
        grad_v = scatter(tn(dv_h, u_h))
        d_x = lax.dynamic_slice_in_dim(gather(d_cur).reshape((4, 1024, dim)), 2 * core, 2, 0)

        def whole(v):
            other = pp_d(v)
            size = v.shape[0]
            out = lax.dynamic_update_slice_in_dim(jnp.zeros((2 * size,) + v.shape[1:], v.dtype), v, core * size, 0)
            return lax.dynamic_update_slice_in_dim(out, other, (1 - core) * size, 0)

        return (whole(grad_q).T, whole(grad_k).T, whole(grad_v).T, whole(grad_o), whole(grad_1).T, whole(grad_2), d_x)

    return jax.shard_map(device_step, mesh=mesh,
                         in_specs=(spec_act, spec_act, spec_rep, spec_col, spec_col, spec_col, spec_row, spec_col, spec_row),
                         out_specs=(spec_col, spec_col, spec_col, spec_row, spec_col, spec_row, spec_act),
                         check_vma=False)
```

```python
import jax
import jax.numpy as jnp
from jax import lax
from jax.experimental import pallas as pl
from jax.experimental.pallas import tpu as pltpu
from jax.sharding import PartitionSpec as P


HEAD_DIM = 64
EPS_NORM = 1e-6
F32 = jnp.float32
BF16 = jnp.bfloat16
LOG2E = 1.4426950408889634
SCALE = HEAD_DIM ** -0.5

SWAP_D = [(0, 1), (1, 0)]


SWAP_X = [(0, 1), (1, 0), (2, 3), (3, 2)]
SWAP_Y = [(0, 2), (2, 0), (1, 3), (3, 1)]


def pp_x(v):
    return lax.ppermute(v, 'model', SWAP_X)


def pp_y(v):
    return lax.ppermute(v, 'model', SWAP_Y)


def pp_d(v):
    return lax.ppermute(v, 'data', SWAP_D)


def rms_norm(values):
    return values * lax.rsqrt(jnp.mean(values * values, axis=-1, keepdims=True) + EPS_NORM)


def dot(a, b, dims):
    return lax.dot_general(a, b, (dims, ((), ())), preferred_element_type=F32)


def nn(a, b):
    return dot(a, b, ((1,), (0,)))


def nt(a, b):
    return dot(a, b, ((1,), (1,)))


def tn(a, b):
    return dot(a, b, ((0,), (0,)))


def pair_masks(rows):
    lane = lax.broadcasted_iota(jnp.int32, (rows, 128), 1)
    return lane < HEAD_DIM


def attn_fwd_body(q_ref, ko_ref, ks_ref, vo_ref, vs_ref, ctx_ref, lse_ref):
    k = jnp.concatenate([ko_ref[...], ks_ref[...]], axis=0)
    v = jnp.concatenate([vo_ref[...], vs_ref[...]], axis=0)
    tq = q_ref.shape[0]
    chunk = 256
    low = pair_masks(chunk)
    scores = []
    for i in range(tq // chunk):
        q = q_ref[i * chunk:(i + 1) * chunk, :]
        zero = jnp.zeros_like(q)
        both = jnp.concatenate([jnp.where(low, q, zero), jnp.where(low, zero, q)], axis=0)
        scores.append(nt(k, both))
    for i, s in enumerate(scores):
        rows = slice(i * chunk, (i + 1) * chunk)
        m = jnp.max(s, axis=0, keepdims=True)
        p = jnp.exp2((s - m) * (SCALE * LOG2E))
        l = jnp.sum(p, axis=0, keepdims=True)
        pb = (p * (1.0 / l)).astype(BF16)
        lse = m * (SCALE * LOG2E) + jnp.log2(l)
        lse_ref[0, 0:1, rows] = lse[:, :chunk]
        lse_ref[0, 1:2, rows] = lse[:, chunk:]
        ctx_t = tn(v, pb)
        ctx_t = jnp.concatenate([ctx_t[:HEAD_DIM, :chunk], ctx_t[HEAD_DIM:, chunk:]], axis=0)
        ctx_ref[rows, :] = ctx_t.T.astype(BF16)


def attn_fwd(q, kv, kv_s):
    tq, width = q.shape
    tk = kv.shape[0]
    pairs = width // 128

    def col(off):
        return lambda j: (0, j + off)

    flops = 2 * 2 * tq * (2 * tk) * 256 * (width // HEAD_DIM)
    return pl.pallas_call(
        attn_fwd_body,
        grid=(pairs,),
        in_specs=[pl.BlockSpec((tq, 128), col(0)),
                  pl.BlockSpec((tk, 128), col(0)), pl.BlockSpec((tk, 128), col(0)),
                  pl.BlockSpec((tk, 128), col(pairs)), pl.BlockSpec((tk, 128), col(pairs))],
        out_specs=[pl.BlockSpec((tq, 128), col(0)),
                   pl.BlockSpec((1, 2, tq), lambda j: (j, 0, 0))],
        out_shape=[jax.ShapeDtypeStruct((tq, width), BF16),
                   jax.ShapeDtypeStruct((pairs, 2, tq), F32)],
        compiler_params=pltpu.CompilerParams(dimension_semantics=('arbitrary',),
                                             vmem_limit_bytes=48 * 1024 * 1024),
        cost_estimate=pl.CostEstimate(flops=flops, bytes_accessed=2 * (tq * width * 2 + 4 * tk * width),
                                      transcendentals=tq * 2 * tk * (width // HEAD_DIM)),
        name='attn_fwd',
    )(q, kv, kv_s, kv, kv_s)


def attn_bwd_body(*refs):
    q_ref, ko_ref, ks_ref, vo_ref, vs_ref, do_ref, lse_ref = refs[:7]
    dq_ref, dko_ref, dks_ref, dvo_ref, dvs_ref = refs[-5:]
    tk = ko_ref.shape[0]
    k = jnp.concatenate([ko_ref[...], ks_ref[...]], axis=0)
    v = jnp.concatenate([vo_ref[...], vs_ref[...]], axis=0)
    tq = q_ref.shape[0]
    chunk = 256
    low = pair_masks(chunk)
    for ref in (dko_ref, dks_ref, dvo_ref, dvs_ref):
        ref[...] = jnp.zeros_like(ref)

    def step(i, carry):
        rows = pl.ds(pl.multiple_of(i * chunk, chunk), chunk)
        q = q_ref[rows, :]
        do = do_ref[rows, :]
        lse = lse_ref[0, :, rows]
        dqs = []
        for h in range(2):
            sel = low if h == 0 else ~low
            qm = jnp.where(sel, q, jnp.zeros_like(q))
            dom = jnp.where(sel, do, jnp.zeros_like(do))
            s = nt(k, qm)
            p = jnp.exp2(s * (SCALE * LOG2E) - lse[h:h + 1, :])
            dp = nt(v, dom).astype(BF16).astype(F32)
            delta = jnp.sum(p * dp, axis=0, keepdims=True)
            ds = (p * (dp - delta)).astype(BF16)
            dv = nn(p.astype(BF16), dom)
            dk = nn(ds, qm) * SCALE
            dvo_ref[...] += dv[:tk]
            dvs_ref[...] += dv[tk:]
            dko_ref[...] += dk[:tk]
            dks_ref[...] += dk[tk:]
            dqs.append(tn(k, ds)[h * HEAD_DIM:(h + 1) * HEAD_DIM, :] * SCALE)
        dq_ref[0, rows, :] = jnp.concatenate(dqs, axis=0).T.astype(BF16)
        return carry

    lax.fori_loop(0, tq // chunk, step, 0)


def attn_bwd(q, kv, kv_s, d_ctx, lse, layer, layers, hist):
    tq, width = q.shape
    tk = kv.shape[0]
    pairs = width // 128

    def col(off):
        return lambda j: (0, j + off)

    flops = 5 * 2 * tq * (2 * tk) * 256 * (width // HEAD_DIM)
    kblk = pl.BlockSpec((tk, 128), col(0))
    extra = [] if hist is None else [hist]
    return pl.pallas_call(
        attn_bwd_body,
        grid=(pairs,),
        in_specs=[pl.BlockSpec((tq, 128), col(0)),
                  kblk, kblk,
                  pl.BlockSpec((tk, 128), col(pairs)), pl.BlockSpec((tk, 128), col(pairs)),
                  pl.BlockSpec((tq, 128), col(0)),
                  pl.BlockSpec((1, 2, tq), lambda j: (j, 0, 0))]
        + [pl.BlockSpec(memory_space=pl.ANY)] * len(extra),
        out_specs=[pl.BlockSpec((1, tq, 128), lambda j: (layer, 0, j)), kblk, kblk, kblk, kblk],
        out_shape=[jax.ShapeDtypeStruct((layers, tq, width), BF16)]
        + [jax.ShapeDtypeStruct((tk, width), F32)] * 4,
        input_output_aliases={7: 0} if extra else {},
        compiler_params=pltpu.CompilerParams(dimension_semantics=('arbitrary',),
                                             vmem_limit_bytes=48 * 1024 * 1024),
        cost_estimate=pl.CostEstimate(flops=flops, bytes_accessed=2 * (2 * tq * width * 2 + 4 * tk * width) + 16 * tk * width,
                                      transcendentals=tq * 2 * tk * (width // HEAD_DIM)),
        name='attn_bwd',
    )(q, kv, kv_s, kv, kv_s, d_ctx, lse, *extra)


GELU_C = 0.7978845608028654
GELU_A = 0.044715
BLOCK_F = 1024
SUB_F = 512
ROWS = (slice(0, 256), slice(256, 512))


def mlp_fwd_body(*refs):
    m_ref, h_ref, w1_ref, w2_ref = refs[:4]
    z_ref, g_ref, x_ref, acc_ref = refs[-4:]
    j = pl.program_id(0)

    @pl.when(j == 0)
    def _():
        acc_ref[...] = h_ref[...].astype(F32)

    for i in range(0, BLOCK_F, SUB_F):
        cols = slice(i, i + SUB_F)
        for rows in ROWS:
            z = nt(m_ref[rows, :], w1_ref[cols, :]).astype(BF16)
            z_ref[rows, cols] = z
            zf = z.astype(F32)
            t = jnp.tanh(zf * (GELU_C + (GELU_A * GELU_C) * (zf * zf)))
            half = 0.5 * zf
            g_ref[0, rows, cols] = (half + half * t).astype(BF16)
    for rows in ROWS:
        acc_ref[rows, :] += nn(g_ref[0, rows, :], w2_ref[...])

    @pl.when(j == pl.num_programs(0) - 1)
    def _():
        x_ref[...] = acc_ref[...].astype(BF16)


def mlp_fwd(m, h, w1t, w2, layer, layers, hist):
    t, dim = m.shape
    hidden = w2.shape[0]
    whole = pl.BlockSpec((t, dim), lambda j: (0, 0))
    wblk = pl.BlockSpec((BLOCK_F, dim), lambda j: (j, 0))
    hspec = pl.BlockSpec((1, t, BLOCK_F), lambda j: (layer, 0, j))
    extra = [] if hist is None else [hist]
    return pl.pallas_call(
        mlp_fwd_body,
        grid=(hidden // BLOCK_F,),
        in_specs=[whole, whole, wblk, wblk] + [pl.BlockSpec(memory_space=pl.ANY)] * len(extra),
        out_specs=[pl.BlockSpec((t, BLOCK_F), lambda j: (0, j)), hspec, whole],
        out_shape=[jax.ShapeDtypeStruct((t, hidden), BF16),
                   jax.ShapeDtypeStruct((layers, t, hidden), BF16),
                   jax.ShapeDtypeStruct((t, dim), BF16)],
        scratch_shapes=[pltpu.VMEM((t, dim), F32)],
        input_output_aliases={4: 1} if extra else {},
        compiler_params=pltpu.CompilerParams(dimension_semantics=('arbitrary',), vmem_limit_bytes=48 * 1024 * 1024),
        cost_estimate=pl.CostEstimate(flops=4 * t * dim * hidden, bytes_accessed=4 * dim * hidden + 4 * t * hidden,
                                      transcendentals=t * hidden),
        name='mlp_fwd',
    )(m, h, w1t, w2, *extra)


def mlp_bwd_body(*refs):
    d_ref, h_ref, z_ref, w1_ref, w2_ref = refs[:5]
    up_ref, mid_ref, acc_ref = refs[-3:]
    j = pl.program_id(0)

    @pl.when(j == 0)
    def _():
        acc_ref[...] = jnp.zeros_like(acc_ref)

    for i in range(0, BLOCK_F, SUB_F):
        cols = slice(i, i + SUB_F)
        for rows in ROWS:
            da = nt(d_ref[rows, :], w2_ref[cols, :]).astype(BF16).astype(F32)
            zf = z_ref[rows, cols].astype(F32)
            z2 = zf * zf
            t = jnp.tanh(zf * (GELU_C + (GELU_A * GELU_C) * z2))
            slope = (1.0 + t) * (0.5 + (1.0 - t) * (zf * (0.5 * GELU_C + (1.5 * GELU_A * GELU_C) * z2)))
            up_ref[0, rows, cols] = (da * slope).astype(BF16)
    for rows in ROWS:
        acc_ref[rows, :] += nn(up_ref[0, rows, :], w1_ref[...])

    @pl.when(j == pl.num_programs(0) - 1)
    def _():
        dn = acc_ref[...].astype(BF16).astype(F32)
        hf = h_ref[...].astype(F32)
        inv = lax.rsqrt(jnp.mean(hf * hf, axis=-1, keepdims=True) + EPS_NORM)
        proj = jnp.mean(hf * dn, axis=-1, keepdims=True)
        mid_ref[...] = (d_ref[...].astype(F32) + inv * dn - hf * (inv * inv * inv * proj)).astype(BF16)


def mlp_bwd(d_next, h, z, w1t, w2, layer, layers, hist):
    t, dim = h.shape
    hidden = w2.shape[0]
    whole = pl.BlockSpec((t, dim), lambda j: (0, 0))
    wblk = pl.BlockSpec((BLOCK_F, dim), lambda j: (j, 0))
    hspec = pl.BlockSpec((1, t, BLOCK_F), lambda j: (layer, 0, j))
    extra = [] if hist is None else [hist]
    return pl.pallas_call(
        mlp_bwd_body,
        grid=(hidden // BLOCK_F,),
        in_specs=[whole, whole, pl.BlockSpec((t, BLOCK_F), lambda j: (0, j)), wblk, wblk]
        + [pl.BlockSpec(memory_space=pl.ANY)] * len(extra),
        out_specs=[hspec, whole],
        out_shape=[jax.ShapeDtypeStruct((layers, t, hidden), BF16), jax.ShapeDtypeStruct((t, dim), BF16)],
        scratch_shapes=[pltpu.VMEM((t, dim), F32)],
        input_output_aliases={5: 0} if extra else {},
        compiler_params=pltpu.CompilerParams(dimension_semantics=('arbitrary',), vmem_limit_bytes=48 * 1024 * 1024),
        cost_estimate=pl.CostEstimate(flops=4 * t * dim * hidden, bytes_accessed=4 * dim * hidden + 4 * t * hidden,
                                      transcendentals=t * hidden),
        name='mlp_bwd',
    )(d_next, h, z, w1t, w2, *extra)


def gather_pieces(part_a, part_b):
    xa, xb = pp_x(part_a), pp_x(part_b)
    ya, yb = pp_y(part_a), pp_y(part_b)
    da, db = pp_y(xa), pp_x(yb)
    own = [(xa, xb), (ya, yb), (da, db)]
    return own, [(pp_d(a), pp_d(b)) for a, b in own]


def reduce_pieces(piece):
    total = {}
    for r in (3, 1, 2, 0):
        for part in (0, 1):
            total[r, part] = piece(r, 0, part) + pp_d(piece(r, 1, part))
    a0 = total[0, 0] + pp_x(total[1, 0])
    a2 = total[2, 0] + pp_x(total[3, 0])
    b0 = total[0, 1] + pp_y(total[2, 1])
    b1 = total[1, 1] + pp_y(total[3, 1])
    own = (a0 + pp_y(a2), b0 + pp_x(b1))
    return own, (pp_d(own[0]), pp_d(own[1]))


BOTH = ('model', 'data')


def solution(mesh):
    spec_col = P(None, 'model')
    spec_row = P('model', None)
    spec_act = P('data', None, None)
    spec_rep = P(None, None)

    def device_step(x_in, cot_out, step_emb, w_q, w_k, w_v, w_o, w_1, w_2):
        layer_count, dim = step_emb.shape
        core = lax.axis_index('data')
        chip = lax.axis_index('model')
        chip_x = lax.rem(chip, 2)
        chip_y = lax.div(chip, 2)
        nbr_x = chip + 1 - 2 * chip_x
        nbr_y = lax.rem(chip + 2, 4)
        diag = lax.rem(nbr_x + 2, 4)
        chips = (chip, nbr_x, nbr_y, diag)
        hid = w_q.shape[1]
        half_d = dim // 2
        quart = half_d // 2

        def take(v, which, axis, size):
            return lax.dynamic_slice_in_dim(v, which * size, size, axis)

        def put(buf, v, which, axis):
            return lax.dynamic_update_slice_in_dim(buf, v, which * v.shape[axis], axis)

        def gather(v):
            return lax.all_gather(v, BOTH, axis=0, tiled=True)

        def scatter(v):
            return lax.psum_scatter(v, BOTH, scatter_dimension=0, tiled=True)

        def ordered(own, sib, axis):
            size = own.shape[axis]
            shape = own.shape[:axis] + (2 * size,) + own.shape[axis + 1:]
            return put(put(jnp.zeros(shape, own.dtype), own, core, axis), sib, 1 - core, axis)

        def keep(hist, v, layer):
            if hist is None:
                hist = jnp.zeros((layer_count,) + v.shape, v.dtype)
            return lax.dynamic_update_slice(hist, v[None], (layer, 0, 0))

        def my_tokens(v):
            mine = lax.dynamic_index_in_dim(v, chip_x, 0, keepdims=False)
            half = mine.shape[0] // 2
            recv = pp_d(take(mine, 1 - core, 0, half))
            return jnp.where(core == chip_y, take(mine, core, 0, half), recv)

        own_2 = take(w_2, core, 0, w_2.shape[0] // 2)
        rows = own_2.shape[0] // 2
        p2_own, p2_sib = gather_pieces(own_2[:rows], own_2[rows:])
        wk = gather(take(w_k, core, 1, hid // 2).T)
        wv = gather(take(w_v, core, 1, hid // 2).T)
        wq = gather(take(w_q, core, 1, hid // 2).T)
        wo = gather(take(w_o, core, 0, hid // 2))
        w1 = gather(take(w_1, core, 1, w_1.shape[1] // 2).T)
        w2 = put(jnp.zeros((4 * w_2.shape[0], dim), BF16), w_2, chip, 0)
        for r in (1, 2, 3):
            for part in (0, 1):
                w2 = put(w2, p2_own[r - 1][part], 4 * chips[r] + 2 * core + part, 0)
                w2 = put(w2, p2_sib[r - 1][part], 4 * chips[r] + 2 * (1 - core) + part, 0)

        x_cur = my_tokens(x_in)
        d_cur = my_tokens(cot_out)

        saved = []
        g_hist = u_hist = m_hist = ctx_hist = None
        for layer in range(layer_count):
            s = x_cur.astype(F32) + step_emb[layer].astype(F32)
            u = rms_norm(s).astype(BF16)
            kv = jnp.concatenate([nt(u, wk).astype(BF16), nt(u, wv).astype(BF16)], axis=1)
            kv_s = pp_d(kv)
            q = nt(u, wq).astype(BF16)
            ctx, lse = attn_fwd(q, kv, kv_s)
            h = (s + nn(ctx, wo)).astype(BF16)
            m = rms_norm(h.astype(F32)).astype(BF16)
            z, g_hist, x_next = mlp_fwd(m, h, w1, w2, layer, layer_count, g_hist)
            u_hist, m_hist, ctx_hist = keep(u_hist, u, layer), keep(m_hist, m, layer), keep(ctx_hist, ctx, layer)
            saved.append((x_cur, q, kv, kv_s, lse, h, z))
            x_cur = x_next

        def flat(v):
            return v.reshape(-1, v.shape[-1])

        up_hist = next_hist = mid_hist = dq_hist = dkv_hist = None
        for layer in reversed(range(layer_count)):
            x_l, q, kv, kv_s, lse, h, z = saved[layer]
            d_next = d_cur
            next_hist = keep(next_hist, d_next, layer)
            if layer == 0:
                term_2, d_next = lax.optimization_barrier((tn(flat(g_hist), flat(next_hist)), d_next))
                grad_2 = scatter(term_2)
            up_hist, d_mid = mlp_bwd(d_next, h, z, w1, w2, layer, layer_count, up_hist)
            mid_hist = keep(mid_hist, d_mid, layer)
            if layer == 0:
                term_1, d_mid = lax.optimization_barrier((tn(flat(up_hist), flat(m_hist)), d_mid))
                grad_1 = scatter(term_1)
            d_ctx = nt(d_mid, wo).astype(BF16)
            dq_hist, dko, dks, dvo, dvs = attn_bwd(q, kv, kv_s, d_ctx, lse, layer, layer_count, dq_hist)
            dk = (dko + pp_d(dks)).astype(BF16)
            dv = (dvo + pp_d(dvs)).astype(BF16)
            dkv_hist = keep(dkv_hist, jnp.concatenate([dk, dv], axis=1), layer)
            d_norm1 = (nn(dq_hist[layer], wq) + nn(dk, wk) + nn(dv, wv)).astype(BF16)
            s = x_l.astype(F32) + step_emb[layer].astype(F32)
            norm_pull_x = jax.vjp(rms_norm, s)[1]
            d_cur = (d_mid.astype(F32) + norm_pull_x(d_norm1.astype(F32))[0]).astype(BF16)

        def fixed(v):
            return lax.optimization_barrier(v)

        ctx_f, dq_f, dkv_f, mid_f, u_f = flat(ctx_hist), flat(dq_hist), flat(dkv_hist), flat(mid_hist), flat(u_hist)
        mid_half = [fixed(take(mid_f, w, 1, half_d)) for w in (core, 1 - core)]
        u_half = [fixed(take(u_f, w, 1, half_d)) for w in (core, 1 - core)]
        ctx_r = [fixed(take(ctx_f, c, 1, hid)) for c in chips]
        dqkv_r = [fixed(jnp.concatenate([take(dq_f, c, 1, hid), take(dkv_f, c, 1, hid), take(dkv_f, 4 + c, 1, hid)], axis=1))
                  for c in chips]

        def piece_o(r, half, part):
            return tn(ctx_r[r], mid_half[half][:, part * quart:(part + 1) * quart])

        def piece_qkv(r, half, part):
            return tn(u_half[half][:, part * quart:(part + 1) * quart], dqkv_r[r])

        own, sib = reduce_pieces(piece_o)
        grad_o = ordered(jnp.concatenate(own, 1), jnp.concatenate(sib, 1), 1)
        own, sib = reduce_pieces(piece_qkv)
        grad_qkv = ordered(jnp.concatenate(own, 0), jnp.concatenate(sib, 0), 0)

        whole = ordered(d_cur, pp_d(d_cur), 0)
        to_row = [(2 * c + d, 2 * (c ^ 2) + d) for c in range(4) for d in range(2) if c // 2 == d]
        from_y = lax.ppermute(whole, BOTH, to_row)
        row_seq = jnp.where(chip_y == core, whole, from_y)
        d_x = jnp.zeros((2,) + whole.shape, BF16)
        d_x = put(put(d_x, row_seq[None], chip_x, 0), pp_x(row_seq)[None], 1 - chip_x, 0)

        grad_1 = ordered(grad_1, pp_d(grad_1), 0).T
        grad_2 = ordered(grad_2, pp_d(grad_2), 0)
        return (grad_qkv[:, :hid], grad_qkv[:, hid:2 * hid], grad_qkv[:, 2 * hid:], grad_o, grad_1, grad_2, d_x)

    return jax.shard_map(device_step, mesh=mesh,
                         in_specs=(spec_act, spec_act, spec_rep, spec_col, spec_col, spec_col, spec_row, spec_col, spec_row),
                         out_specs=(spec_col, spec_col, spec_col, spec_row, spec_col, spec_row, spec_act),
                         check_vma=False)
```

```python
import jax
import jax.numpy as jnp
from jax import lax
from jax.experimental import pallas as pl
from jax.experimental.pallas import tpu as pltpu
from jax.sharding import PartitionSpec as P


HEAD_DIM = 64
EPS_NORM = 1e-6
F32 = jnp.float32
BF16 = jnp.bfloat16
LOG2E = 1.4426950408889634
SCALE = HEAD_DIM ** -0.5

SWAP_D = [(0, 1), (1, 0)]


SWAP_X = [(0, 1), (1, 0), (2, 3), (3, 2)]
SWAP_Y = [(0, 2), (2, 0), (1, 3), (3, 1)]


def pp_x(v):
    return lax.ppermute(v, 'model', SWAP_X)


def pp_y(v):
    return lax.ppermute(v, 'model', SWAP_Y)


def pp_d(v):
    return lax.ppermute(v, 'data', SWAP_D)


def rms_norm(values):
    return values * lax.rsqrt(jnp.mean(values * values, axis=-1, keepdims=True) + EPS_NORM)


def dot(a, b, dims):
    return lax.dot_general(a, b, (dims, ((), ())), preferred_element_type=F32)


def nn(a, b):
    return dot(a, b, ((1,), (0,)))


def nt(a, b):
    return dot(a, b, ((1,), (1,)))


def tn(a, b):
    return dot(a, b, ((0,), (0,)))


def pair_masks(rows):
    lane = lax.broadcasted_iota(jnp.int32, (rows, 128), 1)
    return lane < HEAD_DIM


def attn_fwd_body(q_ref, ko_ref, ks_ref, vo_ref, vs_ref, ctx_ref, lse_ref):
    k = jnp.concatenate([ko_ref[...], ks_ref[...]], axis=0)
    v = jnp.concatenate([vo_ref[...], vs_ref[...]], axis=0)
    tq = q_ref.shape[0]
    chunk = 256
    low = pair_masks(chunk)
    scores = []
    for i in range(tq // chunk):
        q = q_ref[i * chunk:(i + 1) * chunk, :]
        zero = jnp.zeros_like(q)
        both = jnp.concatenate([jnp.where(low, q, zero), jnp.where(low, zero, q)], axis=0)
        scores.append(nt(k, both))
    for i, s in enumerate(scores):
        rows = slice(i * chunk, (i + 1) * chunk)
        m = jnp.max(s, axis=0, keepdims=True)
        p = jnp.exp2((s - m) * (SCALE * LOG2E))
        l = jnp.sum(p, axis=0, keepdims=True)
        pb = (p * (1.0 / l)).astype(BF16)
        lse = m * (SCALE * LOG2E) + jnp.log2(l)
        lse_ref[0, 0:1, rows] = lse[:, :chunk]
        lse_ref[0, 1:2, rows] = lse[:, chunk:]
        ctx_t = tn(v, pb)
        ctx_t = jnp.concatenate([ctx_t[:HEAD_DIM, :chunk], ctx_t[HEAD_DIM:, chunk:]], axis=0)
        ctx_ref[rows, :] = ctx_t.T.astype(BF16)


def attn_fwd(q, kv, kv_s):
    tq, width = q.shape
    tk = kv.shape[0]
    pairs = width // 128

    def col(off):
        return lambda j: (0, j + off)

    flops = 2 * 2 * tq * (2 * tk) * 256 * (width // HEAD_DIM)
    return pl.pallas_call(
        attn_fwd_body,
        grid=(pairs,),
        in_specs=[pl.BlockSpec((tq, 128), col(0)),
                  pl.BlockSpec((tk, 128), col(0)), pl.BlockSpec((tk, 128), col(0)),
                  pl.BlockSpec((tk, 128), col(pairs)), pl.BlockSpec((tk, 128), col(pairs))],
        out_specs=[pl.BlockSpec((tq, 128), col(0)),
                   pl.BlockSpec((1, 2, tq), lambda j: (j, 0, 0))],
        out_shape=[jax.ShapeDtypeStruct((tq, width), BF16),
                   jax.ShapeDtypeStruct((pairs, 2, tq), F32)],
        compiler_params=pltpu.CompilerParams(dimension_semantics=('arbitrary',),
                                             vmem_limit_bytes=48 * 1024 * 1024),
        cost_estimate=pl.CostEstimate(flops=flops, bytes_accessed=2 * (tq * width * 2 + 4 * tk * width),
                                      transcendentals=tq * 2 * tk * (width // HEAD_DIM)),
        name='attn_fwd',
    )(q, kv, kv_s, kv, kv_s)


def attn_bwd_body(*refs):
    q_ref, ko_ref, ks_ref, vo_ref, vs_ref, do_ref, lse_ref = refs[:7]
    dq_ref, dko_ref, dks_ref, dvo_ref, dvs_ref = refs[-5:]
    tk = ko_ref.shape[0]
    k = jnp.concatenate([ko_ref[...], ks_ref[...]], axis=0)
    v = jnp.concatenate([vo_ref[...], vs_ref[...]], axis=0)
    tq = q_ref.shape[0]
    chunk = 256
    low = pair_masks(chunk)
    for ref in (dko_ref, dks_ref, dvo_ref, dvs_ref):
        ref[...] = jnp.zeros_like(ref)

    def step(i, carry):
        rows = pl.ds(pl.multiple_of(i * chunk, chunk), chunk)
        q = q_ref[rows, :]
        do = do_ref[rows, :]
        lse = lse_ref[0, :, rows]
        dqs = []
        for h in range(2):
            sel = low if h == 0 else ~low
            qm = jnp.where(sel, q, jnp.zeros_like(q))
            dom = jnp.where(sel, do, jnp.zeros_like(do))
            s = nt(k, qm)
            p = jnp.exp2(s * (SCALE * LOG2E) - lse[h:h + 1, :])
            dp = nt(v, dom).astype(BF16).astype(F32)
            delta = jnp.sum(p * dp, axis=0, keepdims=True)
            ds = (p * (dp - delta)).astype(BF16)
            dv = nn(p.astype(BF16), dom)
            dk = nn(ds, qm) * SCALE
            dvo_ref[...] += dv[:tk]
            dvs_ref[...] += dv[tk:]
            dko_ref[...] += dk[:tk]
            dks_ref[...] += dk[tk:]
            dqs.append(tn(k, ds)[h * HEAD_DIM:(h + 1) * HEAD_DIM, :] * SCALE)
        dq_ref[0, rows, :] = jnp.concatenate(dqs, axis=0).T.astype(BF16)
        return carry

    lax.fori_loop(0, tq // chunk, step, 0)


def attn_bwd(q, kv, kv_s, d_ctx, lse, layer, layers, hist):
    tq, width = q.shape
    tk = kv.shape[0]
    pairs = width // 128

    def col(off):
        return lambda j: (0, j + off)

    flops = 5 * 2 * tq * (2 * tk) * 256 * (width // HEAD_DIM)
    kblk = pl.BlockSpec((tk, 128), col(0))
    extra = [] if hist is None else [hist]
    return pl.pallas_call(
        attn_bwd_body,
        grid=(pairs,),
        in_specs=[pl.BlockSpec((tq, 128), col(0)),
                  kblk, kblk,
                  pl.BlockSpec((tk, 128), col(pairs)), pl.BlockSpec((tk, 128), col(pairs)),
                  pl.BlockSpec((tq, 128), col(0)),
                  pl.BlockSpec((1, 2, tq), lambda j: (j, 0, 0))]
        + [pl.BlockSpec(memory_space=pl.ANY)] * len(extra),
        out_specs=[pl.BlockSpec((1, tq, 128), lambda j: (layer, 0, j)), kblk, kblk, kblk, kblk],
        out_shape=[jax.ShapeDtypeStruct((layers, tq, width), BF16)]
        + [jax.ShapeDtypeStruct((tk, width), F32)] * 4,
        input_output_aliases={7: 0} if extra else {},
        compiler_params=pltpu.CompilerParams(dimension_semantics=('arbitrary',),
                                             vmem_limit_bytes=48 * 1024 * 1024),
        cost_estimate=pl.CostEstimate(flops=flops, bytes_accessed=2 * (2 * tq * width * 2 + 4 * tk * width) + 16 * tk * width,
                                      transcendentals=tq * 2 * tk * (width // HEAD_DIM)),
        name='attn_bwd',
    )(q, kv, kv_s, kv, kv_s, d_ctx, lse, *extra)


GELU_C = 0.7978845608028654
GELU_A = 0.044715
BLOCK_F = 768
SUB_F = 768
ROWS = (slice(0, 256), slice(256, 512))


def mlp_fwd_body(m_ref, h_ref, w1_ref, w2_ref, z_ref, g_ref, x_ref, acc_ref):
    j = pl.program_id(0)

    @pl.when(j == 0)
    def _():
        acc_ref[...] = h_ref[...].astype(F32)

    for i in range(0, BLOCK_F, SUB_F):
        cols = slice(i, i + SUB_F)
        for rows in ROWS:
            z = nt(m_ref[rows, :], w1_ref[cols, :]).astype(BF16)
            z_ref[rows, cols] = z
            zf = z.astype(F32)
            t = jnp.tanh(zf * (GELU_C + (GELU_A * GELU_C) * (zf * zf)))
            half = 0.5 * zf
            g_ref[0, rows, cols] = (half + half * t).astype(BF16)
    for rows in ROWS:
        acc_ref[rows, :] += nn(g_ref[0, rows, :], w2_ref[...])

    @pl.when(j == pl.num_programs(0) - 1)
    def _():
        x_ref[...] = acc_ref[...].astype(BF16)


def mlp_fwd(m, h, w1t, w2):
    t, dim = m.shape
    hidden = w2.shape[0]
    whole = pl.BlockSpec((t, dim), lambda j: (0, 0))
    wblk = pl.BlockSpec((BLOCK_F, dim), lambda j: (j, 0))
    return pl.pallas_call(
        mlp_fwd_body,
        grid=(hidden // BLOCK_F,),
        in_specs=[whole, whole, wblk, wblk],
        out_specs=[pl.BlockSpec((t, BLOCK_F), lambda j: (0, j)),
                   pl.BlockSpec((1, t, BLOCK_F), lambda j: (j, 0, 0)), whole],
        out_shape=[jax.ShapeDtypeStruct((t, hidden), BF16),
                   jax.ShapeDtypeStruct((hidden // BLOCK_F, t, BLOCK_F), BF16),
                   jax.ShapeDtypeStruct((t, dim), BF16)],
        scratch_shapes=[pltpu.VMEM((t, dim), F32)],
        compiler_params=pltpu.CompilerParams(dimension_semantics=('arbitrary',), vmem_limit_bytes=48 * 1024 * 1024),
        cost_estimate=pl.CostEstimate(flops=4 * t * dim * hidden, bytes_accessed=4 * dim * hidden + 4 * t * hidden,
                                      transcendentals=t * hidden),
        name='mlp_fwd',
    )(m, h, w1t, w2)


def mlp_bwd_body(*refs):
    d_ref, h_ref, z_ref, w1_ref, w2_ref = refs[:5]
    up_ref, mid_ref, acc_ref = refs[-3:]
    j = pl.program_id(0)

    @pl.when(j == 0)
    def _():
        acc_ref[...] = jnp.zeros_like(acc_ref)

    for i in range(0, BLOCK_F, SUB_F):
        cols = slice(i, i + SUB_F)
        for rows in ROWS:
            da = nt(d_ref[rows, :], w2_ref[cols, :]).astype(BF16).astype(F32)
            zf = z_ref[rows, cols].astype(F32)
            z2 = zf * zf
            t = jnp.tanh(zf * (GELU_C + (GELU_A * GELU_C) * z2))
            slope = (1.0 + t) * (0.5 + (1.0 - t) * (zf * (0.5 * GELU_C + (1.5 * GELU_A * GELU_C) * z2)))
            up_ref[0, rows, cols] = (da * slope).astype(BF16)
    for rows in ROWS:
        acc_ref[rows, :] += nn(up_ref[0, rows, :], w1_ref[...])

    @pl.when(j == pl.num_programs(0) - 1)
    def _():
        dn = acc_ref[...].astype(BF16).astype(F32)
        hf = h_ref[...].astype(F32)
        inv = lax.rsqrt(jnp.mean(hf * hf, axis=-1, keepdims=True) + EPS_NORM)
        proj = jnp.mean(hf * dn, axis=-1, keepdims=True)
        mid_ref[...] = (d_ref[...].astype(F32) + inv * dn - hf * (inv * inv * inv * proj)).astype(BF16)


def mlp_bwd(d_next, h, z, w1t, w2, layer, layers, hist):
    t, dim = h.shape
    hidden = w2.shape[0]
    whole = pl.BlockSpec((t, dim), lambda j: (0, 0))
    wblk = pl.BlockSpec((BLOCK_F, dim), lambda j: (j, 0))
    hspec = pl.BlockSpec((1, t, BLOCK_F), lambda j: (layer, 0, j))
    extra = [] if hist is None else [hist]
    return pl.pallas_call(
        mlp_bwd_body,
        grid=(hidden // BLOCK_F,),
        in_specs=[whole, whole, pl.BlockSpec((t, BLOCK_F), lambda j: (0, j)), wblk, wblk]
        + [pl.BlockSpec(memory_space=pl.ANY)] * len(extra),
        out_specs=[hspec, whole],
        out_shape=[jax.ShapeDtypeStruct((layers, t, hidden), BF16), jax.ShapeDtypeStruct((t, dim), BF16)],
        scratch_shapes=[pltpu.VMEM((t, dim), F32)],
        input_output_aliases={5: 0} if extra else {},
        compiler_params=pltpu.CompilerParams(dimension_semantics=('arbitrary',), vmem_limit_bytes=48 * 1024 * 1024),
        cost_estimate=pl.CostEstimate(flops=4 * t * dim * hidden, bytes_accessed=4 * dim * hidden + 4 * t * hidden,
                                      transcendentals=t * hidden),
        name='mlp_bwd',
    )(d_next, h, z, w1t, w2, *extra)


def gather_pieces(part_a, part_b):
    xa, xb = pp_x(part_a), pp_x(part_b)
    ya, yb = pp_y(part_a), pp_y(part_b)
    da, db = pp_y(xa), pp_x(yb)
    own = [(xa, xb), (ya, yb), (da, db)]
    return own, [(pp_d(a), pp_d(b)) for a, b in own]


def reduce_pieces(piece):
    total = {}
    for r in (3, 1, 2, 0):
        for part in (0, 1):
            total[r, part] = piece(r, 0, part) + pp_d(piece(r, 1, part))
    a0 = total[0, 0] + pp_x(total[1, 0])
    a2 = total[2, 0] + pp_x(total[3, 0])
    b0 = total[0, 1] + pp_y(total[2, 1])
    b1 = total[1, 1] + pp_y(total[3, 1])
    own = (a0 + pp_y(a2), b0 + pp_x(b1))
    return own, (pp_d(own[0]), pp_d(own[1]))


BOTH = ('model', 'data')


def solution(mesh):
    spec_col = P(None, 'model')
    spec_row = P('model', None)
    spec_act = P('data', None, None)
    spec_rep = P(None, None)

    def device_step(x_in, cot_out, step_emb, w_q, w_k, w_v, w_o, w_1, w_2):
        layer_count, dim = step_emb.shape
        core = lax.axis_index('data')
        chip = lax.axis_index('model')
        chip_x = lax.rem(chip, 2)
        chip_y = lax.div(chip, 2)
        nbr_x = chip + 1 - 2 * chip_x
        nbr_y = lax.rem(chip + 2, 4)
        diag = lax.rem(nbr_x + 2, 4)
        chips = (chip, nbr_x, nbr_y, diag)
        hid = w_q.shape[1]
        half_d = dim // 2
        quart = half_d // 2

        def take(v, which, axis, size):
            return lax.dynamic_slice_in_dim(v, which * size, size, axis)

        def put(buf, v, which, axis):
            return lax.dynamic_update_slice_in_dim(buf, v, which * v.shape[axis], axis)

        def gather(v):
            return lax.all_gather(v, BOTH, axis=0, tiled=True)

        def scatter(v):
            return lax.psum_scatter(v, BOTH, scatter_dimension=0, tiled=True)

        def ordered(own, sib, axis):
            size = own.shape[axis]
            shape = own.shape[:axis] + (2 * size,) + own.shape[axis + 1:]
            return put(put(jnp.zeros(shape, own.dtype), own, core, axis), sib, 1 - core, axis)

        def keep(hist, v, layer):
            if hist is None:
                hist = jnp.zeros((layer_count,) + v.shape, v.dtype)
            return lax.dynamic_update_slice(hist, v[None], (layer, 0, 0))

        def my_tokens(v):
            mine = lax.dynamic_index_in_dim(v, chip_x, 0, keepdims=False)
            half = mine.shape[0] // 2
            recv = pp_d(take(mine, 1 - core, 0, half))
            return jnp.where(core == chip_y, take(mine, core, 0, half), recv)

        own_2 = take(w_2, core, 0, w_2.shape[0] // 2)
        rows = own_2.shape[0] // 2
        p2_own, p2_sib = gather_pieces(own_2[:rows], own_2[rows:])
        wk = gather(take(w_k, core, 1, hid // 2).T)
        wv = gather(take(w_v, core, 1, hid // 2).T)
        wq = gather(take(w_q, core, 1, hid // 2).T)
        wo = gather(take(w_o, core, 0, hid // 2))
        w1 = gather(take(w_1, core, 1, w_1.shape[1] // 2).T)
        w2 = put(jnp.zeros((4 * w_2.shape[0], dim), BF16), w_2, chip, 0)
        for r in (1, 2, 3):
            for part in (0, 1):
                w2 = put(w2, p2_own[r - 1][part], 4 * chips[r] + 2 * core + part, 0)
                w2 = put(w2, p2_sib[r - 1][part], 4 * chips[r] + 2 * (1 - core) + part, 0)

        x_cur = my_tokens(x_in)
        d_cur = my_tokens(cot_out)

        saved = []
        g_mine = []
        u_hist = m_hist = ctx_hist = None
        for layer in range(layer_count):
            s = x_cur.astype(F32) + step_emb[layer].astype(F32)
            u = rms_norm(s).astype(BF16)
            kv = jnp.concatenate([nt(u, wk).astype(BF16), nt(u, wv).astype(BF16)], axis=1)
            kv_s = pp_d(kv)
            q = nt(u, wq).astype(BF16)
            ctx, lse = attn_fwd(q, kv, kv_s)
            h = (s + nn(ctx, wo)).astype(BF16)
            m = rms_norm(h.astype(F32)).astype(BF16)
            z, g, x_next = mlp_fwd(m, h, w1, w2)
            g_mine.append(lax.all_to_all(g.reshape(-1, g.shape[-1]), BOTH, split_axis=0, concat_axis=0, tiled=True))
            u_hist, m_hist, ctx_hist = keep(u_hist, u, layer), keep(m_hist, m, layer), keep(ctx_hist, ctx, layer)
            saved.append((x_cur, q, kv, kv_s, lse, h, z))
            x_cur = x_next

        def flat(v):
            return v.reshape(-1, v.shape[-1])

        up_hist = mid_hist = dq_hist = dkv_hist = grad_2 = None
        for layer in reversed(range(layer_count)):
            x_l, q, kv, kv_s, lse, h, z = saved[layer]
            d_next = d_cur
            next_all = gather(d_next)
            term = tn(g_mine[layer], next_all)
            grad_2 = term if grad_2 is None else grad_2 + term
            up_hist, d_mid = mlp_bwd(d_next, h, z, w1, w2, layer, layer_count, up_hist)
            mid_hist = keep(mid_hist, d_mid, layer)
            if layer == 0:
                term_1, d_mid = lax.optimization_barrier((tn(flat(up_hist), flat(m_hist)), d_mid))
                grad_1 = scatter(term_1)
            d_ctx = nt(d_mid, wo).astype(BF16)
            dq_hist, dko, dks, dvo, dvs = attn_bwd(q, kv, kv_s, d_ctx, lse, layer, layer_count, dq_hist)
            dk = (dko + pp_d(dks)).astype(BF16)
            dv = (dvo + pp_d(dvs)).astype(BF16)
            dkv_hist = keep(dkv_hist, jnp.concatenate([dk, dv], axis=1), layer)
            d_norm1 = (nn(dq_hist[layer], wq) + nn(dk, wk) + nn(dv, wv)).astype(BF16)
            s = x_l.astype(F32) + step_emb[layer].astype(F32)
            norm_pull_x = jax.vjp(rms_norm, s)[1]
            d_cur = (d_mid.astype(F32) + norm_pull_x(d_norm1.astype(F32))[0]).astype(BF16)

        def fixed(v):
            return lax.optimization_barrier(v)

        ctx_f, dq_f, dkv_f, mid_f, u_f = flat(ctx_hist), flat(dq_hist), flat(dkv_hist), flat(mid_hist), flat(u_hist)
        mid_half = [fixed(take(mid_f, w, 1, half_d)) for w in (core, 1 - core)]
        u_half = [fixed(take(u_f, w, 1, half_d)) for w in (core, 1 - core)]
        ctx_r = [fixed(take(ctx_f, c, 1, hid)) for c in chips]
        dqkv_r = [fixed(jnp.concatenate([take(dq_f, c, 1, hid), take(dkv_f, c, 1, hid), take(dkv_f, 4 + c, 1, hid)], axis=1))
                  for c in chips]

        def piece_o(r, half, part):
            return tn(ctx_r[r], mid_half[half][:, part * quart:(part + 1) * quart])

        def piece_qkv(r, half, part):
            return tn(u_half[half][:, part * quart:(part + 1) * quart], dqkv_r[r])

        own, sib = reduce_pieces(piece_o)
        grad_o = ordered(jnp.concatenate(own, 1), jnp.concatenate(sib, 1), 1)
        own, sib = reduce_pieces(piece_qkv)
        grad_qkv = ordered(jnp.concatenate(own, 0), jnp.concatenate(sib, 0), 0)

        whole = ordered(d_cur, pp_d(d_cur), 0)
        to_row = [(2 * c + d, 2 * (c ^ 2) + d) for c in range(4) for d in range(2) if c // 2 == d]
        from_y = lax.ppermute(whole, BOTH, to_row)
        row_seq = jnp.where(chip_y == core, whole, from_y)
        d_x = jnp.zeros((2,) + whole.shape, BF16)
        d_x = put(put(d_x, row_seq[None], chip_x, 0), pp_x(row_seq)[None], 1 - chip_x, 0)

        def both_halves(v):
            return lax.all_gather(v, 'data', axis=0, tiled=True)

        grad_1 = both_halves(grad_1).T
        grad_2 = both_halves(grad_2)
        return (grad_qkv[:, :hid], grad_qkv[:, hid:2 * hid], grad_qkv[:, 2 * hid:], grad_o, grad_1, grad_2, d_x)

    return jax.shard_map(device_step, mesh=mesh,
                         in_specs=(spec_act, spec_act, spec_rep, spec_col, spec_col, spec_col, spec_row, spec_col, spec_row),
                         out_specs=(spec_col, spec_col, spec_col, spec_row, spec_col, spec_row, spec_act),
                         check_vma=False)
```

```python
import functools

import jax
import jax.numpy as jnp
from jax import lax
from jax.experimental import pallas as pl
from jax.experimental.pallas import tpu as pltpu
from jax.sharding import PartitionSpec as P


HEAD_DIM = 64
EPS_NORM = 1e-6
F32 = jnp.float32
BF16 = jnp.bfloat16
LOG2E = 1.4426950408889634
VMEM_ALL = 60 * 1024 * 1024
SCALE = HEAD_DIM ** -0.5

SWAP_D = [(0, 1), (1, 0)]


SWAP_X = [(0, 1), (1, 0), (2, 3), (3, 2)]
SWAP_Y = [(0, 2), (2, 0), (1, 3), (3, 1)]


def pp_x(v):
    return lax.ppermute(v, 'model', SWAP_X)


def pp_y(v):
    return lax.ppermute(v, 'model', SWAP_Y)


def pp_d(v):
    return lax.ppermute(v, 'data', SWAP_D)


def rms_norm(values):
    return values * lax.rsqrt(jnp.mean(values * values, axis=-1, keepdims=True) + EPS_NORM)


def dot(a, b, dims):
    return lax.dot_general(a, b, (dims, ((), ())), preferred_element_type=F32)


def nn(a, b):
    return dot(a, b, ((1,), (0,)))


def nt(a, b):
    return dot(a, b, ((1,), (1,)))


def tn(a, b):
    return dot(a, b, ((0,), (0,)))


def pair_masks(rows):
    lane = lax.broadcasted_iota(jnp.int32, (rows, 128), 1)
    return lane < HEAD_DIM


CHUNK = 256


def masked_pair(q):
    low = pair_masks(CHUNK)
    zero = jnp.zeros_like(q)
    return jnp.concatenate([jnp.where(low, q, zero), jnp.where(low, zero, q)], axis=0)


def attn_fwd_body(*refs):
    q_ref, qn_ref, ko_ref, ks_ref, kno_ref, kns_ref, vo_ref, vs_ref = refs[:8]
    ctx_ref, lse_ref, a_ref, b_ref, ma_ref, mb_ref = refs[-6:]

    def scores(ko, ks, q, s_ref, m_ref):
        s = nt(jnp.concatenate([ko[...], ks[...]], axis=0), masked_pair(q))
        s_ref[...] = s
        m_ref[...] = jnp.max(s, axis=0, keepdims=True)

    def finish(s_ref, m_ref, i):
        rows = slice(i * CHUNK, (i + 1) * CHUNK)
        m = m_ref[...]
        p = jnp.exp2((s_ref[...] - m) * (SCALE * LOG2E))
        l = jnp.sum(p, axis=0, keepdims=True)
        pb = (p * (1.0 / l)).astype(BF16)
        lse = m * (SCALE * LOG2E) + jnp.log2(l)
        lse_ref[0, 0:1, rows] = lse[:, :CHUNK]
        lse_ref[0, 1:2, rows] = lse[:, CHUNK:]
        ctx_t = tn(jnp.concatenate([vo_ref[...], vs_ref[...]], axis=0), pb)
        ctx_t = jnp.concatenate([ctx_t[:HEAD_DIM, :CHUNK], ctx_t[HEAD_DIM:, CHUNK:]], axis=0)
        ctx_ref[0, rows, :] = ctx_t.T.astype(BF16)

    @pl.when(pl.program_id(0) == 0)
    def _():
        scores(ko_ref, ks_ref, q_ref[:CHUNK, :], a_ref, ma_ref)

    scores(ko_ref, ks_ref, q_ref[CHUNK:, :], b_ref, mb_ref)
    finish(a_ref, ma_ref, 0)
    scores(kno_ref, kns_ref, qn_ref[:CHUNK, :], a_ref, ma_ref)
    finish(b_ref, mb_ref, 1)


def attn_fwd(q, kv, kv_s, layer, layers, hist):
    tq, width = q.shape
    tk = kv.shape[0]
    pairs = width // 128
    last = pairs - 1

    def col(off):
        return lambda j: (0, j + off)

    def nxt(j):
        return (0, jnp.minimum(j + 1, last))

    extra = [] if hist is None else [hist]
    flops = 2 * 2 * tq * (2 * tk) * 256 * (width // HEAD_DIM)
    return pl.pallas_call(
        attn_fwd_body,
        grid=(pairs,),
        in_specs=[pl.BlockSpec((tq, 128), col(0)), pl.BlockSpec((tq, 128), nxt),
                  pl.BlockSpec((tk, 128), col(0)), pl.BlockSpec((tk, 128), col(0)),
                  pl.BlockSpec((tk, 128), nxt), pl.BlockSpec((tk, 128), nxt),
                  pl.BlockSpec((tk, 128), col(pairs)), pl.BlockSpec((tk, 128), col(pairs))]
        + [pl.BlockSpec(memory_space=pl.ANY)] * len(extra),
        out_specs=[pl.BlockSpec((1, tq, 128), lambda j: (layer, 0, j)),
                   pl.BlockSpec((1, 2, tq), lambda j: (j, 0, 0))],
        out_shape=[jax.ShapeDtypeStruct((layers, tq, width), BF16),
                   jax.ShapeDtypeStruct((pairs, 2, tq), F32)],
        input_output_aliases={8: 0} if extra else {},
        scratch_shapes=[pltpu.VMEM((2 * tk, 2 * CHUNK), F32), pltpu.VMEM((2 * tk, 2 * CHUNK), F32),
                        pltpu.VMEM((1, 2 * CHUNK), F32), pltpu.VMEM((1, 2 * CHUNK), F32)],
        compiler_params=pltpu.CompilerParams(dimension_semantics=('arbitrary',),
                                             vmem_limit_bytes=VMEM_ALL),
        cost_estimate=pl.CostEstimate(flops=flops, bytes_accessed=2 * (tq * width * 2 + 4 * tk * width),
                                      transcendentals=tq * 2 * tk * (width // HEAD_DIM)),
        name='attn_fwd',
    )(q, q, kv, kv_s, kv, kv_s, kv, kv_s, *extra)


def attn_bwd_body(*refs):
    q_ref, ko_ref, ks_ref, vo_ref, vs_ref, do_ref, lse_ref = refs[:7]
    dq_ref, dko_ref, dks_ref, dvo_ref, dvs_ref = refs[-5:]
    tk = ko_ref.shape[0]
    k = jnp.concatenate([ko_ref[...], ks_ref[...]], axis=0)
    v = jnp.concatenate([vo_ref[...], vs_ref[...]], axis=0)
    tq = q_ref.shape[0]
    chunk = 256
    low = pair_masks(chunk)
    for i in range(tq // chunk):
        rows = slice(i * chunk, (i + 1) * chunk)
        q = q_ref[rows, :]
        do = do_ref[rows, :]
        dqs = []
        for h in range(2):
            sel = low if h == 0 else ~low
            qm = jnp.where(sel, q, jnp.zeros_like(q))
            dom = jnp.where(sel, do, jnp.zeros_like(do))
            s = nt(k, qm)
            p = jnp.exp2(s * (SCALE * LOG2E) - lse_ref[0, h:h + 1, rows])
            dp = nt(v, dom).astype(BF16).astype(F32)
            delta = jnp.sum(p * dp, axis=0, keepdims=True)
            ds = (p * (dp - delta)).astype(BF16)
            dv = nn(p.astype(BF16), dom)
            dk = nn(ds, qm) * SCALE
            if i == 0 and h == 0:
                dvo_ref[...] = dv[:tk]
                dvs_ref[...] = dv[tk:]
                dko_ref[...] = dk[:tk]
                dks_ref[...] = dk[tk:]
            else:
                dvo_ref[...] += dv[:tk]
                dvs_ref[...] += dv[tk:]
                dko_ref[...] += dk[:tk]
                dks_ref[...] += dk[tk:]
            dqs.append(tn(k, ds)[h * HEAD_DIM:(h + 1) * HEAD_DIM, :] * SCALE)
        dq_ref[0, rows, :] = jnp.concatenate(dqs, axis=0).T.astype(BF16)


def attn_bwd(q, kv, kv_s, d_ctx, lse, layer, layers, hist):
    tq, width = q.shape
    tk = kv.shape[0]
    pairs = width // 128

    def col(off):
        return lambda j: (0, j + off)

    flops = 5 * 2 * tq * (2 * tk) * 256 * (width // HEAD_DIM)
    kblk = pl.BlockSpec((tk, 128), col(0))
    extra = [] if hist is None else [hist]
    return pl.pallas_call(
        attn_bwd_body,
        grid=(pairs,),
        in_specs=[pl.BlockSpec((tq, 128), col(0)),
                  kblk, kblk,
                  pl.BlockSpec((tk, 128), col(pairs)), pl.BlockSpec((tk, 128), col(pairs)),
                  pl.BlockSpec((tq, 128), col(0)),
                  pl.BlockSpec((1, 2, tq), lambda j: (j, 0, 0))]
        + [pl.BlockSpec(memory_space=pl.ANY)] * len(extra),
        out_specs=[pl.BlockSpec((1, tq, 128), lambda j: (layer, 0, j)), kblk, kblk, kblk, kblk],
        out_shape=[jax.ShapeDtypeStruct((layers, tq, width), BF16)]
        + [jax.ShapeDtypeStruct((tk, width), F32)] * 4,
        input_output_aliases={7: 0} if extra else {},
        compiler_params=pltpu.CompilerParams(dimension_semantics=('arbitrary',),
                                             vmem_limit_bytes=VMEM_ALL),
        cost_estimate=pl.CostEstimate(flops=flops, bytes_accessed=2 * (2 * tq * width * 2 + 4 * tk * width) + 16 * tk * width,
                                      transcendentals=tq * 2 * tk * (width // HEAD_DIM)),
        name='attn_bwd',
    )(q, kv, kv_s, kv, kv_s, d_ctx, lse, *extra)


GELU_C = 0.7978845608028654
GELU_A = 0.044715
BLOCK_F = 768
SUB_F = 768
ROWS = (slice(0, 256), slice(256, 512))


def mlp_fwd_body(*refs):
    h_ref, w1_ref, w2_ref = refs[:3]
    z_ref, g_ref, x_ref, m_ref, acc_ref = refs[-5:]
    j = pl.program_id(0)

    @pl.when(j == 0)
    def _():
        hf = h_ref[...].astype(F32)
        acc_ref[...] = hf
        m_ref[0] = (hf * lax.rsqrt(jnp.mean(hf * hf, axis=-1, keepdims=True) + EPS_NORM)).astype(BF16)

    for rows in ROWS:
        z = nt(m_ref[0, rows, :], w1_ref[...]).astype(BF16)
        z_ref[rows, :] = z
        zf = z.astype(F32)
        t = jnp.tanh(zf * (GELU_C + (GELU_A * GELU_C) * (zf * zf)))
        half = 0.5 * zf
        g_ref[0, rows, :] = (half + half * t).astype(BF16)
    for rows in ROWS:
        acc_ref[rows, :] += nn(g_ref[0, rows, :], w2_ref[...])

    @pl.when(j == pl.num_programs(0) - 1)
    def _():
        x_ref[...] = acc_ref[...].astype(BF16)


def mlp_fwd(h, w1t, w2, layer, layers, hist):
    t, dim = h.shape
    hidden = w2.shape[0]
    whole = pl.BlockSpec((t, dim), lambda j: (0, 0))
    wblk = pl.BlockSpec((BLOCK_F, dim), lambda j: (j, 0))
    extra = [] if hist is None else [hist]
    return pl.pallas_call(
        mlp_fwd_body,
        grid=(hidden // BLOCK_F,),
        in_specs=[whole, wblk, wblk] + [pl.BlockSpec(memory_space=pl.ANY)] * len(extra),
        out_specs=[pl.BlockSpec((t, BLOCK_F), lambda j: (0, j)),
                   pl.BlockSpec((1, t, BLOCK_F), lambda j: (j, 0, 0)), whole,
                   pl.BlockSpec((1, t, dim), lambda j: (layer, 0, 0))],
        out_shape=[jax.ShapeDtypeStruct((t, hidden), BF16),
                   jax.ShapeDtypeStruct((hidden // BLOCK_F, t, BLOCK_F), BF16),
                   jax.ShapeDtypeStruct((t, dim), BF16),
                   jax.ShapeDtypeStruct((layers, t, dim), BF16)],
        scratch_shapes=[pltpu.VMEM((t, dim), F32)],
        input_output_aliases={3: 3} if extra else {},
        compiler_params=pltpu.CompilerParams(dimension_semantics=('arbitrary',), vmem_limit_bytes=VMEM_ALL),
        cost_estimate=pl.CostEstimate(flops=4 * t * dim * hidden, bytes_accessed=4 * dim * hidden + 4 * t * hidden,
                                      transcendentals=t * hidden),
        name='mlp_fwd',
    )(h, w1t, w2, *extra)


def mlp_bwd_body(*refs):
    d_ref, h_ref, z_ref, w1_ref, w2_ref = refs[:5]
    up_ref, mid_ref, acc_ref = refs[-3:]
    j = pl.program_id(0)

    @pl.when(j == 0)
    def _():
        acc_ref[...] = jnp.zeros_like(acc_ref)

    for i in range(0, BLOCK_F, SUB_F):
        cols = slice(i, i + SUB_F)
        for rows in ROWS:
            da = nt(d_ref[rows, :], w2_ref[cols, :]).astype(BF16).astype(F32)
            zf = z_ref[rows, cols].astype(F32)
            z2 = zf * zf
            t = jnp.tanh(zf * (GELU_C + (GELU_A * GELU_C) * z2))
            slope = (1.0 + t) * (0.5 + (1.0 - t) * (zf * (0.5 * GELU_C + (1.5 * GELU_A * GELU_C) * z2)))
            up_ref[0, rows, cols] = (da * slope).astype(BF16)
    for rows in ROWS:
        acc_ref[rows, :] += nn(up_ref[0, rows, :], w1_ref[...])

    @pl.when(j == pl.num_programs(0) - 1)
    def _():
        dn = acc_ref[...].astype(BF16).astype(F32)
        hf = h_ref[...].astype(F32)
        inv = lax.rsqrt(jnp.mean(hf * hf, axis=-1, keepdims=True) + EPS_NORM)
        proj = jnp.mean(hf * dn, axis=-1, keepdims=True)
        mid_ref[0] = (d_ref[...].astype(F32) + inv * dn - hf * (inv * inv * inv * proj)).astype(BF16)


def mlp_bwd(d_next, h, z, w1t, w2, layer, layers, hist, mid_hist):
    t, dim = h.shape
    hidden = w2.shape[0]
    whole = pl.BlockSpec((t, dim), lambda j: (0, 0))
    wblk = pl.BlockSpec((BLOCK_F, dim), lambda j: (j, 0))
    hspec = pl.BlockSpec((1, t, BLOCK_F), lambda j: (layer, 0, j))
    extra = [] if hist is None else [hist, mid_hist]
    return pl.pallas_call(
        mlp_bwd_body,
        grid=(hidden // BLOCK_F,),
        in_specs=[whole, whole, pl.BlockSpec((t, BLOCK_F), lambda j: (0, j)), wblk, wblk]
        + [pl.BlockSpec(memory_space=pl.ANY)] * len(extra),
        out_specs=[hspec, pl.BlockSpec((1, t, dim), lambda j: (layer, 0, 0))],
        out_shape=[jax.ShapeDtypeStruct((layers, t, hidden), BF16), jax.ShapeDtypeStruct((layers, t, dim), BF16)],
        scratch_shapes=[pltpu.VMEM((t, dim), F32)],
        input_output_aliases={5: 0, 6: 1} if extra else {},
        compiler_params=pltpu.CompilerParams(dimension_semantics=('arbitrary',), vmem_limit_bytes=VMEM_ALL),
        cost_estimate=pl.CostEstimate(flops=4 * t * dim * hidden, bytes_accessed=4 * dim * hidden + 4 * t * hidden,
                                      transcendentals=t * hidden),
        name='mlp_bwd',
    )(d_next, h, z, w1t, w2, *extra)


def join_body(count, core_ref, *refs):
    for n in range(count):
        own, other, out = refs[n], refs[count + n], refs[2 * count + n]
        for i, src in enumerate((own, other)):
            @pl.when(pl.program_id(0) == i)
            def _():
                out[...] = src[...]


def join_call(core, body, grid, own, other, in_specs, out_specs, out_shape):
    size = sum(v.size for v in own)
    return pl.pallas_call(
        body,
        grid_spec=pltpu.PrefetchScalarGridSpec(num_scalar_prefetch=1, grid=grid, in_specs=in_specs * 2, out_specs=out_specs),
        out_shape=out_shape,
        compiler_params=pltpu.CompilerParams(dimension_semantics=('arbitrary', 'arbitrary'), vmem_limit_bytes=VMEM_ALL),
        cost_estimate=pl.CostEstimate(flops=8 * size, bytes_accessed=16 * size, transcendentals=0),
    )(core.reshape(1), *own, *other)


def join(core, own, other, axes, parts):
    in_specs, out_specs, out_shape = [], [], []
    for v, axis in zip(own, axes):
        rows, cols = v.shape[0], v.shape[1] // parts
        in_specs.append(pl.BlockSpec((rows, cols), lambda i, j, c: (0, j)))
        if axis == 0:
            out_shape.append(jax.ShapeDtypeStruct((2 * rows, v.shape[1]), v.dtype))
            out_specs.append(pl.BlockSpec((rows, cols), lambda i, j, c: ((c[0] + i) % 2, j)))
        else:
            out_shape.append(jax.ShapeDtypeStruct((rows, 2 * v.shape[1]), v.dtype))
            out_specs.append(pl.BlockSpec((rows, cols), lambda i, j, c, parts=parts: (0, ((c[0] + i) % 2) * parts + j)))
    return join_call(core, functools.partial(join_body, len(own)), (2, parts), own, other, in_specs, out_specs, out_shape)


def join_flip_body(core_ref, oa_ref, ob_ref, sa_ref, sb_ref, out_ref):
    for i, srcs in enumerate(((oa_ref, ob_ref), (sa_ref, sb_ref))):
        for j, src in enumerate(srcs):
            @pl.when((pl.program_id(0) == i) & (pl.program_id(1) == j))
            def _():
                out_ref[...] = src[...].T


def join_flip(core, own, other):
    rows, cols = own[0].shape
    block = pl.BlockSpec((rows, cols), lambda i, j, c: (0, 0))
    return join_call(core, join_flip_body, (2, 2), own, other, [block] * 2,
                     pl.BlockSpec((cols, rows), lambda i, j, c: (j, (c[0] + i) % 2)),
                     jax.ShapeDtypeStruct((2 * cols, 2 * rows), F32))


def gather_pieces(part_a, part_b):
    xa, xb = pp_x(part_a), pp_x(part_b)
    ya, yb = pp_y(part_a), pp_y(part_b)
    da, db = pp_y(xa), pp_x(yb)
    own = [(xa, xb), (ya, yb), (da, db)]
    return own, [(pp_d(a), pp_d(b)) for a, b in own]


def own_terms(tile, first, second):
    order = (3, first, second, 0)
    sent = {r: pp_d(tile(r, 1)) for r in order}
    return {r: tile(r, 0) + sent[r] for r in order}


def reduce_terms(total, pp_first, pp_second, first, second):
    here = total[0] + pp_first(total[first])
    there = total[second] + pp_first(total[3])
    return here + pp_second(there)


BOTH = ('model', 'data')


def solution(mesh):
    spec_col = P(None, 'model')
    spec_row = P('model', None)
    spec_act = P('data', None, None)
    spec_rep = P(None, None)

    def device_step(x_in, cot_out, step_emb, w_q, w_k, w_v, w_o, w_1, w_2):
        layer_count, dim = step_emb.shape
        core = lax.axis_index('data')
        chip = lax.axis_index('model')
        chip_x = lax.rem(chip, 2)
        chip_y = lax.div(chip, 2)
        nbr_x = chip + 1 - 2 * chip_x
        nbr_y = lax.rem(chip + 2, 4)
        diag = lax.rem(nbr_x + 2, 4)
        chips = (chip, nbr_x, nbr_y, diag)
        hid = w_q.shape[1]
        half_d = dim // 2

        def take(v, which, axis, size):
            return lax.dynamic_slice_in_dim(v, which * size, size, axis)

        def put(buf, v, which, axis):
            return lax.dynamic_update_slice_in_dim(buf, v, which * v.shape[axis], axis)

        def gather(v):
            return lax.all_gather(v, BOTH, axis=0, tiled=True)

        def scatter(v):
            return lax.psum_scatter(v, BOTH, scatter_dimension=0, tiled=True)

        def after(v, *deps):
            return lax.optimization_barrier((v,) + deps)[0]

        def keep(hist, v, layer):
            if hist is None:
                hist = jnp.zeros((layer_count,) + v.shape, v.dtype)
            return lax.dynamic_update_slice(hist, v[None], (layer, 0, 0))

        def my_tokens(v):
            mine = lax.dynamic_index_in_dim(v, chip_x, 0, keepdims=False)
            half = mine.shape[0] // 2
            recv = pp_d(take(mine, 1 - core, 0, half))
            return jnp.where(core == chip_y, take(mine, core, 0, half), recv)

        def gather_permuted(local):
            own = take(local, core, 0, local.shape[0] // 2)
            rows = own.shape[0] // 2
            p_own, p_sib = gather_pieces(own[:rows], own[rows:])
            full = put(jnp.zeros((4 * local.shape[0], dim), BF16), local, chip, 0)
            for r in (1, 2, 3):
                for part in (0, 1):
                    full = put(full, p_own[r - 1][part], 4 * chips[r] + 2 * core + part, 0)
                    full = put(full, p_sib[r - 1][part], 4 * chips[r] + 2 * (1 - core) + part, 0)
            return full

        x_cur = my_tokens(x_in)
        qkv_t = jnp.concatenate([w_q, w_k, w_v], axis=1).T
        qkv_all = gather(take(qkv_t, core, 0, qkv_t.shape[0] // 2))
        o_all = gather(take(w_o, core, 0, hid // 2))
        w2 = gather_permuted(w_2)
        w1 = gather_permuted(w_1.T)
        wq, wk, wv = [jnp.concatenate([take(qkv_all, 3 * c + i, 0, hid) for c in chips], axis=0) for i in range(3)]
        wo = jnp.concatenate([take(o_all, c, 0, hid) for c in chips], axis=0)
        d_cur = my_tokens(cot_out)

        saved = []
        g_mine = []
        u_hist = m_hist = ctx_hist = None
        for layer in range(layer_count):
            s = x_cur.astype(F32) + step_emb[layer].astype(F32)
            u = rms_norm(s).astype(BF16)
            kv = jnp.concatenate([nt(u, wk).astype(BF16), nt(u, wv).astype(BF16)], axis=1)
            kv_s = pp_d(kv)
            q = nt(u, wq).astype(BF16)
            ctx_hist, lse = attn_fwd(q, kv, kv_s, layer, layer_count, ctx_hist)
            h = (s + nn(ctx_hist[layer], wo)).astype(BF16)
            z, g, x_next, m_hist = mlp_fwd(h, w1, w2, layer, layer_count, m_hist)
            g_mine.append(lax.all_to_all(g.reshape(-1, g.shape[-1]), BOTH, split_axis=0, concat_axis=0, tiled=True))
            u_hist = keep(u_hist, u, layer)
            u_hist, x_next = lax.optimization_barrier((u_hist, x_next))
            saved.append((x_cur, q, kv, kv_s, lse, h, z))
            x_cur = x_next

        def flat(v):
            return v.reshape(-1, v.shape[-1])

        up_hist = mid_hist = dq_hist = dk_hist = dv_hist = None
        next_all = [None] * layer_count
        for layer in reversed(range(layer_count)):
            x_l, q, kv, kv_s, lse, h, z = saved[layer]
            d_next = d_cur
            next_all[layer] = gather(d_next)
            up_hist, mid_hist = mlp_bwd(d_next, h, z, w1, w2, layer, layer_count, up_hist, mid_hist)
            d_mid = mid_hist[layer]
            if layer == 0:
                up_f, m_f = flat(up_hist), flat(m_hist)
                term_1a, d_mid, up_f = lax.optimization_barrier((tn(up_f, m_f[:, :half_d]), d_mid, up_f))
                grad_1a = scatter(term_1a)
                term_1b = tn(up_f, m_f[:, half_d:])
                term_1b, d_mid = lax.optimization_barrier((term_1b, d_mid))
                grad_1b = scatter(term_1b)
            d_ctx = nt(d_mid, wo).astype(BF16)
            dq_hist, dko, dks, dvo, dvs = attn_bwd(q, kv, kv_s, d_ctx, lse, layer, layer_count, dq_hist)
            dk = (dko + pp_d(dks)).astype(BF16)
            dv = (dvo + pp_d(dvs)).astype(BF16)
            dk_hist, dv_hist = keep(dk_hist, dk, layer), keep(dv_hist, dv, layer)
            d_norm1 = (nn(dq_hist[layer], wq) + nn(dk, wk) + nn(dv, wv)).astype(BF16)
            s = x_l.astype(F32) + step_emb[layer].astype(F32)
            norm_pull_x = jax.vjp(rms_norm, s)[1]
            d_cur = (d_mid.astype(F32) + norm_pull_x(d_norm1.astype(F32))[0]).astype(BF16)
            if layer > 0:
                d_cur, dk_hist, dv_hist = lax.optimization_barrier((d_cur, dk_hist, dv_hist))

        mid_half = [lax.optimization_barrier(take(flat(mid_hist), w, 1, half_d)) for w in (core, 1 - core)]
        u_half = [lax.optimization_barrier(take(flat(u_hist), w, 1, half_d)) for w in (core, 1 - core)]

        def cols(v, r):
            return flat(v)[:, r * hid:(r + 1) * hid]

        t_o = own_terms(lambda r, half: tn(cols(ctx_hist, r), mid_half[half]), 2, 1)
        t_q = own_terms(lambda r, half: tn(u_half[half], cols(dq_hist, r)), 1, 2)
        t_k = own_terms(lambda r, half: tn(u_half[half], cols(dk_hist, r)), 1, 2)
        t_v = own_terms(lambda r, half: tn(u_half[half], cols(dv_hist, r)), 2, 1)
        own_o = reduce_terms(t_o, pp_y, pp_x, 2, 1)
        own_q = reduce_terms(t_q, pp_x, pp_y, 1, 2)
        own_k = reduce_terms(t_k, pp_x, pp_y, 1, 2)
        own_v = reduce_terms(t_v, pp_y, pp_x, 2, 1)

        def ordered(own, sib, axis):
            size = own.shape[axis]
            shape = own.shape[:axis] + (2 * size,) + own.shape[axis + 1:]
            return put(put(jnp.zeros(shape, own.dtype), own, core, axis), sib, 1 - core, axis)

        other_half = pp_d(d_cur)
        whole = ordered(d_cur, other_half, 0)
        to_row = [(2 * c + d, 2 * (c ^ 2) + d) for c in range(4) for d in range(2) if c // 2 == d]
        from_y = lax.ppermute(whole, BOTH, to_row)
        row_seq = jnp.where(chip_y == core, whole, from_y)
        from_x = pp_x(row_seq)
        d_x = jnp.zeros((2,) + whole.shape, BF16)
        d_x = put(put(d_x, row_seq[None], chip_x, 0), from_x[None], 1 - chip_x, 0)

        ready = tuple(t[r] for t in (t_o, t_q, t_k, t_v) for r in (1, 2, 3))
        grad_2 = None
        for layer in reversed(range(layer_count)):
            term = tn(after(g_mine[layer], *ready), next_all[layer])
            grad_2 = term if grad_2 is None else grad_2 + term

        (grad_2,) = join(core, [grad_2], [pp_d(grad_2)], (0,), 4)
        grad_1 = join_flip(core, [grad_1a, grad_1b], [pp_d(grad_1a), pp_d(grad_1b)])
        own = [own_q, own_k, own_v, own_o]
        gq, gk, gv, go = join(core, own, [pp_d(v) for v in own], (0, 0, 0, 1), 1)
        return gq, gk, gv, go, grad_1, grad_2, d_x

    return jax.shard_map(device_step, mesh=mesh,
                         in_specs=(spec_act, spec_act, spec_rep, spec_col, spec_col, spec_col, spec_row, spec_col, spec_row),
                         out_specs=(spec_col, spec_col, spec_col, spec_row, spec_col, spec_row, spec_act),
                         check_vma=False)
```

```python
import functools

import jax
import jax.numpy as jnp
from jax import lax
from jax.experimental import pallas as pl
from jax.experimental.pallas import tpu as pltpu
from jax.sharding import PartitionSpec as P


HEAD_DIM = 64
EPS_NORM = 1e-6
F32 = jnp.float32
BF16 = jnp.bfloat16
LOG2E = 1.4426950408889634
VMEM_ALL = 60 * 1024 * 1024
SCALE = HEAD_DIM ** -0.5

SWAP_D = [(0, 1), (1, 0)]


SWAP_X = [(0, 1), (1, 0), (2, 3), (3, 2)]
SWAP_Y = [(0, 2), (2, 0), (1, 3), (3, 1)]


def pp_x(v):
    return lax.ppermute(v, 'model', SWAP_X)


def pp_y(v):
    return lax.ppermute(v, 'model', SWAP_Y)


def pp_d(v):
    return lax.ppermute(v, 'data', SWAP_D)


def dot(a, b, dims):
    return lax.dot_general(a, b, (dims, ((), ())), preferred_element_type=F32)


def nn(a, b):
    return dot(a, b, ((1,), (0,)))


def nt(a, b):
    return dot(a, b, ((1,), (1,)))


def tn(a, b):
    return dot(a, b, ((0,), (0,)))


def pair_masks(rows):
    lane = lax.broadcasted_iota(jnp.int32, (rows, 128), 1)
    return lane < HEAD_DIM


CHUNK = 256


def masked_pair(q):
    low = pair_masks(CHUNK)
    zero = jnp.zeros_like(q)
    return jnp.concatenate([jnp.where(low, q, zero), jnp.where(low, zero, q)], axis=0)


def attn_fwd_body(*refs):
    q_ref, qn_ref, ko_ref, ks_ref, kno_ref, kns_ref, vo_ref, vs_ref = refs[:8]
    ctx_ref, lse_ref, a_ref, b_ref, ma_ref, mb_ref = refs[-6:]

    def scores(ko, ks, q, s_ref, m_ref):
        s = nt(jnp.concatenate([ko[...], ks[...]], axis=0), masked_pair(q))
        s_ref[...] = s
        m_ref[...] = jnp.max(s, axis=0, keepdims=True)

    def finish(s_ref, m_ref, i):
        rows = slice(i * CHUNK, (i + 1) * CHUNK)
        m = m_ref[...]
        p = jnp.exp2((s_ref[...] - m) * (SCALE * LOG2E))
        l = jnp.sum(p, axis=0, keepdims=True)
        pb = (p * (1.0 / l)).astype(BF16)
        lse = m * (SCALE * LOG2E) + jnp.log2(l)
        lse_ref[0, 0:1, rows] = lse[:, :CHUNK]
        lse_ref[0, 1:2, rows] = lse[:, CHUNK:]
        ctx_t = tn(jnp.concatenate([vo_ref[...], vs_ref[...]], axis=0), pb)
        ctx_t = jnp.concatenate([ctx_t[:HEAD_DIM, :CHUNK], ctx_t[HEAD_DIM:, CHUNK:]], axis=0)
        ctx_ref[0, rows, :] = ctx_t.T.astype(BF16)

    @pl.when(pl.program_id(0) == 0)
    def _():
        scores(ko_ref, ks_ref, q_ref[:CHUNK, :], a_ref, ma_ref)

    scores(ko_ref, ks_ref, q_ref[CHUNK:, :], b_ref, mb_ref)
    finish(a_ref, ma_ref, 0)
    scores(kno_ref, kns_ref, qn_ref[:CHUNK, :], a_ref, ma_ref)
    finish(b_ref, mb_ref, 1)


def attn_fwd(q, kv, kv_s, layer, layers, hist):
    tq, width = q.shape
    tk = kv.shape[0]
    pairs = width // 128
    last = pairs - 1

    def col(off):
        return lambda j: (0, j + off)

    def nxt(j):
        return (0, jnp.minimum(j + 1, last))

    extra = [] if hist is None else [hist]
    flops = 2 * 2 * tq * (2 * tk) * 256 * (width // HEAD_DIM)
    return pl.pallas_call(
        attn_fwd_body,
        grid=(pairs,),
        in_specs=[pl.BlockSpec((tq, 128), col(0)), pl.BlockSpec((tq, 128), nxt),
                  pl.BlockSpec((tk, 128), col(0)), pl.BlockSpec((tk, 128), col(0)),
                  pl.BlockSpec((tk, 128), nxt), pl.BlockSpec((tk, 128), nxt),
                  pl.BlockSpec((tk, 128), col(pairs)), pl.BlockSpec((tk, 128), col(pairs))]
        + [pl.BlockSpec(memory_space=pl.ANY)] * len(extra),
        out_specs=[pl.BlockSpec((1, tq, 128), lambda j: (layer, 0, j)),
                   pl.BlockSpec((1, 2, tq), lambda j: (j, 0, 0))],
        out_shape=[jax.ShapeDtypeStruct((layers, tq, width), BF16),
                   jax.ShapeDtypeStruct((pairs, 2, tq), F32)],
        input_output_aliases={8: 0} if extra else {},
        scratch_shapes=[pltpu.VMEM((2 * tk, 2 * CHUNK), F32), pltpu.VMEM((2 * tk, 2 * CHUNK), F32),
                        pltpu.VMEM((1, 2 * CHUNK), F32), pltpu.VMEM((1, 2 * CHUNK), F32)],
        compiler_params=pltpu.CompilerParams(dimension_semantics=('arbitrary',),
                                             vmem_limit_bytes=VMEM_ALL),
        cost_estimate=pl.CostEstimate(flops=flops, bytes_accessed=2 * (tq * width * 2 + 4 * tk * width),
                                      transcendentals=tq * 2 * tk * (width // HEAD_DIM)),
        name='attn_fwd',
    )(q, q, kv, kv_s, kv, kv_s, kv, kv_s, *extra)


def attn_bwd_body(*refs):
    q_ref, ko_ref, ks_ref, vo_ref, vs_ref, do_ref, lse_ref = refs[:7]
    dq_ref, down_ref, dsib_ref = refs[-3:]
    tk = ko_ref.shape[0]
    k = jnp.concatenate([ko_ref[...], ks_ref[...]], axis=0)
    v = jnp.concatenate([vo_ref[...], vs_ref[...]], axis=0)
    low = pair_masks(CHUNK)
    for i in range(q_ref.shape[0] // CHUNK):
        rows = slice(i * CHUNK, (i + 1) * CHUNK)
        q = q_ref[rows, :]
        do = do_ref[rows, :]
        dqs = []
        for h in range(2):
            sel = low if h == 0 else ~low
            qm = jnp.where(sel, q, jnp.zeros_like(q))
            dom = jnp.where(sel, do, jnp.zeros_like(do))
            s = nt(k, qm)
            p = jnp.exp2(s * (SCALE * LOG2E) - lse_ref[0, h:h + 1, rows])
            dp = nt(v, dom).astype(BF16).astype(F32)
            delta = jnp.sum(p * dp, axis=0, keepdims=True)
            ds = (p * (dp - delta)).astype(BF16)
            dv = nn(p.astype(BF16), dom)
            dk = nn(ds, qm) * SCALE
            for n, grad in enumerate((dk, dv)):
                for ref, part in ((down_ref, grad[:tk]), (dsib_ref, grad[tk:])):
                    if i == 0 and h == 0:
                        ref[n] = part
                    else:
                        ref[n] += part
            dqs.append(tn(k, ds)[h * HEAD_DIM:(h + 1) * HEAD_DIM, :] * SCALE)
        dq_ref[0, rows, :] = jnp.concatenate(dqs, axis=0).T.astype(BF16)


def attn_bwd(q, kv, kv_s, d_ctx, lse, layer, layers, hist):
    tq, width = q.shape
    tk = kv.shape[0]
    pairs = width // 128

    def col(off):
        return lambda j: (0, j + off)

    flops = 5 * 2 * tq * (2 * tk) * 256 * (width // HEAD_DIM)
    kblk = pl.BlockSpec((tk, 128), col(0))
    both = pl.BlockSpec((2, tk, 128), lambda j: (0, 0, j))
    extra = [] if hist is None else [hist]
    return pl.pallas_call(
        attn_bwd_body,
        grid=(pairs,),
        in_specs=[pl.BlockSpec((tq, 128), col(0)),
                  kblk, kblk,
                  pl.BlockSpec((tk, 128), col(pairs)), pl.BlockSpec((tk, 128), col(pairs)),
                  pl.BlockSpec((tq, 128), col(0)),
                  pl.BlockSpec((1, 2, tq), lambda j: (j, 0, 0))]
        + [pl.BlockSpec(memory_space=pl.ANY)] * len(extra),
        out_specs=[pl.BlockSpec((1, tq, 128), lambda j: (layer, 0, j)), both, both],
        out_shape=[jax.ShapeDtypeStruct((layers, tq, width), BF16)]
        + [jax.ShapeDtypeStruct((2, tk, width), F32)] * 2,
        input_output_aliases={7: 0} if extra else {},
        compiler_params=pltpu.CompilerParams(dimension_semantics=('arbitrary',),
                                             vmem_limit_bytes=VMEM_ALL),
        cost_estimate=pl.CostEstimate(flops=flops, bytes_accessed=2 * (2 * tq * width * 2 + 4 * tk * width) + 16 * tk * width,
                                      transcendentals=tq * 2 * tk * (width // HEAD_DIM)),
        name='attn_bwd',
    )(q, kv, kv_s, kv, kv_s, d_ctx, lse, *extra)


def kv_body(*refs):
    x_ref, e_ref, w_ref = refs[:3]
    kv_ref, u_ref = refs[-2:]

    @pl.when(pl.program_id(0) == 0)
    def _():
        s = x_ref[...].astype(F32) + e_ref[...]
        u_ref[0] = (s * lax.rsqrt(jnp.mean(s * s, axis=-1, keepdims=True) + EPS_NORM)).astype(BF16)

    for rows in ROWS:
        kv_ref[rows, :] = nt(u_ref[0, rows, :], w_ref[...]).astype(BF16)


def norm_kv(x, e, wkv, layer, layers, hist):
    t, dim = x.shape
    width = wkv.shape[0]
    blk = 1024
    extra = [] if hist is None else [hist]
    return pl.pallas_call(
        kv_body,
        grid=(width // blk,),
        in_specs=[pl.BlockSpec((t, dim), lambda j: (0, 0)), pl.BlockSpec((1, dim), lambda j: (0, 0)),
                  pl.BlockSpec((blk, dim), lambda j: (j, 0))] + [pl.BlockSpec(memory_space=pl.ANY)] * len(extra),
        out_specs=[pl.BlockSpec((t, blk), lambda j: (0, j)), pl.BlockSpec((1, t, dim), lambda j: (layer, 0, 0))],
        out_shape=[jax.ShapeDtypeStruct((t, width), BF16), jax.ShapeDtypeStruct((layers, t, dim), BF16)],
        input_output_aliases={3: 1} if extra else {},
        compiler_params=pltpu.CompilerParams(dimension_semantics=('arbitrary',), vmem_limit_bytes=VMEM_ALL),
        cost_estimate=pl.CostEstimate(flops=2 * t * dim * width, bytes_accessed=2 * (dim * width + t * width + 2 * t * dim),
                                      transcendentals=t),
        name='norm_kv',
    )(x, e, wkv, *extra)


def d_kv_body(*refs):
    acc0_ref, x_ref, e_ref, mid_ref, own_ref, recv_ref, w_ref = refs[:7]
    dk_ref, dv_ref, prev_ref, acc_ref = refs[-4:]
    j = pl.program_id(0)

    @pl.when(j == 0)
    def _():
        acc_ref[...] = acc0_ref[...]

    grad = (own_ref[0] + recv_ref[0]).astype(BF16)
    half = grad.shape[1]
    for n, ref in enumerate((dk_ref, dv_ref)):
        for part in range(2):
            @pl.when(j == 2 * n + part)
            def _():
                ref[0, :, part * half:(part + 1) * half] = grad

    for rows in ROWS:
        acc_ref[rows, :] += nn(grad[rows, :], w_ref[...])

    @pl.when(j == pl.num_programs(0) - 1)
    def _():
        dn = acc_ref[...].astype(BF16).astype(F32)
        s = x_ref[...].astype(F32) + e_ref[...]
        inv = lax.rsqrt(jnp.mean(s * s, axis=-1, keepdims=True) + EPS_NORM)
        proj = jnp.mean(s * dn, axis=-1, keepdims=True)
        prev_ref[...] = (mid_ref[0].astype(F32) + inv * dn - s * (inv * inv * inv * proj)).astype(BF16)


def d_kv(acc0, x, e, mid_hist, own, recv, wkv, layer, layers, dk_hist, dv_hist):
    t, dim = x.shape
    half = dim // 2
    whole = pl.BlockSpec((t, dim), lambda j: (0, 0))
    slab = pl.BlockSpec((1, t, dim), lambda j: (layer, 0, 0))
    gblk = pl.BlockSpec((1, t, half), lambda j: (j // 2, 0, j % 2))
    extra = [] if dk_hist is None else [dk_hist, dv_hist]
    return pl.pallas_call(
        d_kv_body,
        grid=(4,),
        in_specs=[whole, whole, pl.BlockSpec((1, dim), lambda j: (0, 0)), slab, gblk, gblk,
                  pl.BlockSpec((half, dim), lambda j: (j, 0))] + [pl.BlockSpec(memory_space=pl.ANY)] * len(extra),
        out_specs=[slab, slab, whole],
        out_shape=[jax.ShapeDtypeStruct((layers, t, dim), BF16)] * 2 + [jax.ShapeDtypeStruct((t, dim), BF16)],
        scratch_shapes=[pltpu.VMEM((t, dim), F32)],
        input_output_aliases={7: 0, 8: 1} if extra else {},
        compiler_params=pltpu.CompilerParams(dimension_semantics=('arbitrary',), vmem_limit_bytes=VMEM_ALL),
        cost_estimate=pl.CostEstimate(flops=4 * t * dim * dim, bytes_accessed=4 * dim * dim + 20 * t * dim, transcendentals=t),
        name='d_kv',
    )(acc0, x, e, mid_hist, own, recv, wkv, *extra)


def terms_body(added, *refs):
    lhs, rhs, recv, outs = refs[:4], (refs[4], refs[4], refs[4], refs[5]), refs[6:6 + 4 * added], refs[-4:]
    r, kind = pl.program_id(0), pl.program_id(1)
    for n in range(4):
        @pl.when(kind == n)
        def _():
            val = tn(lhs[n][...], rhs[n][...])
            for c in range(2):
                @pl.when(r == c)
                def _():
                    slot = 2 * c + n // 2
                    outs[slot][0] = val + recv[slot][0] if added else val


def terms(dq, dk, dv, ctx, u_half, mid_half, chips, recv):
    tokens, dim = dq.shape
    hid = dim // 4
    half_d = u_half.shape[1]
    first, second = chips
    whole = pl.BlockSpec((tokens, half_d), lambda r, kind: (0, 0))
    src = pl.BlockSpec((tokens, hid), lambda r, kind: (0, first + r * (second - first)))
    slots = [pl.BlockSpec((1, hid, half_d), lambda r, kind, at=2 * n: (jnp.clip(4 * r + kind - at, 0, 1), 0, 0))
             for n in range(4)]
    out = pl.pallas_call(
        functools.partial(terms_body, len(recv) // 4),
        grid=(2, 4),
        in_specs=[src] * 4 + [whole] * 2 + slots[:len(recv)],
        out_specs=slots,
        out_shape=[jax.ShapeDtypeStruct((2, hid, half_d), F32)] * 4,
        compiler_params=pltpu.CompilerParams(dimension_semantics=('arbitrary', 'arbitrary'), vmem_limit_bytes=VMEM_ALL),
        cost_estimate=pl.CostEstimate(flops=16 * tokens * hid * half_d, bytes_accessed=24 * tokens * hid, transcendentals=0),
    )(dq, dk, dv, ctx, u_half, mid_half, *recv)
    return {first: out[:2], second: out[2:]}


GELU_C = 0.7978845608028654
GELU_A = 0.044715
BLOCK_F = 768
ROWS = (slice(0, 256), slice(256, 512))


def mlp_fwd_body(*refs):
    x0_ref, e_ref, ctx_ref, wo_ref, w1_ref, w2_ref = refs[:6]
    z_ref, g_ref, x_ref, h_ref, m_ref, acc_ref = refs[-6:]
    j = pl.program_id(0)

    @pl.when(j == 0)
    def _():
        for rows in ROWS:
            s = x0_ref[rows, :].astype(F32) + e_ref[...]
            h = (s + nn(ctx_ref[0, rows, :], wo_ref[...])).astype(BF16)
            h_ref[rows, :] = h
            hf = h.astype(F32)
            acc_ref[rows, :] = hf
            m_ref[0, rows, :] = (hf * lax.rsqrt(jnp.mean(hf * hf, axis=-1, keepdims=True) + EPS_NORM)).astype(BF16)

    for rows in ROWS:
        z = nt(m_ref[0, rows, :], w1_ref[...]).astype(BF16)
        z_ref[rows, :] = z
        zf = z.astype(F32)
        t = jnp.tanh(zf * (GELU_C + (GELU_A * GELU_C) * (zf * zf)))
        half = 0.5 * zf
        g_ref[0, rows, :] = (half + half * t).astype(BF16)
    for rows in ROWS:
        acc_ref[rows, :] += nn(g_ref[0, rows, :], w2_ref[...])

    @pl.when(j == pl.num_programs(0) - 1)
    def _():
        x_ref[...] = acc_ref[...].astype(BF16)


def mlp_fwd(x, e, ctx_hist, wo, w1t, w2, layer, layers, hist):
    t, dim = x.shape
    hidden = w2.shape[0]
    whole = pl.BlockSpec((t, dim), lambda j: (0, 0))
    slab = pl.BlockSpec((1, t, dim), lambda j: (layer, 0, 0))
    wblk = pl.BlockSpec((BLOCK_F, dim), lambda j: (j, 0))
    extra = [] if hist is None else [hist]
    return pl.pallas_call(
        mlp_fwd_body,
        grid=(hidden // BLOCK_F,),
        in_specs=[whole, pl.BlockSpec((1, dim), lambda j: (0, 0)), slab, pl.BlockSpec((dim, dim), lambda j: (0, 0)), wblk, wblk]
        + [pl.BlockSpec(memory_space=pl.ANY)] * len(extra),
        out_specs=[pl.BlockSpec((t, BLOCK_F), lambda j: (0, j)),
                   pl.BlockSpec((1, t, BLOCK_F), lambda j: (j, 0, 0)), whole, whole, slab],
        out_shape=[jax.ShapeDtypeStruct((t, hidden), BF16),
                   jax.ShapeDtypeStruct((hidden // BLOCK_F, t, BLOCK_F), BF16),
                   jax.ShapeDtypeStruct((t, dim), BF16), jax.ShapeDtypeStruct((t, dim), BF16),
                   jax.ShapeDtypeStruct((layers, t, dim), BF16)],
        scratch_shapes=[pltpu.VMEM((t, dim), F32)],
        input_output_aliases={6: 4} if extra else {},
        compiler_params=pltpu.CompilerParams(dimension_semantics=('arbitrary',), vmem_limit_bytes=VMEM_ALL),
        cost_estimate=pl.CostEstimate(flops=4 * t * dim * hidden, bytes_accessed=4 * dim * hidden + 4 * t * hidden,
                                      transcendentals=t * hidden),
        name='mlp_fwd',
    )(x, e, ctx_hist, wo, w1t, w2, *extra)


BLOCK_B = 1024
SUB_B = 512


def mlp_bwd_body(*refs):
    d_ref, h_ref, z_ref, wo_ref, w1_ref, w2_ref = refs[:6]
    up_ref, mid_ref, dctx_ref, acc_ref = refs[-4:]
    j = pl.program_id(0)

    @pl.when(j == 0)
    def _():
        acc_ref[...] = jnp.zeros_like(acc_ref)

    for i in range(0, BLOCK_B, SUB_B):
        cols = slice(i, i + SUB_B)
        for rows in ROWS:
            da = nt(d_ref[rows, :], w2_ref[cols, :]).astype(BF16).astype(F32)
            zf = z_ref[rows, cols].astype(F32)
            z2 = zf * zf
            t = jnp.tanh(zf * (GELU_C + (GELU_A * GELU_C) * z2))
            slope = (1.0 + t) * (0.5 + (1.0 - t) * (zf * (0.5 * GELU_C + (1.5 * GELU_A * GELU_C) * z2)))
            up_ref[0, rows, cols] = (da * slope).astype(BF16)
    for rows in ROWS:
        acc_ref[rows, :] += nn(up_ref[0, rows, :], w1_ref[...])

    @pl.when(j == pl.num_programs(0) - 1)
    def _():
        for rows in ROWS:
            dn = acc_ref[rows, :].astype(BF16).astype(F32)
            hf = h_ref[rows, :].astype(F32)
            inv = lax.rsqrt(jnp.mean(hf * hf, axis=-1, keepdims=True) + EPS_NORM)
            proj = jnp.mean(hf * dn, axis=-1, keepdims=True)
            mid = (d_ref[rows, :].astype(F32) + inv * dn - hf * (inv * inv * inv * proj)).astype(BF16)
            mid_ref[0, rows, :] = mid
            dctx_ref[rows, :] = nt(mid, wo_ref[...]).astype(BF16)


def mlp_bwd(d_next, h, z, wo, w1t, w2, layer, layers, hist, mid_hist):
    t, dim = h.shape
    hidden = w2.shape[0]
    whole = pl.BlockSpec((t, dim), lambda j: (0, 0))
    wblk = pl.BlockSpec((BLOCK_B, dim), lambda j: (j, 0))
    extra = [] if hist is None else [hist, mid_hist]
    return pl.pallas_call(
        mlp_bwd_body,
        grid=(hidden // BLOCK_B,),
        in_specs=[whole, whole, pl.BlockSpec((t, BLOCK_B), lambda j: (0, j)), pl.BlockSpec((dim, dim), lambda j: (0, 0)), wblk, wblk]
        + [pl.BlockSpec(memory_space=pl.ANY)] * len(extra),
        out_specs=[pl.BlockSpec((1, t, BLOCK_B), lambda j: (layer, 0, j)), pl.BlockSpec((1, t, dim), lambda j: (layer, 0, 0)), whole],
        out_shape=[jax.ShapeDtypeStruct((layers, t, hidden), BF16), jax.ShapeDtypeStruct((layers, t, dim), BF16),
                   jax.ShapeDtypeStruct((t, dim), BF16)],
        scratch_shapes=[pltpu.VMEM((t, dim), F32)],
        input_output_aliases={6: 0, 7: 1} if extra else {},
        compiler_params=pltpu.CompilerParams(dimension_semantics=('arbitrary',), vmem_limit_bytes=VMEM_ALL),
        cost_estimate=pl.CostEstimate(flops=4 * t * dim * hidden, bytes_accessed=4 * dim * hidden + 4 * t * hidden,
                                      transcendentals=t * hidden),
        name='mlp_bwd',
    )(d_next, h, z, wo, w1t, w2, *extra)


def join_body(count, core_ref, *refs):
    for n in range(count):
        own, other, out = refs[n], refs[count + n], refs[2 * count + n]
        for i, src in enumerate((own, other)):
            @pl.when(pl.program_id(0) == i)
            def _():
                out[...] = src[...]


def join_call(core, body, grid, own, other, in_specs, out_specs, out_shape):
    size = sum(v.size for v in own)
    return pl.pallas_call(
        body,
        grid_spec=pltpu.PrefetchScalarGridSpec(num_scalar_prefetch=1, grid=grid, in_specs=in_specs * 2, out_specs=out_specs),
        out_shape=out_shape,
        compiler_params=pltpu.CompilerParams(dimension_semantics=('arbitrary', 'arbitrary'), vmem_limit_bytes=VMEM_ALL),
        cost_estimate=pl.CostEstimate(flops=8 * size, bytes_accessed=16 * size, transcendentals=0),
    )(core.reshape(1), *own, *other)


def join(core, own, other):
    rows, cols = own.shape[0], own.shape[1] // 4
    block = pl.BlockSpec((rows, cols), lambda i, j, c: (0, j))
    return join_call(core, functools.partial(join_body, 1), (2, 4), [own], [other], [block],
                     pl.BlockSpec((rows, cols), lambda i, j, c: ((c[0] + i) % 2, j)),
                     jax.ShapeDtypeStruct((2 * rows, own.shape[1]), F32))


def join_attn_body(core_ref, own_a, own_b, sib_a, sib_b, q_ref, k_ref, v_ref, o_ref):
    for i, (a_ref, b_ref) in enumerate(((own_a, own_b), (sib_a, sib_b))):
        @pl.when(pl.program_id(0) == i)
        def _():
            q_ref[...] = a_ref[0].T
            k_ref[...] = a_ref[1].T
            v_ref[...] = b_ref[0].T
            o_ref[...] = b_ref[1]


def join_attn(core, own, other):
    _, hid, half_d = own[0].shape
    block = pl.BlockSpec((2, hid, half_d), lambda i, j, c: (0, 0, 0))
    tall = pl.BlockSpec((half_d, hid), lambda i, j, c: ((c[0] + i) % 2, 0))
    wide = pl.BlockSpec((hid, half_d), lambda i, j, c: (0, (c[0] + i) % 2))
    return join_call(core, join_attn_body, (2, 1), list(own), list(other), [block] * 2, [tall] * 3 + [wide],
                     [jax.ShapeDtypeStruct((2 * half_d, hid), F32)] * 3 + [jax.ShapeDtypeStruct((hid, 2 * half_d), F32)])


def join_flip_body(core_ref, oa_ref, ob_ref, sa_ref, sb_ref, out_ref):
    for i, srcs in enumerate(((oa_ref, ob_ref), (sa_ref, sb_ref))):
        for j, src in enumerate(srcs):
            @pl.when((pl.program_id(0) == i) & (pl.program_id(1) == j))
            def _():
                out_ref[...] = src[...].T


def join_flip(core, own, other):
    rows, cols = own[0].shape
    block = pl.BlockSpec((rows, cols), lambda i, j, c: (0, 0))
    return join_call(core, join_flip_body, (2, 2), own, other, [block] * 2,
                     pl.BlockSpec((cols, rows), lambda i, j, c: (j, (c[0] + i) % 2)),
                     jax.ShapeDtypeStruct((2 * cols, 2 * rows), F32))


def gather_pieces(part_a, part_b):
    xa, xb = pp_x(part_a), pp_x(part_b)
    ya, yb = pp_y(part_a), pp_y(part_b)
    da, db = pp_y(xa), pp_x(yb)
    own = [(xa, xb), (ya, yb), (da, db)]
    return own, [(pp_d(a), pp_d(b)) for a, b in own]


def reduce_terms(total, pp_first, pp_second, first, second):
    here, there = pp_first(total[first]), pp_first(total[3])
    last = pp_second(total[second] + there)
    return total[0] + here + last


BOTH = ('model', 'data')


def solution(mesh):
    spec_col = P(None, 'model')
    spec_row = P('model', None)
    spec_act = P('data', None, None)
    spec_rep = P(None, None)

    def device_step(x_in, cot_out, step_emb, w_q, w_k, w_v, w_o, w_1, w_2):
        layer_count, dim = step_emb.shape
        core = lax.axis_index('data')
        chip = lax.axis_index('model')
        chip_x = lax.rem(chip, 2)
        chip_y = lax.div(chip, 2)
        nbr_x = chip + 1 - 2 * chip_x
        nbr_y = lax.rem(chip + 2, 4)
        diag = lax.rem(nbr_x + 2, 4)
        chips = (chip, nbr_x, nbr_y, diag)
        hid = w_q.shape[1]
        half_d = dim // 2

        def take(v, which, axis, size):
            return lax.dynamic_slice_in_dim(v, which * size, size, axis)

        def put(buf, v, which, axis):
            return lax.dynamic_update_slice_in_dim(buf, v, which * v.shape[axis], axis)

        def gather(v):
            return lax.all_gather(v, BOTH, axis=0, tiled=True)

        def scatter(v):
            return lax.psum_scatter(v, BOTH, scatter_dimension=0, tiled=True)

        def after(v, *deps):
            return lax.optimization_barrier((v,) + deps)[0]

        def my_tokens(v):
            mine = lax.dynamic_index_in_dim(v, chip_x, 0, keepdims=False)
            half = mine.shape[0] // 2
            recv = pp_d(take(mine, 1 - core, 0, half))
            return jnp.where(core == chip_y, take(mine, core, 0, half), recv)

        def gather_permuted(local):
            own = take(local, core, 0, local.shape[0] // 2)
            rows = own.shape[0] // 2
            p_own, p_sib = gather_pieces(own[:rows], own[rows:])
            full = put(jnp.zeros((4 * local.shape[0], dim), BF16), local, chip, 0)
            for r in (1, 2, 3):
                for part in (0, 1):
                    full = put(full, p_own[r - 1][part], 4 * chips[r] + 2 * core + part, 0)
                    full = put(full, p_sib[r - 1][part], 4 * chips[r] + 2 * (1 - core) + part, 0)
            return full

        x_cur = my_tokens(x_in)
        qkv_t = jnp.concatenate([w_q, w_k, w_v], axis=1).T
        qkv_all = gather(take(qkv_t, core, 0, qkv_t.shape[0] // 2))
        o_all = gather(take(w_o, core, 0, hid // 2))
        w2 = gather_permuted(w_2)
        w1 = gather_permuted(w_1.T)
        wq = jnp.concatenate([take(qkv_all, 3 * c, 0, hid) for c in chips], axis=0)
        wkv = jnp.concatenate([take(qkv_all, 3 * c + i, 0, hid) for i in (1, 2) for c in chips], axis=0)
        wo = jnp.concatenate([take(o_all, c, 0, hid) for c in chips], axis=0)
        d_cur = my_tokens(cot_out)
        emb = step_emb.astype(F32)

        saved = []
        g_mine = []
        u_hist = m_hist = ctx_hist = None
        for layer in range(layer_count):
            e = emb[layer:layer + 1]
            kv, u_hist = norm_kv(x_cur, e, wkv, layer, layer_count, u_hist)
            kv_s = pp_d(kv)
            q = nt(u_hist[layer], wq).astype(BF16)
            ctx_hist, lse = attn_fwd(q, kv, kv_s, layer, layer_count, ctx_hist)
            z, g, x_next, h, m_hist = mlp_fwd(x_cur, e, ctx_hist, wo, w1, w2, layer, layer_count, m_hist)
            g_mine.append(lax.all_to_all(g.reshape(-1, g.shape[-1]), BOTH, split_axis=0, concat_axis=0, tiled=True))
            saved.append((x_cur, q, kv, kv_s, lse, h, z))
            x_cur = x_next

        def flat(v):
            return v.reshape(-1, v.shape[-1])

        up_hist = mid_hist = dq_hist = dk_hist = dv_hist = None
        next_all = [None] * layer_count
        for layer in reversed(range(layer_count)):
            x_l, q, kv, kv_s, lse, h, z = saved[layer]
            e = emb[layer:layer + 1]
            d_next = d_cur
            if layer < layer_count - 1:
                next_all[layer] = gather(d_next)
            up_hist, mid_hist, d_ctx = mlp_bwd(d_next, h, z, wo, w1, w2, layer, layer_count, up_hist, mid_hist)
            if layer == 0:
                up_f, m_f = flat(up_hist), flat(m_hist)
                term_1a, d_ctx, up_f = lax.optimization_barrier((tn(up_f, m_f[:, :half_d]), d_ctx, up_f))
                grad_1a = scatter(term_1a)
                term_1b = tn(up_f, m_f[:, half_d:])
                term_1b, d_ctx = lax.optimization_barrier((term_1b, d_ctx))
                grad_1b = scatter(term_1b)
            dq_hist, own_kv, sib_kv = attn_bwd(q, kv, kv_s, d_ctx, lse, layer, layer_count, dq_hist)
            recv_kv = pp_d(sib_kv)
            acc0 = nn(dq_hist[layer], wq)
            dk_hist, dv_hist, d_cur = d_kv(acc0, x_l, e, mid_hist, own_kv, recv_kv, wkv, layer, layer_count, dk_hist, dv_hist)

        mid_half = [lax.optimization_barrier(take(flat(mid_hist), w, 1, half_d)) for w in (core, 1 - core)]
        u_half = [lax.optimization_barrier(take(flat(u_hist), w, 1, half_d)) for w in (core, 1 - core)]
        lhs = [flat(v) for v in (dq_hist, dk_hist, dv_hist, ctx_hist)]
        sent = {}
        for pair in ((3, 1), (2, 0)):
            for r, ab in terms(*lhs, u_half[1], mid_half[1], pair, []).items():
                sent[r] = [pp_d(v) for v in ab]
        total = {}
        for pair in ((3, 1), (2, 0)):
            total.update(terms(*lhs, u_half[0], mid_half[0], pair, sent[pair[0]] + sent[pair[1]]))
        own_qk = reduce_terms({r: v[0] for r, v in total.items()}, pp_x, pp_y, 1, 2)
        own_vo = reduce_terms({r: v[1] for r, v in total.items()}, pp_y, pp_x, 2, 1)

        def ordered(own, sib, axis):
            size = own.shape[axis]
            shape = own.shape[:axis] + (2 * size,) + own.shape[axis + 1:]
            return put(put(jnp.zeros(shape, own.dtype), own, core, axis), sib, 1 - core, axis)

        other_half = pp_d(d_cur)
        whole = ordered(d_cur, other_half, 0)
        to_row = [(2 * c + d, 2 * (c ^ 2) + d) for c in range(4) for d in range(2) if c // 2 == d]
        from_y = lax.ppermute(whole, BOTH, to_row)
        row_seq = jnp.where(chip_y == core, whole, from_y)
        from_x = pp_x(row_seq)
        d_x = jnp.zeros((2,) + whole.shape, BF16)
        d_x = put(put(d_x, row_seq[None], chip_x, 0), from_x[None], 1 - chip_x, 0)

        ready = tuple(v for ab in total.values() for v in ab)
        cot_mine = cot_out.reshape(-1, dim)
        cot_other = pp_d(cot_mine)
        grad_2 = None
        for layer in reversed(range(layer_count)):
            g_all = after(g_mine[layer], *ready)
            if layer == layer_count - 1:
                rows = g_all.shape[0] // 2
                grad_2 = tn(take(g_all, core, 0, rows), cot_mine) + tn(take(g_all, 1 - core, 0, rows), cot_other)
            else:
                grad_2 = grad_2 + tn(g_all, next_all[layer])

        grad_2 = join(core, grad_2, pp_d(grad_2))
        grad_1 = join_flip(core, [grad_1a, grad_1b], [pp_d(grad_1a), pp_d(grad_1b)])
        gq, gk, gv, go = join_attn(core, (own_qk, own_vo), (pp_d(own_qk), pp_d(own_vo)))
        return gq, gk, gv, go, grad_1, grad_2, d_x

    return jax.shard_map(device_step, mesh=mesh,
                         in_specs=(spec_act, spec_act, spec_rep, spec_col, spec_col, spec_col, spec_row, spec_col, spec_row),
                         out_specs=(spec_col, spec_col, spec_col, spec_row, spec_col, spec_row, spec_act),
                         check_vma=False)
```

```python
import functools

import jax
import jax.numpy as jnp
from jax import lax
from jax.experimental import pallas as pl
from jax.experimental.pallas import tpu as pltpu
from jax.sharding import PartitionSpec as P


HEAD_DIM = 64
EPS_NORM = 1e-6
F32 = jnp.float32
BF16 = jnp.bfloat16
LOG2E = 1.4426950408889634
VMEM_ALL = 60 * 1024 * 1024
SCALE = HEAD_DIM ** -0.5

SWAP_D = [(0, 1), (1, 0)]


SWAP_X = [(0, 1), (1, 0), (2, 3), (3, 2)]
SWAP_Y = [(0, 2), (2, 0), (1, 3), (3, 1)]


def pp_x(v):
    return lax.ppermute(v, 'model', SWAP_X)


def pp_y(v):
    return lax.ppermute(v, 'model', SWAP_Y)


def pp_d(v):
    return lax.ppermute(v, 'data', SWAP_D)


def dot(a, b, dims):
    return lax.dot_general(a, b, (dims, ((), ())), preferred_element_type=F32)


def nn(a, b):
    return dot(a, b, ((1,), (0,)))


def nt(a, b):
    return dot(a, b, ((1,), (1,)))


def tn(a, b):
    return dot(a, b, ((0,), (0,)))


def pair_masks(rows):
    lane = lax.broadcasted_iota(jnp.int32, (rows, 128), 1)
    return lane < HEAD_DIM


CHUNK = 256


def masked_pair(q):
    low = pair_masks(CHUNK)
    zero = jnp.zeros_like(q)
    return jnp.concatenate([jnp.where(low, q, zero), jnp.where(low, zero, q)], axis=0)


def attn_fwd_body(*refs):
    q_ref, qn_ref, ko_ref, ks_ref, kno_ref, kns_ref, vo_ref, vs_ref = refs[:8]
    ctx_ref, lse_ref, a_ref, b_ref, ma_ref, mb_ref = refs[-6:]

    def scores(ko, ks, q, s_ref, m_ref):
        s = nt(jnp.concatenate([ko[...], ks[...]], axis=0), masked_pair(q))
        s_ref[...] = s
        m_ref[...] = jnp.max(s, axis=0, keepdims=True)

    def finish(s_ref, m_ref, i):
        rows = slice(i * CHUNK, (i + 1) * CHUNK)
        m = m_ref[...]
        p = jnp.exp2((s_ref[...] - m) * (SCALE * LOG2E))
        l = jnp.sum(p, axis=0, keepdims=True)
        pb = (p * (1.0 / l)).astype(BF16)
        lse = m * (SCALE * LOG2E) + jnp.log2(l)
        lse_ref[0, 0:1, rows] = lse[:, :CHUNK]
        lse_ref[0, 1:2, rows] = lse[:, CHUNK:]
        ctx_t = tn(jnp.concatenate([vo_ref[...], vs_ref[...]], axis=0), pb)
        ctx_t = jnp.concatenate([ctx_t[:HEAD_DIM, :CHUNK], ctx_t[HEAD_DIM:, CHUNK:]], axis=0)
        ctx_ref[0, 0, rows, :] = ctx_t.T.astype(BF16)

    @pl.when(pl.program_id(0) == 0)
    def _():
        scores(ko_ref, ks_ref, q_ref[:CHUNK, :], a_ref, ma_ref)

    scores(ko_ref, ks_ref, q_ref[CHUNK:, :], b_ref, mb_ref)
    finish(a_ref, ma_ref, 0)
    scores(kno_ref, kns_ref, qn_ref[:CHUNK, :], a_ref, ma_ref)
    finish(b_ref, mb_ref, 1)


def attn_fwd(q, kv, kv_s, layer, layers, hist):
    tq, width = q.shape
    tk = kv.shape[0]
    pairs = width // 128
    last = pairs - 1

    def col(off):
        return lambda j: (0, j + off)

    def nxt(j):
        return (0, jnp.minimum(j + 1, last))

    extra = [] if hist is None else [hist]
    flops = 2 * 2 * tq * (2 * tk) * 256 * (width // HEAD_DIM)
    return pl.pallas_call(
        attn_fwd_body,
        grid=(pairs,),
        in_specs=[pl.BlockSpec((tq, 128), col(0)), pl.BlockSpec((tq, 128), nxt),
                  pl.BlockSpec((tk, 128), col(0)), pl.BlockSpec((tk, 128), col(0)),
                  pl.BlockSpec((tk, 128), nxt), pl.BlockSpec((tk, 128), nxt),
                  pl.BlockSpec((tk, 128), col(pairs)), pl.BlockSpec((tk, 128), col(pairs))]
        + [pl.BlockSpec(memory_space=pl.ANY)] * len(extra),
        out_specs=[pl.BlockSpec((1, 1, tq, 128), lambda j: (3, layer, 0, j)),
                   pl.BlockSpec((1, 2, tq), lambda j: (j, 0, 0))],
        out_shape=[jax.ShapeDtypeStruct((4, layers, tq, width), BF16),
                   jax.ShapeDtypeStruct((pairs, 2, tq), F32)],
        input_output_aliases={8: 0} if extra else {},
        scratch_shapes=[pltpu.VMEM((2 * tk, 2 * CHUNK), F32), pltpu.VMEM((2 * tk, 2 * CHUNK), F32),
                        pltpu.VMEM((1, 2 * CHUNK), F32), pltpu.VMEM((1, 2 * CHUNK), F32)],
        compiler_params=pltpu.CompilerParams(dimension_semantics=('arbitrary',),
                                             vmem_limit_bytes=VMEM_ALL),
        cost_estimate=pl.CostEstimate(flops=flops, bytes_accessed=2 * (tq * width * 2 + 4 * tk * width),
                                      transcendentals=tq * 2 * tk * (width // HEAD_DIM)),
        name='attn_fwd',
    )(q, q, kv, kv_s, kv, kv_s, kv, kv_s, *extra)


WIDE = 256


def attn_bwd_body(q_ref, ko_ref, ks_ref, vo_ref, vs_ref, do_ref, lse_ref, hist_ref, dq_ref, down_ref, dsib_ref):
    tk = ko_ref.shape[0]
    low = pair_masks(CHUNK)
    for sub in range(WIDE // 128):
        cols = slice(sub * 128, (sub + 1) * 128)
        k = jnp.concatenate([ko_ref[:, cols], ks_ref[:, cols]], axis=0)
        v = jnp.concatenate([vo_ref[:, cols], vs_ref[:, cols]], axis=0)
        for i in range(q_ref.shape[0] // CHUNK):
            rows = slice(i * CHUNK, (i + 1) * CHUNK)
            q = q_ref[rows, cols]
            do = do_ref[rows, cols]
            dqs = []
            for h in range(2):
                sel = low if h == 0 else ~low
                qm = jnp.where(sel, q, jnp.zeros_like(q))
                dom = jnp.where(sel, do, jnp.zeros_like(do))
                s = nt(k, qm)
                p = jnp.exp2(s * (SCALE * LOG2E) - lse_ref[sub, h:h + 1, rows])
                dp = nt(v, dom).astype(BF16).astype(F32)
                delta = jnp.sum(p * dp, axis=0, keepdims=True)
                ds = (p * (dp - delta)).astype(BF16)
                dv = nn(p.astype(BF16), dom)
                dk = nn(ds, qm) * SCALE
                for n, grad in enumerate((dk, dv)):
                    for ref, part in ((down_ref, grad[:tk]), (dsib_ref, grad[tk:])):
                        if i == 0 and h == 0:
                            ref[n, :, cols] = part
                        else:
                            ref[n, :, cols] += part
                dqs.append(tn(k, ds)[h * HEAD_DIM:(h + 1) * HEAD_DIM, :] * SCALE)
            dq_ref[0, 0, rows, cols] = jnp.concatenate(dqs, axis=0).T.astype(BF16)


def attn_bwd(q, kv, kv_s, d_ctx, lse, layer, layers, hist):
    tq, width = q.shape
    tk = kv.shape[0]
    steps = width // WIDE

    def col(off):
        return lambda j: (0, j + off)

    flops = 5 * 2 * tq * (2 * tk) * 256 * (width // HEAD_DIM)
    qblk = pl.BlockSpec((tq, WIDE), col(0))
    kblk = pl.BlockSpec((tk, WIDE), col(0))
    vblk = pl.BlockSpec((tk, WIDE), col(steps))
    both = pl.BlockSpec((2, tk, WIDE), lambda j: (0, 0, j))
    return pl.pallas_call(
        attn_bwd_body,
        grid=(steps,),
        in_specs=[qblk, kblk, kblk, vblk, vblk, qblk,
                  pl.BlockSpec((WIDE // 128, 2, tq), lambda j: (j, 0, 0)), pl.BlockSpec(memory_space=pl.ANY)],
        out_specs=[pl.BlockSpec((1, 1, tq, WIDE), lambda j: (0, layer, 0, j)), both, both],
        out_shape=[jax.ShapeDtypeStruct((4, layers, tq, width), BF16)]
        + [jax.ShapeDtypeStruct((2, tk, width), F32)] * 2,
        input_output_aliases={7: 0},
        compiler_params=pltpu.CompilerParams(dimension_semantics=('arbitrary',),
                                             vmem_limit_bytes=VMEM_ALL),
        cost_estimate=pl.CostEstimate(flops=flops, bytes_accessed=2 * (2 * tq * width * 2 + 4 * tk * width) + 16 * tk * width,
                                      transcendentals=tq * 2 * tk * (width // HEAD_DIM)),
        name='attn_bwd',
    )(q, kv, kv_s, kv, kv_s, d_ctx, lse, hist)


def kv_body(*refs):
    x_ref, e_ref, w_ref = refs[:3]
    kv_ref, u_ref = refs[-2:]

    @pl.when(pl.program_id(0) == 0)
    def _():
        s = x_ref[...].astype(F32) + e_ref[...]
        u_ref[0, 0] = (s * lax.rsqrt(jnp.mean(s * s, axis=-1, keepdims=True) + EPS_NORM)).astype(BF16)

    for rows in ROWS:
        kv_ref[rows, :] = nt(u_ref[0, 0, rows, :], w_ref[...]).astype(BF16)


def norm_kv(x, e, wkv, layer, layers, hist):
    t, dim = x.shape
    width = wkv.shape[0]
    blk = 1024
    extra = [] if hist is None else [hist]
    return pl.pallas_call(
        kv_body,
        grid=(width // blk,),
        in_specs=[pl.BlockSpec((t, dim), lambda j: (0, 0)), pl.BlockSpec((1, dim), lambda j: (0, 0)),
                  pl.BlockSpec((blk, dim), lambda j: (j, 0))] + [pl.BlockSpec(memory_space=pl.ANY)] * len(extra),
        out_specs=[pl.BlockSpec((t, blk), lambda j: (0, j)), pl.BlockSpec((1, 1, t, dim), lambda j: (0, layer, 0, 0))],
        out_shape=[jax.ShapeDtypeStruct((t, width), BF16), jax.ShapeDtypeStruct((2, layers, t, dim), BF16)],
        input_output_aliases={3: 1} if extra else {},
        compiler_params=pltpu.CompilerParams(dimension_semantics=('arbitrary',), vmem_limit_bytes=VMEM_ALL),
        cost_estimate=pl.CostEstimate(flops=2 * t * dim * width, bytes_accessed=2 * (dim * width + t * width + 2 * t * dim),
                                      transcendentals=t),
        name='norm_kv',
    )(x, e, wkv, *extra)


def d_kv_body(acc0_ref, x_ref, e_ref, mid_ref, own_ref, recv_ref, w_ref, hist_ref, dkv_ref, prev_ref, acc_ref):
    j = pl.program_id(0)

    @pl.when(j == 0)
    def _():
        acc_ref[...] = acc0_ref[...]

    dkv_ref[0, 0] = (own_ref[0] + recv_ref[0]).astype(BF16)
    for rows in ROWS:
        acc_ref[rows, :] += nn(dkv_ref[0, 0, rows, :], w_ref[...])

    @pl.when(j == pl.num_programs(0) - 1)
    def _():
        dn = acc_ref[...].astype(BF16).astype(F32)
        s = x_ref[...].astype(F32) + e_ref[...]
        inv = lax.rsqrt(jnp.mean(s * s, axis=-1, keepdims=True) + EPS_NORM)
        proj = jnp.mean(s * dn, axis=-1, keepdims=True)
        prev_ref[...] = (mid_ref[0, 0].astype(F32) + inv * dn - s * (inv * inv * inv * proj)).astype(BF16)


def d_kv(acc0, x, e, um_hist, own, recv, wkv, layer, layers, hist):
    t, dim = x.shape
    half = dim // 2
    whole = pl.BlockSpec((t, dim), lambda j: (0, 0))
    gblk = pl.BlockSpec((1, t, half), lambda j: (j // 2, 0, j % 2))
    return pl.pallas_call(
        d_kv_body,
        grid=(4,),
        in_specs=[whole, whole, pl.BlockSpec((1, dim), lambda j: (0, 0)),
                  pl.BlockSpec((1, 1, t, dim), lambda j: (1, layer, 0, 0)), gblk, gblk,
                  pl.BlockSpec((half, dim), lambda j: (j, 0)), pl.BlockSpec(memory_space=pl.ANY)],
        out_specs=[pl.BlockSpec((1, 1, t, half), lambda j: (1 + j // 2, layer, 0, j % 2)), whole],
        out_shape=[jax.ShapeDtypeStruct((4, layers, t, dim), BF16), jax.ShapeDtypeStruct((t, dim), BF16)],
        scratch_shapes=[pltpu.VMEM((t, dim), F32)],
        input_output_aliases={7: 0},
        compiler_params=pltpu.CompilerParams(dimension_semantics=('arbitrary',), vmem_limit_bytes=VMEM_ALL),
        cost_estimate=pl.CostEstimate(flops=4 * t * dim * dim, bytes_accessed=4 * dim * dim + 20 * t * dim, transcendentals=t),
        name='d_kv',
    )(acc0, x, e, um_hist, own, recv, wkv, hist)


def terms_body(added, places_ref, lhs_ref, rhs_ref, *refs):
    recv, outs = refs[:4 * added], refs[-4:]
    step = 4 * pl.program_id(0) + pl.program_id(1)
    val = tn(lhs_ref[0], rhs_ref[0])
    for slot in range(4):
        @pl.when(step // 2 == slot)
        def _():
            outs[slot][0] = val + recv[slot][0] if added else val


def terms(lhs, rhs, rows, cols, places, lhs_at, rhs_at, chips, recv):
    tokens = lhs.shape[1]
    first, second = chips

    def rel(r):
        return first + r * (second - first)

    slots = [pl.BlockSpec((1, rows, cols), lambda r, kind, p, at=2 * n: (jnp.clip(4 * r + kind - at, 0, 1), 0, 0))
             for n in range(4)]
    out = pl.pallas_call(
        functools.partial(terms_body, len(recv) // 4),
        grid_spec=pltpu.PrefetchScalarGridSpec(
            num_scalar_prefetch=1, grid=(2, 4),
            in_specs=[pl.BlockSpec((1, tokens, rows), lambda r, kind, p: lhs_at(rel(r), kind, p)),
                      pl.BlockSpec((1, tokens, cols), lambda r, kind, p: rhs_at(rel(r), kind, p))] + slots[:len(recv)],
            out_specs=slots),
        out_shape=[jax.ShapeDtypeStruct((2, rows, cols), F32)] * 4,
        compiler_params=pltpu.CompilerParams(dimension_semantics=('arbitrary', 'arbitrary'), vmem_limit_bytes=VMEM_ALL),
        cost_estimate=pl.CostEstimate(flops=16 * tokens * rows * cols, bytes_accessed=24 * tokens * rows, transcendentals=0),
    )(places, lhs, rhs, *recv)
    return {first: out[:2], second: out[2:]}


def attn_lhs_at(rel, kind, p):
    return kind, 0, rel


def attn_rhs_at(rel, kind, p):
    return kind // 3, 0, p[0]


def up_lhs_at(rel, kind, p):
    return 0, 0, 4 * p[1 + rel] + 2 * p[0] + kind % 2


def up_rhs_at(rel, kind, p):
    return 0, 0, kind // 2


def summed_terms(lhs, rhs, rows, cols, places, lhs_at, rhs_at):
    sent = {}
    for pair in ((3, 1), (2, 0)):
        for r, ab in terms(lhs, rhs, rows, cols, places[1], lhs_at, rhs_at, pair, []).items():
            sent[r] = [pp_d(v) for v in ab]
    total = {}
    for pair in ((3, 1), (2, 0)):
        total.update(terms(lhs, rhs, rows, cols, places[0], lhs_at, rhs_at, pair, sent[pair[0]] + sent[pair[1]]))
    return total


GELU_C = 0.7978845608028654
GELU_A = 0.044715
BLOCK_F = 768
ROWS = (slice(0, 256), slice(256, 512))


def mlp_fwd_body(*refs):
    x0_ref, e_ref, ctx_ref, wo_ref, w1_ref, w2_ref = refs[:6]
    z_ref, g_ref, x_ref, h_ref, m_ref, acc_ref = refs[-6:]
    j = pl.program_id(0)

    @pl.when(j == 0)
    def _():
        for rows in ROWS:
            s = x0_ref[rows, :].astype(F32) + e_ref[...]
            h = (s + nn(ctx_ref[0, 0, rows, :], wo_ref[...])).astype(BF16)
            h_ref[rows, :] = h
            hf = h.astype(F32)
            acc_ref[rows, :] = hf
            m_ref[0, rows, :] = (hf * lax.rsqrt(jnp.mean(hf * hf, axis=-1, keepdims=True) + EPS_NORM)).astype(BF16)

    for rows in ROWS:
        z = nt(m_ref[0, rows, :], w1_ref[...]).astype(BF16)
        z_ref[rows, :] = z
        zf = z.astype(F32)
        t = jnp.tanh(zf * (GELU_C + (GELU_A * GELU_C) * (zf * zf)))
        half = 0.5 * zf
        g_ref[0, rows, :] = (half + half * t).astype(BF16)
    for rows in ROWS:
        acc_ref[rows, :] += nn(g_ref[0, rows, :], w2_ref[...])

    @pl.when(j == pl.num_programs(0) - 1)
    def _():
        x_ref[...] = acc_ref[...].astype(BF16)


def mlp_fwd(x, e, ctx_hist, wo, w1t, w2, layer, layers, hist):
    t, dim = x.shape
    hidden = w2.shape[0]
    whole = pl.BlockSpec((t, dim), lambda j: (0, 0))
    slab = pl.BlockSpec((1, t, dim), lambda j: (layer, 0, 0))
    wblk = pl.BlockSpec((BLOCK_F, dim), lambda j: (j, 0))
    extra = [] if hist is None else [hist]
    return pl.pallas_call(
        mlp_fwd_body,
        grid=(hidden // BLOCK_F,),
        in_specs=[whole, pl.BlockSpec((1, dim), lambda j: (0, 0)), pl.BlockSpec((1, 1, t, dim), lambda j: (3, layer, 0, 0)),
                  pl.BlockSpec((dim, dim), lambda j: (0, 0)), wblk, wblk]
        + [pl.BlockSpec(memory_space=pl.ANY)] * len(extra),
        out_specs=[pl.BlockSpec((t, BLOCK_F), lambda j: (0, j)),
                   pl.BlockSpec((1, t, BLOCK_F), lambda j: (j, 0, 0)), whole, whole, slab],
        out_shape=[jax.ShapeDtypeStruct((t, hidden), BF16),
                   jax.ShapeDtypeStruct((hidden // BLOCK_F, t, BLOCK_F), BF16),
                   jax.ShapeDtypeStruct((t, dim), BF16), jax.ShapeDtypeStruct((t, dim), BF16),
                   jax.ShapeDtypeStruct((layers, t, dim), BF16)],
        scratch_shapes=[pltpu.VMEM((t, dim), F32)],
        input_output_aliases={6: 4} if extra else {},
        compiler_params=pltpu.CompilerParams(dimension_semantics=('arbitrary',), vmem_limit_bytes=VMEM_ALL),
        cost_estimate=pl.CostEstimate(flops=4 * t * dim * hidden, bytes_accessed=4 * dim * hidden + 4 * t * hidden,
                                      transcendentals=t * hidden),
        name='mlp_fwd',
    )(x, e, ctx_hist, wo, w1t, w2, *extra)


BLOCK_B = 1024
SUB_B = 512


def mlp_bwd_body(*refs):
    d_ref, h_ref, z_ref, wo_ref, w1_ref, w2_ref = refs[:6]
    up_ref, mid_ref, dctx_ref, acc_ref = refs[-4:]
    j = pl.program_id(0)

    @pl.when(j == 0)
    def _():
        acc_ref[...] = jnp.zeros_like(acc_ref)

    for i in range(0, BLOCK_B, SUB_B):
        cols = slice(i, i + SUB_B)
        for rows in ROWS:
            da = nt(d_ref[rows, :], w2_ref[cols, :]).astype(BF16).astype(F32)
            zf = z_ref[rows, cols].astype(F32)
            z2 = zf * zf
            t = jnp.tanh(zf * (GELU_C + (GELU_A * GELU_C) * z2))
            slope = (1.0 + t) * (0.5 + (1.0 - t) * (zf * (0.5 * GELU_C + (1.5 * GELU_A * GELU_C) * z2)))
            up_ref[0, rows, cols] = (da * slope).astype(BF16)
    for rows in ROWS:
        acc_ref[rows, :] += nn(up_ref[0, rows, :], w1_ref[...])

    @pl.when(j == pl.num_programs(0) - 1)
    def _():
        for rows in ROWS:
            dn = acc_ref[rows, :].astype(BF16).astype(F32)
            hf = h_ref[rows, :].astype(F32)
            inv = lax.rsqrt(jnp.mean(hf * hf, axis=-1, keepdims=True) + EPS_NORM)
            proj = jnp.mean(hf * dn, axis=-1, keepdims=True)
            mid = (d_ref[rows, :].astype(F32) + inv * dn - hf * (inv * inv * inv * proj)).astype(BF16)
            mid_ref[0, 0, rows, :] = mid
            dctx_ref[rows, :] = nt(mid, wo_ref[...]).astype(BF16)


def mlp_bwd(d_next, h, z, wo, w1t, w2, layer, layers, um_hist, hist):
    t, dim = h.shape
    hidden = w2.shape[0]
    whole = pl.BlockSpec((t, dim), lambda j: (0, 0))
    wblk = pl.BlockSpec((BLOCK_B, dim), lambda j: (j, 0))
    extra = [um_hist] if hist is None else [um_hist, hist]
    return pl.pallas_call(
        mlp_bwd_body,
        grid=(hidden // BLOCK_B,),
        in_specs=[whole, whole, pl.BlockSpec((t, BLOCK_B), lambda j: (0, j)), pl.BlockSpec((dim, dim), lambda j: (0, 0)), wblk, wblk]
        + [pl.BlockSpec(memory_space=pl.ANY)] * len(extra),
        out_specs=[pl.BlockSpec((1, t, BLOCK_B), lambda j: (layer, 0, j)), pl.BlockSpec((1, 1, t, dim), lambda j: (1, layer, 0, 0)), whole],
        out_shape=[jax.ShapeDtypeStruct((layers, t, hidden), BF16), jax.ShapeDtypeStruct((2, layers, t, dim), BF16),
                   jax.ShapeDtypeStruct((t, dim), BF16)],
        scratch_shapes=[pltpu.VMEM((t, dim), F32)],
        input_output_aliases={6: 1} if hist is None else {6: 1, 7: 0},
        compiler_params=pltpu.CompilerParams(dimension_semantics=('arbitrary',), vmem_limit_bytes=VMEM_ALL),
        cost_estimate=pl.CostEstimate(flops=4 * t * dim * hidden, bytes_accessed=4 * dim * hidden + 4 * t * hidden,
                                      transcendentals=t * hidden),
        name='mlp_bwd',
    )(d_next, h, z, wo, w1t, w2, *extra)


def join_body(count, core_ref, *refs):
    for n in range(count):
        own, other, out = refs[n], refs[count + n], refs[2 * count + n]
        for i, src in enumerate((own, other)):
            @pl.when(pl.program_id(0) == i)
            def _():
                out[...] = src[...]


def join_call(core, body, grid, own, other, in_specs, out_specs, out_shape):
    size = sum(v.size for v in own)
    return pl.pallas_call(
        body,
        grid_spec=pltpu.PrefetchScalarGridSpec(num_scalar_prefetch=1, grid=grid, in_specs=in_specs * 2, out_specs=out_specs),
        out_shape=out_shape,
        compiler_params=pltpu.CompilerParams(dimension_semantics=('arbitrary', 'arbitrary'), vmem_limit_bytes=VMEM_ALL),
        cost_estimate=pl.CostEstimate(flops=8 * size, bytes_accessed=16 * size, transcendentals=0),
    )(core.reshape(1), *own, *other)


def join(core, own, other):
    rows, cols = own.shape[0], own.shape[1] // 4
    block = pl.BlockSpec((rows, cols), lambda i, j, c: (0, j))
    return join_call(core, functools.partial(join_body, 1), (2, 4), [own], [other], [block],
                     pl.BlockSpec((rows, cols), lambda i, j, c: ((c[0] + i) % 2, j)),
                     jax.ShapeDtypeStruct((2 * rows, own.shape[1]), F32))


def join_attn_body(core_ref, own_a, own_b, sib_a, sib_b, q_ref, k_ref, v_ref, o_ref):
    for i, (a_ref, b_ref) in enumerate(((own_a, own_b), (sib_a, sib_b))):
        @pl.when(pl.program_id(0) == i)
        def _():
            q_ref[...] = a_ref[0].T
            k_ref[...] = a_ref[1].T
            v_ref[...] = b_ref[0].T
            o_ref[...] = b_ref[1]


def join_attn(core, own, other):
    _, hid, half_d = own[0].shape
    block = pl.BlockSpec((2, hid, half_d), lambda i, j, c: (0, 0, 0))
    tall = pl.BlockSpec((half_d, hid), lambda i, j, c: ((c[0] + i) % 2, 0))
    wide = pl.BlockSpec((hid, half_d), lambda i, j, c: (0, (c[0] + i) % 2))
    return join_call(core, join_attn_body, (2, 1), list(own), list(other), [block] * 2, [tall] * 3 + [wide],
                     [jax.ShapeDtypeStruct((2 * half_d, hid), F32)] * 3 + [jax.ShapeDtypeStruct((hid, 2 * half_d), F32)])


def join_flip_body(core_ref, oa_ref, ob_ref, sa_ref, sb_ref, out_ref):
    for i, srcs in enumerate(((oa_ref, ob_ref), (sa_ref, sb_ref))):
        for j, src in enumerate(srcs):
            @pl.when((pl.program_id(0) == i) & (pl.program_id(1) == j))
            def _():
                out_ref[...] = src[...].T


def join_flip(core, own, other):
    rows, cols = own[0].shape
    block = pl.BlockSpec((rows, cols), lambda i, j, c: (0, 0))
    return join_call(core, join_flip_body, (2, 2), own, other, [block] * 2,
                     pl.BlockSpec((cols, rows), lambda i, j, c: (j, (c[0] + i) % 2)),
                     jax.ShapeDtypeStruct((2 * cols, 2 * rows), F32))


def gather_pieces(part_a, part_b):
    xa, xb = pp_x(part_a), pp_x(part_b)
    ya, yb = pp_y(part_a), pp_y(part_b)
    da, db = pp_y(xa), pp_x(yb)
    own = [(xa, xb), (ya, yb), (da, db)]
    return own, [(pp_d(a), pp_d(b)) for a, b in own]


def reduce_terms(total, pp_first, pp_second, first, second):
    here, there = pp_first(total[first]), pp_first(total[3])
    last = pp_second(total[second] + there)
    return total[0] + here + last


BOTH = ('model', 'data')


def solution(mesh):
    spec_col = P(None, 'model')
    spec_row = P('model', None)
    spec_act = P('data', None, None)
    spec_rep = P(None, None)

    def device_step(x_in, cot_out, step_emb, w_q, w_k, w_v, w_o, w_1, w_2):
        layer_count, dim = step_emb.shape
        core = lax.axis_index('data')
        chip = lax.axis_index('model')
        chip_x = lax.rem(chip, 2)
        chip_y = lax.div(chip, 2)
        nbr_x = chip + 1 - 2 * chip_x
        nbr_y = lax.rem(chip + 2, 4)
        diag = lax.rem(nbr_x + 2, 4)
        chips = (chip, nbr_x, nbr_y, diag)
        hid = w_q.shape[1]
        half_d = dim // 2

        def take(v, which, axis, size):
            return lax.dynamic_slice_in_dim(v, which * size, size, axis)

        def put(buf, v, which, axis):
            return lax.dynamic_update_slice_in_dim(buf, v, which * v.shape[axis], axis)

        def gather(v):
            return lax.all_gather(v, BOTH, axis=0, tiled=True)

        def after(v, *deps):
            return lax.optimization_barrier((v,) + deps)[0]

        def my_tokens(v):
            mine = lax.dynamic_index_in_dim(v, chip_x, 0, keepdims=False)
            half = mine.shape[0] // 2
            recv = pp_d(take(mine, 1 - core, 0, half))
            return jnp.where(core == chip_y, take(mine, core, 0, half), recv)

        def gather_permuted(local):
            own = take(local, core, 0, local.shape[0] // 2)
            rows = own.shape[0] // 2
            p_own, p_sib = gather_pieces(own[:rows], own[rows:])
            full = put(jnp.zeros((4 * local.shape[0], dim), BF16), local, chip, 0)
            for r in (1, 2, 3):
                for part in (0, 1):
                    full = put(full, p_own[r - 1][part], 4 * chips[r] + 2 * core + part, 0)
                    full = put(full, p_sib[r - 1][part], 4 * chips[r] + 2 * (1 - core) + part, 0)
            return full

        x_cur = my_tokens(x_in)
        qkv_t = jnp.concatenate([w_q, w_k, w_v], axis=1).T
        qkv_all = gather(take(qkv_t, core, 0, qkv_t.shape[0] // 2))
        o_all = gather(take(w_o, core, 0, hid // 2))
        w2 = gather_permuted(w_2)
        w1 = gather_permuted(w_1.T)
        wq = jnp.concatenate([take(qkv_all, 3 * c, 0, hid) for c in chips], axis=0)
        wkv = jnp.concatenate([take(qkv_all, 3 * c + i, 0, hid) for i in (1, 2) for c in chips], axis=0)
        wo = jnp.concatenate([take(o_all, c, 0, hid) for c in chips], axis=0)
        d_cur = my_tokens(cot_out)
        emb = step_emb.astype(F32)

        saved = []
        g_mine = []
        um_hist = m_hist = att_hist = None
        for layer in range(layer_count):
            e = emb[layer:layer + 1]
            kv, um_hist = norm_kv(x_cur, e, wkv, layer, layer_count, um_hist)
            kv_s = pp_d(kv)
            q = nt(um_hist[0, layer], wq).astype(BF16)
            att_hist, lse = attn_fwd(q, kv, kv_s, layer, layer_count, att_hist)
            z, g, x_next, h, m_hist = mlp_fwd(x_cur, e, att_hist, wo, w1, w2, layer, layer_count, m_hist)
            g_mine.append(lax.all_to_all(g.reshape(-1, g.shape[-1]), BOTH, split_axis=0, concat_axis=0, tiled=True))
            saved.append((x_cur, q, kv, kv_s, lse, h, z))
            x_cur = x_next

        def flat(v, lead):
            return v.reshape(lead, -1, v.shape[-1])

        places = [jnp.stack([w, *chips]).astype(jnp.int32) for w in (core, 1 - core)]
        up_hist = None
        next_all = [None] * layer_count
        for layer in reversed(range(layer_count)):
            x_l, q, kv, kv_s, lse, h, z = saved[layer]
            e = emb[layer:layer + 1]
            d_next = d_cur
            if layer < layer_count - 1:
                next_all[layer] = gather(d_next)
            up_hist, um_hist, d_ctx = mlp_bwd(d_next, h, z, wo, w1, w2, layer, layer_count, um_hist, up_hist)
            if layer == 0:
                total = summed_terms(flat(up_hist, 1), flat(m_hist, 1), hid, half_d, places, up_lhs_at, up_rhs_at)
                d_ctx = after(d_ctx, *[v for r in (1, 2, 3) for v in total[r]])
                own_1a = reduce_terms({r: v[0] for r, v in total.items()}, pp_x, pp_y, 1, 2)
                own_1b = reduce_terms({r: v[1] for r, v in total.items()}, pp_y, pp_x, 2, 1)
            att_hist, own_kv, sib_kv = attn_bwd(q, kv, kv_s, d_ctx, lse, layer, layer_count, att_hist)
            recv_kv = pp_d(sib_kv)
            acc0 = nn(att_hist[0, layer], wq)
            att_hist, d_cur = d_kv(acc0, x_l, e, um_hist, own_kv, recv_kv, wkv, layer, layer_count, att_hist)

        total = summed_terms(flat(att_hist, 4), flat(um_hist, 2), hid, half_d, places, attn_lhs_at, attn_rhs_at)
        own_qk = reduce_terms({r: v[0] for r, v in total.items()}, pp_x, pp_y, 1, 2)
        own_vo = reduce_terms({r: v[1] for r, v in total.items()}, pp_y, pp_x, 2, 1)

        def ordered(own, sib, axis):
            size = own.shape[axis]
            shape = own.shape[:axis] + (2 * size,) + own.shape[axis + 1:]
            return put(put(jnp.zeros(shape, own.dtype), own, core, axis), sib, 1 - core, axis)

        other_half = pp_d(d_cur)
        whole = ordered(d_cur, other_half, 0)
        to_row = [(2 * c + d, 2 * (c ^ 2) + d) for c in range(4) for d in range(2) if c // 2 == d]
        from_y = lax.ppermute(whole, BOTH, to_row)
        row_seq = jnp.where(chip_y == core, whole, from_y)
        from_x = pp_x(row_seq)
        d_x = jnp.zeros((2,) + whole.shape, BF16)
        d_x = put(put(d_x, row_seq[None], chip_x, 0), from_x[None], 1 - chip_x, 0)

        ready = tuple(v for ab in total.values() for v in ab)
        cot_mine = cot_out.reshape(-1, dim)
        cot_other = pp_d(cot_mine)
        grad_2 = None
        for layer in reversed(range(layer_count)):
            g_all = after(g_mine[layer], *ready)
            if layer == layer_count - 1:
                rows = g_all.shape[0] // 2
                grad_2 = tn(take(g_all, core, 0, rows), cot_mine) + tn(take(g_all, 1 - core, 0, rows), cot_other)
            else:
                grad_2 = grad_2 + tn(g_all, next_all[layer])

        grad_2 = join(core, grad_2, pp_d(grad_2))
        own_1 = [v.reshape(-1, half_d) for v in (own_1a, own_1b)]
        grad_1 = join_flip(core, own_1, [pp_d(v) for v in own_1])
        gq, gk, gv, go = join_attn(core, (own_qk, own_vo), (pp_d(own_qk), pp_d(own_vo)))
        return gq, gk, gv, go, grad_1, grad_2, d_x

    return jax.shard_map(device_step, mesh=mesh,
                         in_specs=(spec_act, spec_act, spec_rep, spec_col, spec_col, spec_col, spec_row, spec_col, spec_row),
                         out_specs=(spec_col, spec_col, spec_col, spec_row, spec_col, spec_row, spec_act),
                         check_vma=False)
```

```python
import functools

import jax
import jax.numpy as jnp
from jax import lax
from jax.experimental import pallas as pl
from jax.experimental.pallas import tpu as pltpu
from jax.sharding import PartitionSpec as P


HEAD_DIM = 64
EPS_NORM = 1e-6
F32 = jnp.float32
BF16 = jnp.bfloat16
LOG2E = 1.4426950408889634
VMEM_ALL = 60 * 1024 * 1024
SCALE = HEAD_DIM ** -0.5

SWAP_D = [(0, 1), (1, 0)]


SWAP_X = [(0, 1), (1, 0), (2, 3), (3, 2)]
SWAP_Y = [(0, 2), (2, 0), (1, 3), (3, 1)]


def pp_x(v):
    return lax.ppermute(v, 'model', SWAP_X)


def pp_y(v):
    return lax.ppermute(v, 'model', SWAP_Y)


def pp_d(v):
    return lax.ppermute(v, 'data', SWAP_D)


def dot(a, b, dims):
    return lax.dot_general(a, b, (dims, ((), ())), preferred_element_type=F32)


def nn(a, b):
    return dot(a, b, ((1,), (0,)))


def nt(a, b):
    return dot(a, b, ((1,), (1,)))


def tn(a, b):
    return dot(a, b, ((0,), (0,)))


def pair_masks(rows):
    lane = lax.broadcasted_iota(jnp.int32, (rows, 128), 1)
    return lane < HEAD_DIM


CHUNK = 256


def masked_pair(q):
    low = pair_masks(CHUNK)
    zero = jnp.zeros_like(q)
    return jnp.concatenate([jnp.where(low, q, zero), jnp.where(low, zero, q)], axis=0)


def attn_fwd_body(*refs):
    q_ref, qn_ref, ko_ref, ks_ref, kno_ref, kns_ref, vo_ref, vs_ref = refs[:8]
    ctx_ref, lse_ref, a_ref, b_ref, ma_ref, mb_ref = refs[-6:]

    def scores(ko, ks, q, s_ref, m_ref):
        s = nt(jnp.concatenate([ko[...], ks[...]], axis=0), masked_pair(q))
        s_ref[...] = s
        m_ref[...] = jnp.max(s, axis=0, keepdims=True)

    def finish(s_ref, m_ref, i):
        rows = slice(i * CHUNK, (i + 1) * CHUNK)
        m = m_ref[...]
        p = jnp.exp2((s_ref[...] - m) * (SCALE * LOG2E))
        l = jnp.sum(p, axis=0, keepdims=True)
        pb = (p * (1.0 / l)).astype(BF16)
        lse = m * (SCALE * LOG2E) + jnp.log2(l)
        lse_ref[0, 0:1, rows] = lse[:, :CHUNK]
        lse_ref[0, 1:2, rows] = lse[:, CHUNK:]
        ctx_t = tn(jnp.concatenate([vo_ref[...], vs_ref[...]], axis=0), pb)
        ctx_t = jnp.concatenate([ctx_t[:HEAD_DIM, :CHUNK], ctx_t[HEAD_DIM:, CHUNK:]], axis=0)
        ctx_ref[0, 0, rows, :] = ctx_t.T.astype(BF16)

    @pl.when(pl.program_id(0) == 0)
    def _():
        scores(ko_ref, ks_ref, q_ref[:CHUNK, :], a_ref, ma_ref)

    scores(ko_ref, ks_ref, q_ref[CHUNK:, :], b_ref, mb_ref)
    finish(a_ref, ma_ref, 0)
    scores(kno_ref, kns_ref, qn_ref[:CHUNK, :], a_ref, ma_ref)
    finish(b_ref, mb_ref, 1)


def attn_fwd(q, kv, kv_s, layer, layers, hist):
    tq, width = q.shape
    tk = kv.shape[0]
    pairs = width // 128
    last = pairs - 1

    def col(off):
        return lambda j: (0, j + off)

    def nxt(j):
        return (0, jnp.minimum(j + 1, last))

    extra = [] if hist is None else [hist]
    flops = 2 * 2 * tq * (2 * tk) * 256 * (width // HEAD_DIM)
    return pl.pallas_call(
        attn_fwd_body,
        grid=(pairs,),
        in_specs=[pl.BlockSpec((tq, 128), col(0)), pl.BlockSpec((tq, 128), nxt),
                  pl.BlockSpec((tk, 128), col(0)), pl.BlockSpec((tk, 128), col(0)),
                  pl.BlockSpec((tk, 128), nxt), pl.BlockSpec((tk, 128), nxt),
                  pl.BlockSpec((tk, 128), col(pairs)), pl.BlockSpec((tk, 128), col(pairs))]
        + [pl.BlockSpec(memory_space=pl.ANY)] * len(extra),
        out_specs=[pl.BlockSpec((1, 1, tq, 128), lambda j: (3, layer, 0, j)),
                   pl.BlockSpec((1, 2, tq), lambda j: (j, 0, 0))],
        out_shape=[jax.ShapeDtypeStruct((4, layers, tq, width), BF16),
                   jax.ShapeDtypeStruct((pairs, 2, tq), F32)],
        input_output_aliases={8: 0} if extra else {},
        scratch_shapes=[pltpu.VMEM((2 * tk, 2 * CHUNK), F32), pltpu.VMEM((2 * tk, 2 * CHUNK), F32),
                        pltpu.VMEM((1, 2 * CHUNK), F32), pltpu.VMEM((1, 2 * CHUNK), F32)],
        compiler_params=pltpu.CompilerParams(dimension_semantics=('arbitrary',),
                                             vmem_limit_bytes=VMEM_ALL),
        cost_estimate=pl.CostEstimate(flops=flops, bytes_accessed=2 * (tq * width * 2 + 4 * tk * width),
                                      transcendentals=tq * 2 * tk * (width // HEAD_DIM)),
        name='attn_fwd',
    )(q, q, kv, kv_s, kv, kv_s, kv, kv_s, *extra)


WIDE = 256


def attn_bwd_body(q_ref, ko_ref, ks_ref, vo_ref, vs_ref, do_ref, lse_ref, hist_ref, dq_ref, down_ref, dsib_ref):
    tk = ko_ref.shape[0]
    low = pair_masks(CHUNK)
    for sub in range(WIDE // 128):
        cols = slice(sub * 128, (sub + 1) * 128)
        k = jnp.concatenate([ko_ref[:, cols], ks_ref[:, cols]], axis=0)
        v = jnp.concatenate([vo_ref[:, cols], vs_ref[:, cols]], axis=0)
        for i in range(q_ref.shape[0] // CHUNK):
            rows = slice(i * CHUNK, (i + 1) * CHUNK)
            q = q_ref[rows, cols]
            do = do_ref[rows, cols]
            dqs = []
            for h in range(2):
                sel = low if h == 0 else ~low
                qm = jnp.where(sel, q, jnp.zeros_like(q))
                dom = jnp.where(sel, do, jnp.zeros_like(do))
                s = nt(k, qm)
                p = jnp.exp2(s * (SCALE * LOG2E) - lse_ref[sub, h:h + 1, rows])
                dp = nt(v, dom).astype(BF16).astype(F32)
                delta = jnp.sum(p * dp, axis=0, keepdims=True)
                ds = (p * (dp - delta)).astype(BF16)
                dv = nn(p.astype(BF16), dom)
                dk = nn(ds, qm) * SCALE
                for n, grad in enumerate((dk, dv)):
                    for ref, part in ((down_ref, grad[:tk]), (dsib_ref, grad[tk:])):
                        if i == 0 and h == 0:
                            ref[n, :, cols] = part
                        else:
                            ref[n, :, cols] += part
                dqs.append(tn(k, ds)[h * HEAD_DIM:(h + 1) * HEAD_DIM, :] * SCALE)
            dq_ref[0, 0, rows, cols] = jnp.concatenate(dqs, axis=0).T.astype(BF16)


def attn_bwd(q, kv, kv_s, d_ctx, lse, layer, layers, hist):
    tq, width = q.shape
    tk = kv.shape[0]
    steps = width // WIDE

    def col(off):
        return lambda j: (0, j + off)

    flops = 5 * 2 * tq * (2 * tk) * 256 * (width // HEAD_DIM)
    qblk = pl.BlockSpec((tq, WIDE), col(0))
    kblk = pl.BlockSpec((tk, WIDE), col(0))
    vblk = pl.BlockSpec((tk, WIDE), col(steps))
    both = pl.BlockSpec((2, tk, WIDE), lambda j: (0, 0, j))
    return pl.pallas_call(
        attn_bwd_body,
        grid=(steps,),
        in_specs=[qblk, kblk, kblk, vblk, vblk, qblk,
                  pl.BlockSpec((WIDE // 128, 2, tq), lambda j: (j, 0, 0)), pl.BlockSpec(memory_space=pl.ANY)],
        out_specs=[pl.BlockSpec((1, 1, tq, WIDE), lambda j: (0, layer, 0, j)), both, both],
        out_shape=[jax.ShapeDtypeStruct((4, layers, tq, width), BF16)]
        + [jax.ShapeDtypeStruct((2, tk, width), F32)] * 2,
        input_output_aliases={7: 0},
        compiler_params=pltpu.CompilerParams(dimension_semantics=('arbitrary',),
                                             vmem_limit_bytes=VMEM_ALL),
        cost_estimate=pl.CostEstimate(flops=flops, bytes_accessed=2 * (2 * tq * width * 2 + 4 * tk * width) + 16 * tk * width,
                                      transcendentals=tq * 2 * tk * (width // HEAD_DIM)),
        name='attn_bwd',
    )(q, kv, kv_s, kv, kv_s, d_ctx, lse, hist)


def kv_body(*refs):
    x_ref, e_ref, w_ref = refs[:3]
    kv_ref, u_ref = refs[-2:]

    @pl.when(pl.program_id(0) == 0)
    def _():
        s = x_ref[...].astype(F32) + e_ref[...]
        u_ref[0, 0] = (s * lax.rsqrt(jnp.mean(s * s, axis=-1, keepdims=True) + EPS_NORM)).astype(BF16)

    for rows in ROWS:
        kv_ref[rows, :] = nt(u_ref[0, 0, rows, :], w_ref[...]).astype(BF16)


def norm_kv(x, e, wkv, layer, layers, hist):
    t, dim = x.shape
    width = wkv.shape[0]
    blk = 1024
    extra = [] if hist is None else [hist]
    return pl.pallas_call(
        kv_body,
        grid=(width // blk,),
        in_specs=[pl.BlockSpec((t, dim), lambda j: (0, 0)), pl.BlockSpec((1, dim), lambda j: (0, 0)),
                  pl.BlockSpec((blk, dim), lambda j: (j, 0))] + [pl.BlockSpec(memory_space=pl.ANY)] * len(extra),
        out_specs=[pl.BlockSpec((t, blk), lambda j: (0, j)), pl.BlockSpec((1, 1, t, dim), lambda j: (0, layer, 0, 0))],
        out_shape=[jax.ShapeDtypeStruct((t, width), BF16), jax.ShapeDtypeStruct((2, layers, t, dim), BF16)],
        input_output_aliases={3: 1} if extra else {},
        compiler_params=pltpu.CompilerParams(dimension_semantics=('arbitrary',), vmem_limit_bytes=VMEM_ALL),
        cost_estimate=pl.CostEstimate(flops=2 * t * dim * width, bytes_accessed=2 * (dim * width + t * width + 2 * t * dim),
                                      transcendentals=t),
        name='norm_kv',
    )(x, e, wkv, *extra)


def d_kv_body(layer, acc0_hbm, x_hbm, e_ref, um_hbm, own_ref, recv_ref, w_ref, hist_ref, dkv_ref, prev_ref,
              acc_ref, acc0_ref, x_ref, mid_ref, sems):
    j = pl.program_id(0)
    late = [pltpu.make_async_copy(src, dst, sems.at[n])
            for n, (src, dst) in enumerate(((acc0_hbm, acc0_ref), (x_hbm, x_ref), (um_hbm.at[1, layer], mid_ref)))]

    @pl.when(j == 0)
    def _():
        for copy in late:
            copy.start()
        acc_ref[...] = jnp.zeros_like(acc_ref)

    dkv_ref[0, 0] = (own_ref[0] + recv_ref[0]).astype(BF16)
    for rows in ROWS:
        acc_ref[rows, :] += nn(dkv_ref[0, 0, rows, :], w_ref[...])

    @pl.when(j == pl.num_programs(0) - 1)
    def _():
        for copy in late:
            copy.wait()
        dn = (acc_ref[...] + acc0_ref[...]).astype(BF16).astype(F32)
        s = x_ref[...].astype(F32) + e_ref[...]
        inv = lax.rsqrt(jnp.mean(s * s, axis=-1, keepdims=True) + EPS_NORM)
        proj = jnp.mean(s * dn, axis=-1, keepdims=True)
        prev_ref[...] = (mid_ref[...].astype(F32) + inv * dn - s * (inv * inv * inv * proj)).astype(BF16)


def d_kv(acc0, x, e, um_hist, own, recv, wkv, layer, layers, hist):
    t, dim = x.shape
    half = dim // 2
    hbm = pl.BlockSpec(memory_space=pl.ANY)
    gblk = pl.BlockSpec((1, t, half), lambda j: (j // 2, 0, j % 2))
    return pl.pallas_call(
        functools.partial(d_kv_body, layer),
        grid=(4,),
        in_specs=[hbm, hbm, pl.BlockSpec((1, dim), lambda j: (0, 0)), hbm, gblk, gblk,
                  pl.BlockSpec((half, dim), lambda j: (j, 0)), hbm],
        out_specs=[pl.BlockSpec((1, 1, t, half), lambda j: (1 + j // 2, layer, 0, j % 2)),
                   pl.BlockSpec((t, dim), lambda j: (0, 0))],
        out_shape=[jax.ShapeDtypeStruct((4, layers, t, dim), BF16), jax.ShapeDtypeStruct((t, dim), BF16)],
        scratch_shapes=[pltpu.VMEM((t, dim), F32), pltpu.VMEM((t, dim), F32), pltpu.VMEM((t, dim), BF16),
                        pltpu.VMEM((t, dim), BF16), pltpu.SemaphoreType.DMA((3,))],
        input_output_aliases={7: 0},
        compiler_params=pltpu.CompilerParams(dimension_semantics=('arbitrary',), vmem_limit_bytes=VMEM_ALL),
        cost_estimate=pl.CostEstimate(flops=4 * t * dim * dim, bytes_accessed=4 * dim * dim + 20 * t * dim, transcendentals=t),
        name='d_kv',
    )(acc0, x, e, um_hist, own, recv, wkv, hist)


def terms_body(added, slot_of, places_ref, lhs_ref, rhs_ref, *refs):
    recv, outs = refs[:4 * added], refs[-4:]
    step = pl.program_id(0)
    val = tn(lhs_ref[0], rhs_ref[0])
    for slot in range(4):
        @pl.when(slot_of(step) == slot)
        def _():
            outs[slot][0] = val + recv[slot][0] if added else val


def terms(lhs, rhs, rows, cols, places, plan, chips, recv):
    tokens = lhs.shape[1]
    first, second = chips
    lhs_at, rhs_at, slot_of, turns = plan

    def rel(r):
        return first + r * (second - first)

    slots = [pl.BlockSpec((1, rows, cols), lambda i, p, at=at: (jnp.clip(i - at, 0, 1), 0, 0)) for at in turns]
    out = pl.pallas_call(
        functools.partial(terms_body, len(recv) // 4, slot_of),
        grid_spec=pltpu.PrefetchScalarGridSpec(
            num_scalar_prefetch=1, grid=(8,),
            in_specs=[pl.BlockSpec((1, tokens, rows), lambda i, p: lhs_at(i, rel, p)),
                      pl.BlockSpec((1, tokens, cols), lambda i, p: rhs_at(i, p))] + slots[:len(recv)],
            out_specs=slots),
        out_shape=[jax.ShapeDtypeStruct((2, rows, cols), F32)] * 4,
        compiler_params=pltpu.CompilerParams(dimension_semantics=('arbitrary',), vmem_limit_bytes=VMEM_ALL),
        cost_estimate=pl.CostEstimate(flops=16 * tokens * rows * cols, bytes_accessed=24 * tokens * rows, transcendentals=0),
    )(places, lhs, rhs, *recv)
    return {first: out[:2], second: out[2:]}


ATTN_PLAN = (lambda i, rel, p: (jnp.where(i < 4, i % 2, i // 2), 0, rel(jnp.where(i < 4, i // 2, i % 2))),
             lambda i, p: (i // 6, 0, p[0]),
             lambda i: jnp.where(i < 4, 2 * (i // 2), 2 * (i % 2) + 1),
             (0, 5, 2, 6))
UP_PLAN = (lambda i, rel, p: (0, 0, 4 * p[1 + rel((i // 2) % 2)] + 2 * p[0] + i % 2),
           lambda i, p: (0, 0, i // 4),
           lambda i: 2 * ((i // 2) % 2) + i // 4,
           (0, 4, 2, 6))


def summed_terms(lhs, rhs, rows, cols, places, plan):
    def in_turn(where, done):
        return lax.optimization_barrier((where, done))[0] if done else where

    sent, total = {}, {}
    where, done = places[1], []
    for pair in ((3, 1), (2, 0)):
        out = terms(lhs, rhs, rows, cols, in_turn(where, done), plan, pair, [])
        done = [v for ab in out.values() for v in ab]
        sent.update({r: [pp_d(v) for v in ab] for r, ab in out.items()})
    where, done = places[0], []
    for pair in ((3, 1), (2, 0)):
        out = terms(lhs, rhs, rows, cols, in_turn(where, done), plan, pair, sent[pair[0]] + sent[pair[1]])
        done = [v for ab in out.values() for v in ab]
        total.update(out)
    return total


GELU_C = 0.7978845608028654
GELU_A = 0.044715
BLOCK_F = 768
ROWS = (slice(0, 256), slice(256, 512))


def mlp_fwd_body(*refs):
    x0_ref, e_ref, ctx_ref, wo_ref, w1_ref, w2_ref = refs[:6]
    z_ref, g_ref, x_ref, h_ref, m_ref, acc_ref = refs[-6:]
    j = pl.program_id(0)

    @pl.when(j == 0)
    def _():
        for rows in ROWS:
            s = x0_ref[rows, :].astype(F32) + e_ref[...]
            h = (s + nn(ctx_ref[0, 0, rows, :], wo_ref[...])).astype(BF16)
            h_ref[rows, :] = h
            hf = h.astype(F32)
            acc_ref[rows, :] = hf
            m_ref[0, rows, :] = (hf * lax.rsqrt(jnp.mean(hf * hf, axis=-1, keepdims=True) + EPS_NORM)).astype(BF16)

    for rows in ROWS:
        z = nt(m_ref[0, rows, :], w1_ref[...]).astype(BF16)
        z_ref[rows, :] = z
        zf = z.astype(F32)
        t = jnp.tanh(zf * (GELU_C + (GELU_A * GELU_C) * (zf * zf)))
        half = 0.5 * zf
        g_ref[0, rows, :] = (half + half * t).astype(BF16)
    for rows in ROWS:
        acc_ref[rows, :] += nn(g_ref[0, rows, :], w2_ref[...])

    @pl.when(j == pl.num_programs(0) - 1)
    def _():
        x_ref[...] = acc_ref[...].astype(BF16)


def mlp_fwd(x, e, ctx_hist, wo, w1t, w2, layer, layers, hist):
    t, dim = x.shape
    hidden = w2.shape[0]
    whole = pl.BlockSpec((t, dim), lambda j: (0, 0))
    slab = pl.BlockSpec((1, t, dim), lambda j: (layer, 0, 0))
    wblk = pl.BlockSpec((BLOCK_F, dim), lambda j: (j, 0))
    extra = [] if hist is None else [hist]
    return pl.pallas_call(
        mlp_fwd_body,
        grid=(hidden // BLOCK_F,),
        in_specs=[whole, pl.BlockSpec((1, dim), lambda j: (0, 0)), pl.BlockSpec((1, 1, t, dim), lambda j: (3, layer, 0, 0)),
                  pl.BlockSpec((dim, dim), lambda j: (0, 0)), wblk, wblk]
        + [pl.BlockSpec(memory_space=pl.ANY)] * len(extra),
        out_specs=[pl.BlockSpec((t, BLOCK_F), lambda j: (0, j)),
                   pl.BlockSpec((1, t, BLOCK_F), lambda j: (j, 0, 0)), whole, whole, slab],
        out_shape=[jax.ShapeDtypeStruct((t, hidden), BF16),
                   jax.ShapeDtypeStruct((hidden // BLOCK_F, t, BLOCK_F), BF16),
                   jax.ShapeDtypeStruct((t, dim), BF16), jax.ShapeDtypeStruct((t, dim), BF16),
                   jax.ShapeDtypeStruct((layers, t, dim), BF16)],
        scratch_shapes=[pltpu.VMEM((t, dim), F32)],
        input_output_aliases={6: 4} if extra else {},
        compiler_params=pltpu.CompilerParams(dimension_semantics=('arbitrary',), vmem_limit_bytes=VMEM_ALL),
        cost_estimate=pl.CostEstimate(flops=4 * t * dim * hidden, bytes_accessed=4 * dim * hidden + 4 * t * hidden,
                                      transcendentals=t * hidden),
        name='mlp_fwd',
    )(x, e, ctx_hist, wo, w1t, w2, *extra)


BLOCK_B = 1024
SUB_B = 512


def mlp_bwd_body(*refs):
    d_ref, h_hbm, z_ref, wo_hbm, w1_ref, w2_ref = refs[:6]
    up_ref, mid_ref, dctx_ref, acc_ref, h_ref, wo_ref, sems = refs[-7:]
    j = pl.program_id(0)
    late = [pltpu.make_async_copy(h_hbm, h_ref, sems.at[0]), pltpu.make_async_copy(wo_hbm, wo_ref, sems.at[1])]

    @pl.when(j == 0)
    def _():
        for copy in late:
            copy.start()
        acc_ref[...] = jnp.zeros_like(acc_ref)

    for i in range(0, BLOCK_B, SUB_B):
        cols = slice(i, i + SUB_B)
        for rows in ROWS:
            da = nt(d_ref[rows, :], w2_ref[cols, :]).astype(BF16).astype(F32)
            zf = z_ref[rows, cols].astype(F32)
            z2 = zf * zf
            t = jnp.tanh(zf * (GELU_C + (GELU_A * GELU_C) * z2))
            slope = (1.0 + t) * (0.5 + (1.0 - t) * (zf * (0.5 * GELU_C + (1.5 * GELU_A * GELU_C) * z2)))
            up_ref[0, rows, cols] = (da * slope).astype(BF16)
    for rows in ROWS:
        acc_ref[rows, :] += nn(up_ref[0, rows, :], w1_ref[...])

    @pl.when(j == pl.num_programs(0) - 1)
    def _():
        for copy in late:
            copy.wait()
        for rows in ROWS:
            dn = acc_ref[rows, :].astype(BF16).astype(F32)
            hf = h_ref[rows, :].astype(F32)
            inv = lax.rsqrt(jnp.mean(hf * hf, axis=-1, keepdims=True) + EPS_NORM)
            proj = jnp.mean(hf * dn, axis=-1, keepdims=True)
            mid = (d_ref[rows, :].astype(F32) + inv * dn - hf * (inv * inv * inv * proj)).astype(BF16)
            mid_ref[0, 0, rows, :] = mid
            dctx_ref[rows, :] = nt(mid, wo_ref[...]).astype(BF16)


def mlp_bwd(d_next, h, z, wo, w1t, w2, layer, layers, um_hist, hist):
    t, dim = h.shape
    hidden = w2.shape[0]
    whole = pl.BlockSpec((t, dim), lambda j: (0, 0))
    hbm = pl.BlockSpec(memory_space=pl.ANY)
    wblk = pl.BlockSpec((BLOCK_B, dim), lambda j: (j, 0))
    extra = [um_hist] if hist is None else [um_hist, hist]
    return pl.pallas_call(
        mlp_bwd_body,
        grid=(hidden // BLOCK_B,),
        in_specs=[whole, hbm, pl.BlockSpec((t, BLOCK_B), lambda j: (0, j)), hbm, wblk, wblk]
        + [pl.BlockSpec(memory_space=pl.ANY)] * len(extra),
        out_specs=[pl.BlockSpec((1, t, BLOCK_B), lambda j: (layer, 0, j)), pl.BlockSpec((1, 1, t, dim), lambda j: (1, layer, 0, 0)), whole],
        out_shape=[jax.ShapeDtypeStruct((layers, t, hidden), BF16), jax.ShapeDtypeStruct((2, layers, t, dim), BF16),
                   jax.ShapeDtypeStruct((t, dim), BF16)],
        scratch_shapes=[pltpu.VMEM((t, dim), F32), pltpu.VMEM((t, dim), BF16), pltpu.VMEM((dim, dim), BF16),
                        pltpu.SemaphoreType.DMA((2,))],
        input_output_aliases={6: 1} if hist is None else {6: 1, 7: 0},
        compiler_params=pltpu.CompilerParams(dimension_semantics=('arbitrary',), vmem_limit_bytes=VMEM_ALL),
        cost_estimate=pl.CostEstimate(flops=4 * t * dim * hidden, bytes_accessed=4 * dim * hidden + 4 * t * hidden,
                                      transcendentals=t * hidden),
        name='mlp_bwd',
    )(d_next, h, z, wo, w1t, w2, *extra)


def join_body(count, core_ref, *refs):
    for n in range(count):
        own, other, out = refs[n], refs[count + n], refs[2 * count + n]
        for i, src in enumerate((own, other)):
            @pl.when(pl.program_id(0) == i)
            def _():
                out[...] = src[...]


def join_call(core, body, grid, own, other, in_specs, out_specs, out_shape):
    size = sum(v.size for v in own)
    return pl.pallas_call(
        body,
        grid_spec=pltpu.PrefetchScalarGridSpec(num_scalar_prefetch=1, grid=grid, in_specs=in_specs * 2, out_specs=out_specs),
        out_shape=out_shape,
        compiler_params=pltpu.CompilerParams(dimension_semantics=('arbitrary', 'arbitrary'), vmem_limit_bytes=VMEM_ALL),
        cost_estimate=pl.CostEstimate(flops=8 * size, bytes_accessed=16 * size, transcendentals=0),
    )(core.reshape(1), *own, *other)


def join(core, own, other):
    rows, cols = own.shape[0] // 4, own.shape[1]
    block = pl.BlockSpec((rows, cols), lambda i, j, c: (j, 0))
    return join_call(core, functools.partial(join_body, 1), (2, 4), [own], [other], [block],
                     pl.BlockSpec((rows, cols), lambda i, j, c: (4 * ((c[0] + i) % 2) + j, 0)),
                     jax.ShapeDtypeStruct((8 * rows, cols), F32))


def join_attn_body(core_ref, own_a, own_b, sib_a, sib_b, q_ref, k_ref, v_ref, o_ref):
    for i, (a_ref, b_ref) in enumerate(((own_a, own_b), (sib_a, sib_b))):
        @pl.when(pl.program_id(0) == i)
        def _():
            q_ref[...] = a_ref[0].T
            k_ref[...] = a_ref[1].T
            v_ref[...] = b_ref[0].T
            o_ref[...] = b_ref[1]


def join_attn(core, own, other):
    _, hid, half_d = own[0].shape
    block = pl.BlockSpec((2, hid, half_d), lambda i, j, c: (0, 0, 0))
    tall = pl.BlockSpec((half_d, hid), lambda i, j, c: ((c[0] + i) % 2, 0))
    wide = pl.BlockSpec((hid, half_d), lambda i, j, c: (0, (c[0] + i) % 2))
    return join_call(core, join_attn_body, (2, 1), list(own), list(other), [block] * 2, [tall] * 3 + [wide],
                     [jax.ShapeDtypeStruct((2 * half_d, hid), F32)] * 3 + [jax.ShapeDtypeStruct((hid, 2 * half_d), F32)])


def join_flip_body(core_ref, oa_ref, ob_ref, sa_ref, sb_ref, out_ref):
    for i, srcs in enumerate(((oa_ref, ob_ref), (sa_ref, sb_ref))):
        for j, src in enumerate(srcs):
            @pl.when((pl.program_id(0) == i) & (pl.program_id(1) == j))
            def _():
                out_ref[...] = src[...].T


def join_flip(core, own, other):
    rows, cols = own[0].shape
    block = pl.BlockSpec((rows, cols), lambda i, j, c: (0, 0))
    return join_call(core, join_flip_body, (2, 2), own, other, [block] * 2,
                     pl.BlockSpec((cols, rows), lambda i, j, c: (j, (c[0] + i) % 2)),
                     jax.ShapeDtypeStruct((2 * cols, 2 * rows), F32))


def gather_pieces(part_a, part_b):
    xa, xb = pp_x(part_a), pp_x(part_b)
    ya, yb = pp_y(part_a), pp_y(part_b)
    da, db = pp_y(xa), pp_x(yb)
    own = [(xa, xb), (ya, yb), (da, db)]
    return own, [(pp_d(a), pp_d(b)) for a, b in own]


def reduce_terms(total, pp_first, pp_second, first, second):
    here, there = pp_first(total[first]), pp_first(total[3])
    last = pp_second(total[second] + there)
    return total[0] + here + last


BOTH = ('model', 'data')


def solution(mesh):
    spec_col = P(None, 'model')
    spec_row = P('model', None)
    spec_act = P('data', None, None)
    spec_rep = P(None, None)

    def device_step(x_in, cot_out, step_emb, w_q, w_k, w_v, w_o, w_1, w_2):
        layer_count, dim = step_emb.shape
        core = lax.axis_index('data')
        chip = lax.axis_index('model')
        chip_x = lax.rem(chip, 2)
        chip_y = lax.div(chip, 2)
        nbr_x = chip + 1 - 2 * chip_x
        nbr_y = lax.rem(chip + 2, 4)
        diag = lax.rem(nbr_x + 2, 4)
        chips = (chip, nbr_x, nbr_y, diag)
        hid = w_q.shape[1]
        half_d = dim // 2
        half_t = x_in.shape[1] // 2

        def take(v, which, axis, size):
            return lax.dynamic_slice_in_dim(v, which * size, size, axis)

        def put(buf, v, which, axis):
            return lax.dynamic_update_slice_in_dim(buf, v, which * v.shape[axis], axis)

        def gather(v):
            return lax.all_gather(v, BOTH, axis=0, tiled=True)

        def after(v, *deps):
            return lax.optimization_barrier((v,) + deps)[0]

        def my_tokens(v):
            mine = lax.dynamic_index_in_dim(v, chip_x, 0, keepdims=False)
            half = mine.shape[0] // 2
            recv = pp_d(take(mine, 1 - core, 0, half))
            return jnp.where(core == chip_y, take(mine, core, 0, half), recv)

        def gather_permuted(local):
            own = take(local, core, 0, local.shape[0] // 2)
            rows = own.shape[0] // 2
            p_own, p_sib = gather_pieces(own[:rows], own[rows:])
            full = put(jnp.zeros((4 * local.shape[0], dim), BF16), local, chip, 0)
            for r in (1, 2, 3):
                for part in (0, 1):
                    full = put(full, p_own[r - 1][part], 4 * chips[r] + 2 * core + part, 0)
                    full = put(full, p_sib[r - 1][part], 4 * chips[r] + 2 * (1 - core) + part, 0)
            return full

        x_cur = my_tokens(x_in)
        qkv_t = jnp.concatenate([w_q, w_k, w_v], axis=1).T
        qkv_all = gather(take(qkv_t, core, 0, qkv_t.shape[0] // 2))
        o_all = gather(take(w_o, core, 0, hid // 2))
        w2 = gather_permuted(w_2)
        w1 = gather_permuted(w_1.T)
        wq = jnp.concatenate([take(qkv_all, 3 * c, 0, hid) for c in chips], axis=0)
        wkv = jnp.concatenate([take(qkv_all, 3 * c + i, 0, hid) for i in (1, 2) for c in chips], axis=0)
        wo = jnp.concatenate([take(o_all, c, 0, hid) for c in chips], axis=0)
        d_cur = my_tokens(cot_out)
        emb = step_emb.astype(F32)

        saved = []
        g_mine = []
        um_hist = m_hist = att_hist = None
        for layer in range(layer_count):
            e = emb[layer:layer + 1]
            kv, um_hist = norm_kv(x_cur, e, wkv, layer, layer_count, um_hist)
            kv_s = pp_d(kv)
            q = nt(um_hist[0, layer], wq).astype(BF16)
            att_hist, lse = attn_fwd(q, kv, kv_s, layer, layer_count, att_hist)
            z, g, x_next, h, m_hist = mlp_fwd(x_cur, e, att_hist, wo, w1, w2, layer, layer_count, m_hist)
            g_mine.append(lax.all_to_all(g.reshape(-1, g.shape[-1]), BOTH, split_axis=0, concat_axis=0, tiled=True))
            saved.append((x_cur, q, kv, kv_s, lse, h, z))
            x_cur = x_next

        def flat(v, lead):
            return v.reshape(lead, -1, v.shape[-1])

        places = [jnp.stack([w, *chips]).astype(jnp.int32) for w in (core, 1 - core)]
        up_hist = None
        next_all = [None] * layer_count
        for layer in reversed(range(layer_count)):
            x_l, q, kv, kv_s, lse, h, z = saved[layer]
            e = emb[layer:layer + 1]
            d_next = d_cur
            if layer < layer_count - 1:
                next_all[layer] = gather(d_next)
            up_hist, um_hist, d_ctx = mlp_bwd(d_next, h, z, wo, w1, w2, layer, layer_count, um_hist, up_hist)
            if layer == 0:
                total = summed_terms(flat(up_hist, 1), flat(m_hist, 1), hid, half_d, places, UP_PLAN)
                d_ctx = after(d_ctx, *[v for r in (1, 2, 3) for v in total[r]])
                own_1a = reduce_terms({r: v[0] for r, v in total.items()}, pp_x, pp_y, 1, 2)
                own_1b = reduce_terms({r: v[1] for r, v in total.items()}, pp_y, pp_x, 2, 1)
            att_hist, own_kv, sib_kv = attn_bwd(q, kv, kv_s, d_ctx, lse, layer, layer_count, att_hist)
            recv_kv = pp_d(sib_kv)
            acc0 = nn(att_hist[0, layer], wq)
            att_hist, d_cur = d_kv(acc0, x_l, e, um_hist, own_kv, recv_kv, wkv, layer, layer_count, att_hist)

        total = summed_terms(flat(att_hist, 4), flat(um_hist, 2), hid, half_d, places, ATTN_PLAN)
        own_qk = reduce_terms({r: v[0] for r, v in total.items()}, pp_x, pp_y, 1, 2)
        own_vo = reduce_terms({r: v[1] for r, v in total.items()}, pp_y, pp_x, 2, 1)

        at_home = chip_y == core
        to_row = [(2 * c + d, 2 * (c ^ 2) + d) for c in range(4) for d in range(2) if c // 2 == d]
        in_row = [(2 * c + d, 2 * (c ^ 1) + d) for c in range(4) for d in range(2) if c // 2 == d]

        def in_order(mine, other):
            return jnp.where(chip_x == 0, mine, other), jnp.where(chip_x == 0, other, mine)

        other_half = pp_d(d_cur)
        part_p = jnp.where(core == 0, d_cur, other_half)
        part_q = jnp.where(core == 0, other_half, d_cur)
        p_y = lax.ppermute(part_p, BOTH, to_row)
        q_x = lax.ppermute(part_q, BOTH, in_row)
        p_row = jnp.where(at_home, part_p, p_y)
        q_row = jnp.concatenate(in_order(part_q, q_x), axis=0)
        p_x = pp_x(p_row)
        q_y = lax.ppermute(q_row, BOTH, to_row)
        q_both = jnp.where(at_home, q_row, q_y)
        p_0, p_1 = in_order(p_row, p_x)
        d_x = jnp.concatenate([p_0, q_both[:half_t], p_1, q_both[half_t:]], axis=0).reshape(2, -1, dim)

        ready = tuple(v for ab in total.values() for v in ab)
        cot_mine = cot_out.reshape(-1, dim)
        cot_other = pp_d(cot_mine)
        grad_2 = None
        for layer in reversed(range(layer_count)):
            g_all = after(g_mine[layer], *ready)
            if layer == layer_count - 1:
                rows = g_all.shape[0] // 2
                grad_2 = tn(take(g_all, core, 0, rows), cot_mine) + tn(take(g_all, 1 - core, 0, rows), cot_other)
            else:
                grad_2 = grad_2 + tn(g_all, next_all[layer])

        grad_2 = join(core, grad_2, pp_d(grad_2))
        own_1 = [v.reshape(-1, half_d) for v in (own_1a, own_1b)]
        grad_1 = join_flip(core, own_1, [pp_d(v) for v in own_1])
        gq, gk, gv, go = join_attn(core, (own_qk, own_vo), (pp_d(own_qk), pp_d(own_vo)))
        return gq, gk, gv, go, grad_1, grad_2, d_x

    return jax.shard_map(device_step, mesh=mesh,
                         in_specs=(spec_act, spec_act, spec_rep, spec_col, spec_col, spec_col, spec_row, spec_col, spec_row),
                         out_specs=(spec_col, spec_col, spec_col, spec_row, spec_col, spec_row, spec_act),
                         check_vma=False)
```

```python
import functools

import jax
import jax.numpy as jnp
from jax import lax
from jax.experimental import pallas as pl
from jax.experimental.pallas import tpu as pltpu
from jax.sharding import PartitionSpec as P


HEAD_DIM = 64
EPS_NORM = 1e-6
F32 = jnp.float32
BF16 = jnp.bfloat16
LOG2E = 1.4426950408889634
VMEM_ALL = 60 * 1024 * 1024
SCALE = HEAD_DIM ** -0.5

SWAP_D = [(0, 1), (1, 0)]


SWAP_X = [(0, 1), (1, 0), (2, 3), (3, 2)]
SWAP_Y = [(0, 2), (2, 0), (1, 3), (3, 1)]


def pp_x(v):
    return lax.ppermute(v, 'model', SWAP_X)


def pp_y(v):
    return lax.ppermute(v, 'model', SWAP_Y)


def pp_d(v):
    return lax.ppermute(v, 'data', SWAP_D)


def dot(a, b, dims):
    return lax.dot_general(a, b, (dims, ((), ())), preferred_element_type=F32)


def nn(a, b):
    return dot(a, b, ((1,), (0,)))


def nt(a, b):
    return dot(a, b, ((1,), (1,)))


def tn(a, b):
    return dot(a, b, ((0,), (0,)))


def pair_masks(rows):
    lane = lax.broadcasted_iota(jnp.int32, (rows, 128), 1)
    return lane < HEAD_DIM


CHUNK = 256
WIDE = 256


def masked_pair(q):
    low = pair_masks(CHUNK)
    zero = jnp.zeros_like(q)
    return jnp.concatenate([jnp.where(low, q, zero), jnp.where(low, zero, q)], axis=0)


def attn_fwd_body(*refs):
    q_ref, qn_ref, ko_ref, ks_ref, kno_ref, kns_ref, vo_ref, vs_ref = refs[:8]
    ctx_ref, lse_ref, a_ref, ma_ref = refs[-4:]
    units = [(sub, i) for sub in range(WIDE // 128) for i in range(q_ref.shape[0] // CHUNK)]

    def joined(own_ref, sib_ref, sub):
        cols = slice(sub * 128, (sub + 1) * 128)
        return jnp.concatenate([own_ref[:, cols], sib_ref[:, cols]], axis=0)

    def scores(ko, ks, q, sub, i):
        s = nt(joined(ko, ks, sub), masked_pair(q[i * CHUNK:(i + 1) * CHUNK, sub * 128:(sub + 1) * 128]))
        return s, jnp.max(s, axis=0, keepdims=True)

    @pl.when(pl.program_id(0) == 0)
    def _():
        a_ref[...], ma_ref[...] = scores(ko_ref, ks_ref, q_ref, 0, 0)

    s, m = a_ref[...], ma_ref[...]
    for n, (sub, i) in enumerate(units):
        if n + 1 < len(units):
            ahead = scores(ko_ref, ks_ref, q_ref, *units[n + 1])
        else:
            ahead = scores(kno_ref, kns_ref, qn_ref, 0, 0)
        rows, cols = slice(i * CHUNK, (i + 1) * CHUNK), slice(sub * 128, (sub + 1) * 128)
        p = jnp.exp2((s - m) * (SCALE * LOG2E))
        l = jnp.sum(p, axis=0, keepdims=True)
        pb = (p * (1.0 / l)).astype(BF16)
        lse = m * (SCALE * LOG2E) + jnp.log2(l)
        lse_ref[sub, 0:1, rows] = lse[:, :CHUNK]
        lse_ref[sub, 1:2, rows] = lse[:, CHUNK:]
        ctx_t = tn(joined(vo_ref, vs_ref, sub), pb)
        ctx_t = jnp.concatenate([ctx_t[:HEAD_DIM, :CHUNK], ctx_t[HEAD_DIM:, CHUNK:]], axis=0)
        ctx_ref[0, 0, rows, cols] = ctx_t.T.astype(BF16)
        s, m = ahead
    a_ref[...], ma_ref[...] = s, m


def attn_fwd(q, kv, kv_s, layer, layers, hist):
    tq, width = q.shape
    tk = kv.shape[0]
    pairs = width // 128
    steps = width // WIDE

    def col(off):
        return lambda j: (0, j + off)

    def nxt(j):
        return (0, jnp.minimum(j + 1, steps - 1))

    extra = [] if hist is None else [hist]
    flops = 2 * 2 * tq * (2 * tk) * 256 * (width // HEAD_DIM)
    return pl.pallas_call(
        attn_fwd_body,
        grid=(steps,),
        in_specs=[pl.BlockSpec((tq, WIDE), col(0)), pl.BlockSpec((tq, WIDE), nxt),
                  pl.BlockSpec((tk, WIDE), col(0)), pl.BlockSpec((tk, WIDE), col(0)),
                  pl.BlockSpec((tk, WIDE), nxt), pl.BlockSpec((tk, WIDE), nxt),
                  pl.BlockSpec((tk, WIDE), col(steps)), pl.BlockSpec((tk, WIDE), col(steps))]
        + [pl.BlockSpec(memory_space=pl.ANY)] * len(extra),
        out_specs=[pl.BlockSpec((1, 1, tq, WIDE), lambda j: (3, layer, 0, j)),
                   pl.BlockSpec((WIDE // 128, 2, tq), lambda j: (j, 0, 0))],
        out_shape=[jax.ShapeDtypeStruct((4, layers, tq, width), BF16),
                   jax.ShapeDtypeStruct((pairs, 2, tq), F32)],
        input_output_aliases={8: 0} if extra else {},
        scratch_shapes=[pltpu.VMEM((2 * tk, 2 * CHUNK), F32), pltpu.VMEM((1, 2 * CHUNK), F32)],
        compiler_params=pltpu.CompilerParams(dimension_semantics=('arbitrary',),
                                             vmem_limit_bytes=VMEM_ALL),
        cost_estimate=pl.CostEstimate(flops=flops, bytes_accessed=2 * (tq * width * 2 + 4 * tk * width),
                                      transcendentals=tq * 2 * tk * (width // HEAD_DIM)),
        name='attn_fwd',
    )(q, q, kv, kv_s, kv, kv_s, kv, kv_s, *extra)


def attn_bwd_body(q_ref, ko_ref, ks_ref, vo_ref, vs_ref, do_ref, lse_ref, hist_ref, dq_ref, down_ref, dsib_ref):
    tk = ko_ref.shape[0]
    low = pair_masks(CHUNK)
    units = [(sub, i, h) for sub in range(WIDE // 128) for i in range(q_ref.shape[0] // CHUNK) for h in range(2)]

    def keys(own_ref, sib_ref, sub):
        cols = slice(sub * 128, (sub + 1) * 128)
        return jnp.concatenate([own_ref[:, cols], sib_ref[:, cols]], axis=0)

    def masked(ref, sub, i, h):
        v = ref[i * CHUNK:(i + 1) * CHUNK, sub * 128:(sub + 1) * 128]
        return jnp.where(low if h == 0 else ~low, v, jnp.zeros_like(v))

    def products(sub, i, h):
        s = nt(keys(ko_ref, ks_ref, sub), masked(q_ref, sub, i, h))
        return s, nt(keys(vo_ref, vs_ref, sub), masked(do_ref, sub, i, h)).astype(BF16)

    dqs = []
    ahead = products(*units[0])
    for n, (sub, i, h) in enumerate(units):
        s, dp = ahead
        if n + 1 < len(units):
            ahead = products(*units[n + 1])
        rows, cols = slice(i * CHUNK, (i + 1) * CHUNK), slice(sub * 128, (sub + 1) * 128)
        p = jnp.exp2(s * (SCALE * LOG2E) - lse_ref[sub, h:h + 1, rows])
        dp = dp.astype(F32)
        delta = jnp.sum(p * dp, axis=0, keepdims=True)
        ds = (p * (dp - delta)).astype(BF16)
        dv = nn(p.astype(BF16), masked(do_ref, sub, i, h))
        dk = nn(ds, masked(q_ref, sub, i, h) * jnp.asarray(SCALE, BF16))
        for m, grad in enumerate((dk, dv)):
            for ref, part in ((down_ref, grad[:tk]), (dsib_ref, grad[tk:])):
                if i == 0 and h == 0:
                    ref[m, :, cols] = part
                else:
                    ref[m, :, cols] += part
        dqs.append(tn(keys(ko_ref, ks_ref, sub), ds)[h * HEAD_DIM:(h + 1) * HEAD_DIM, :] * SCALE)
        if h == 1:
            dq_ref[0, 0, rows, cols] = jnp.concatenate(dqs, axis=0).T.astype(BF16)
            dqs = []


def attn_bwd(q, kv, kv_s, d_ctx, lse, layer, layers, hist):
    tq, width = q.shape
    tk = kv.shape[0]
    steps = width // WIDE

    def col(off):
        return lambda j: (0, j + off)

    flops = 5 * 2 * tq * (2 * tk) * 256 * (width // HEAD_DIM)
    qblk = pl.BlockSpec((tq, WIDE), col(0))
    kblk = pl.BlockSpec((tk, WIDE), col(0))
    vblk = pl.BlockSpec((tk, WIDE), col(steps))
    both = pl.BlockSpec((2, tk, WIDE), lambda j: (0, 0, j))
    return pl.pallas_call(
        attn_bwd_body,
        grid=(steps,),
        in_specs=[qblk, kblk, kblk, vblk, vblk, qblk,
                  pl.BlockSpec((WIDE // 128, 2, tq), lambda j: (j, 0, 0)), pl.BlockSpec(memory_space=pl.ANY)],
        out_specs=[pl.BlockSpec((1, 1, tq, WIDE), lambda j: (0, layer, 0, j)), both, both],
        out_shape=[jax.ShapeDtypeStruct((4, layers, tq, width), BF16)]
        + [jax.ShapeDtypeStruct((2, tk, width), F32)] * 2,
        input_output_aliases={7: 0},
        compiler_params=pltpu.CompilerParams(dimension_semantics=('arbitrary',),
                                             vmem_limit_bytes=VMEM_ALL),
        cost_estimate=pl.CostEstimate(flops=flops, bytes_accessed=2 * (2 * tq * width * 2 + 4 * tk * width) + 16 * tk * width,
                                      transcendentals=tq * 2 * tk * (width // HEAD_DIM)),
        name='attn_bwd',
    )(q, kv, kv_s, kv, kv_s, d_ctx, lse, hist)


def kv_body(*refs):
    x_ref, e_ref, w_ref = refs[:3]
    kv_ref, u_ref = refs[-2:]

    @pl.when(pl.program_id(0) == 0)
    def _():
        s = x_ref[...].astype(F32) + e_ref[...]
        u_ref[0, 0] = (s * lax.rsqrt(jnp.mean(s * s, axis=-1, keepdims=True) + EPS_NORM)).astype(BF16)

    for rows in ROWS:
        kv_ref[rows, :] = nt(u_ref[0, 0, rows, :], w_ref[...]).astype(BF16)


def norm_kv(x, e, wkv, layer, layers, hist):
    t, dim = x.shape
    width = wkv.shape[0]
    blk = 1024
    extra = [] if hist is None else [hist]
    return pl.pallas_call(
        kv_body,
        grid=(width // blk,),
        in_specs=[pl.BlockSpec((t, dim), lambda j: (0, 0)), pl.BlockSpec((1, dim), lambda j: (0, 0)),
                  pl.BlockSpec((blk, dim), lambda j: (j, 0))] + [pl.BlockSpec(memory_space=pl.ANY)] * len(extra),
        out_specs=[pl.BlockSpec((t, blk), lambda j: (0, j)), pl.BlockSpec((1, 1, t, dim), lambda j: (0, layer, 0, 0))],
        out_shape=[jax.ShapeDtypeStruct((t, width), BF16), jax.ShapeDtypeStruct((2, layers, t, dim), BF16)],
        input_output_aliases={3: 1} if extra else {},
        compiler_params=pltpu.CompilerParams(dimension_semantics=('arbitrary',), vmem_limit_bytes=VMEM_ALL),
        cost_estimate=pl.CostEstimate(flops=2 * t * dim * width, bytes_accessed=2 * (dim * width + t * width + 2 * t * dim),
                                      transcendentals=t),
        name='norm_kv',
    )(x, e, wkv, *extra)


def d_kv_body(layer, acc0_hbm, x_hbm, e_ref, um_hbm, own_ref, recv_ref, w_ref, hist_ref, dkv_ref, prev_ref,
              acc_ref, acc0_ref, x_ref, mid_ref, sems):
    j = pl.program_id(0)
    late = [pltpu.make_async_copy(src, dst, sems.at[n])
            for n, (src, dst) in enumerate(((acc0_hbm, acc0_ref), (x_hbm, x_ref), (um_hbm.at[1, layer], mid_ref)))]

    @pl.when(j == 0)
    def _():
        for copy in late:
            copy.start()
        acc_ref[...] = jnp.zeros_like(acc_ref)

    dkv_ref[0, 0] = (own_ref[0] + recv_ref[0]).astype(BF16)
    for rows in ROWS:
        acc_ref[rows, :] += nn(dkv_ref[0, 0, rows, :], w_ref[...])

    @pl.when(j == pl.num_programs(0) - 1)
    def _():
        for copy in late:
            copy.wait()
        dn = (acc_ref[...] + acc0_ref[...]).astype(BF16).astype(F32)
        s = x_ref[...].astype(F32) + e_ref[...]
        inv = lax.rsqrt(jnp.mean(s * s, axis=-1, keepdims=True) + EPS_NORM)
        proj = jnp.mean(s * dn, axis=-1, keepdims=True)
        prev_ref[...] = (mid_ref[...].astype(F32) + inv * dn - s * (inv * inv * inv * proj)).astype(BF16)


def d_kv(acc0, x, e, um_hist, own, recv, wkv, layer, layers, hist):
    t, dim = x.shape
    half = dim // 2
    hbm = pl.BlockSpec(memory_space=pl.ANY)
    gblk = pl.BlockSpec((1, t, half), lambda j: (j // 2, 0, j % 2))
    return pl.pallas_call(
        functools.partial(d_kv_body, layer),
        grid=(4,),
        in_specs=[hbm, hbm, pl.BlockSpec((1, dim), lambda j: (0, 0)), hbm, gblk, gblk,
                  pl.BlockSpec((half, dim), lambda j: (j, 0)), hbm],
        out_specs=[pl.BlockSpec((1, 1, t, half), lambda j: (1 + j // 2, layer, 0, j % 2)),
                   pl.BlockSpec((t, dim), lambda j: (0, 0))],
        out_shape=[jax.ShapeDtypeStruct((4, layers, t, dim), BF16), jax.ShapeDtypeStruct((t, dim), BF16)],
        scratch_shapes=[pltpu.VMEM((t, dim), F32), pltpu.VMEM((t, dim), F32), pltpu.VMEM((t, dim), BF16),
                        pltpu.VMEM((t, dim), BF16), pltpu.SemaphoreType.DMA((3,))],
        input_output_aliases={7: 0},
        compiler_params=pltpu.CompilerParams(dimension_semantics=('arbitrary',), vmem_limit_bytes=VMEM_ALL),
        cost_estimate=pl.CostEstimate(flops=4 * t * dim * dim, bytes_accessed=4 * dim * dim + 20 * t * dim, transcendentals=t),
        name='d_kv',
    )(acc0, x, e, um_hist, own, recv, wkv, hist)


def terms_body(added, slot_of, places_ref, lhs_ref, rhs_ref, *refs):
    recv, outs = refs[:4 * added], refs[-4:]
    step = pl.program_id(0)
    val = tn(lhs_ref[0], rhs_ref[0])
    for slot in range(4):
        @pl.when(slot_of(step) == slot)
        def _():
            outs[slot][0] = val + recv[slot][0] if added else val


def terms(lhs, rhs, rows, cols, places, plan, chips, recv):
    tokens = lhs.shape[1]
    first, second = chips
    lhs_at, rhs_at, slot_of, turns = plan

    def rel(r):
        return first + r * (second - first)

    slots = [pl.BlockSpec((1, rows, cols), lambda i, p, at=at: (jnp.clip(i - at, 0, 1), 0, 0)) for at in turns]
    out = pl.pallas_call(
        functools.partial(terms_body, len(recv) // 4, slot_of),
        grid_spec=pltpu.PrefetchScalarGridSpec(
            num_scalar_prefetch=1, grid=(8,),
            in_specs=[pl.BlockSpec((1, tokens, rows), lambda i, p: lhs_at(i, rel, p)),
                      pl.BlockSpec((1, tokens, cols), lambda i, p: rhs_at(i, p))] + slots[:len(recv)],
            out_specs=slots),
        out_shape=[jax.ShapeDtypeStruct((2, rows, cols), F32)] * 4,
        compiler_params=pltpu.CompilerParams(dimension_semantics=('arbitrary',), vmem_limit_bytes=VMEM_ALL),
        cost_estimate=pl.CostEstimate(flops=16 * tokens * rows * cols, bytes_accessed=24 * tokens * rows, transcendentals=0),
    )(places, lhs, rhs, *recv)
    return {first: out[:2], second: out[2:]}


ATTN_PLAN = (lambda i, rel, p: (jnp.where(i < 4, i % 2, i // 2), 0, rel(jnp.where(i < 4, i // 2, i % 2))),
             lambda i, p: (i // 6, 0, p[0]),
             lambda i: jnp.where(i < 4, 2 * (i // 2), 2 * (i % 2) + 1),
             (0, 5, 2, 6))
UP_PLAN = (lambda i, rel, p: (0, 0, 4 * p[1 + rel((i // 2) % 2)] + 2 * p[0] + i % 2),
           lambda i, p: (0, 0, i // 4),
           lambda i: 2 * ((i // 2) % 2) + i // 4,
           (0, 4, 2, 6))


def summed_terms(lhs, rhs, rows, cols, places, plan):
    def in_turn(where, done):
        return lax.optimization_barrier((where, done))[0] if done else where

    sent, total = {}, {}
    where, done = places[1], []
    for pair in ((3, 1), (2, 0)):
        out = terms(lhs, rhs, rows, cols, in_turn(where, done), plan, pair, [])
        done = [v for ab in out.values() for v in ab]
        sent.update({r: [pp_d(v) for v in ab] for r, ab in out.items()})
    where, done = places[0], []
    for pair in ((3, 1), (2, 0)):
        out = terms(lhs, rhs, rows, cols, in_turn(where, done), plan, pair, sent[pair[0]] + sent[pair[1]])
        done = [v for ab in out.values() for v in ab]
        total.update(out)
    return total


GELU_C = 0.7978845608028654
GELU_A = 0.044715
BLOCK_F = 768
ROWS = (slice(0, 256), slice(256, 512))


def mlp_fwd_body(*refs):
    x0_ref, e_ref, ctx_ref, wo_ref, w1_ref, w2_ref = refs[:6]
    z_ref, g_ref, x_ref, h_ref, m_ref, acc_ref = refs[-6:]
    j = pl.program_id(0)

    @pl.when(j == 0)
    def _():
        for rows in ROWS:
            s = x0_ref[rows, :].astype(F32) + e_ref[...]
            h = (s + nn(ctx_ref[0, 0, rows, :], wo_ref[...])).astype(BF16)
            h_ref[rows, :] = h
            hf = h.astype(F32)
            acc_ref[rows, :] = hf
            m_ref[0, rows, :] = (hf * lax.rsqrt(jnp.mean(hf * hf, axis=-1, keepdims=True) + EPS_NORM)).astype(BF16)

    for rows in ROWS:
        z = nt(m_ref[0, rows, :], w1_ref[...]).astype(BF16)
        z_ref[rows, :] = z
        zf = z.astype(F32)
        t = jnp.tanh(zf * (GELU_C + (GELU_A * GELU_C) * (zf * zf)))
        half = 0.5 * zf
        g_ref[0, rows, :] = (half + half * t).astype(BF16)
    for rows in ROWS:
        acc_ref[rows, :] += nn(g_ref[0, rows, :], w2_ref[...])

    @pl.when(j == pl.num_programs(0) - 1)
    def _():
        x_ref[...] = acc_ref[...].astype(BF16)


def mlp_fwd(x, e, ctx_hist, wo, w1t, w2, layer, layers, hist):
    t, dim = x.shape
    hidden = w2.shape[0]
    whole = pl.BlockSpec((t, dim), lambda j: (0, 0))
    slab = pl.BlockSpec((1, t, dim), lambda j: (layer, 0, 0))
    wblk = pl.BlockSpec((BLOCK_F, dim), lambda j: (j, 0))
    extra = [] if hist is None else [hist]
    return pl.pallas_call(
        mlp_fwd_body,
        grid=(hidden // BLOCK_F,),
        in_specs=[whole, pl.BlockSpec((1, dim), lambda j: (0, 0)), pl.BlockSpec((1, 1, t, dim), lambda j: (3, layer, 0, 0)),
                  pl.BlockSpec((dim, dim), lambda j: (0, 0)), wblk, wblk]
        + [pl.BlockSpec(memory_space=pl.ANY)] * len(extra),
        out_specs=[pl.BlockSpec((t, BLOCK_F), lambda j: (0, j)),
                   pl.BlockSpec((1, t, BLOCK_F), lambda j: (j, 0, 0)), whole, whole, slab],
        out_shape=[jax.ShapeDtypeStruct((t, hidden), BF16),
                   jax.ShapeDtypeStruct((hidden // BLOCK_F, t, BLOCK_F), BF16),
                   jax.ShapeDtypeStruct((t, dim), BF16), jax.ShapeDtypeStruct((t, dim), BF16),
                   jax.ShapeDtypeStruct((layers, t, dim), BF16)],
        scratch_shapes=[pltpu.VMEM((t, dim), F32)],
        input_output_aliases={6: 4} if extra else {},
        compiler_params=pltpu.CompilerParams(dimension_semantics=('arbitrary',), vmem_limit_bytes=VMEM_ALL),
        cost_estimate=pl.CostEstimate(flops=4 * t * dim * hidden, bytes_accessed=4 * dim * hidden + 4 * t * hidden,
                                      transcendentals=t * hidden),
        name='mlp_fwd',
    )(x, e, ctx_hist, wo, w1t, w2, *extra)


BLOCK_B = 1024
SUB_B = 512


def mlp_bwd_body(*refs):
    d_ref, h_hbm, z_ref, wo_hbm, w1_ref, w2_ref = refs[:6]
    up_ref, mid_ref, dctx_ref, acc_ref, h_ref, wo_ref, sems = refs[-7:]
    j = pl.program_id(0)
    late = [pltpu.make_async_copy(h_hbm, h_ref, sems.at[0]), pltpu.make_async_copy(wo_hbm, wo_ref, sems.at[1])]

    @pl.when(j == 0)
    def _():
        for copy in late:
            copy.start()
        acc_ref[...] = jnp.zeros_like(acc_ref)

    for i in range(0, BLOCK_B, SUB_B):
        cols = slice(i, i + SUB_B)
        for rows in ROWS:
            da = nt(d_ref[rows, :], w2_ref[cols, :]).astype(BF16).astype(F32)
            zf = z_ref[rows, cols].astype(F32)
            z2 = zf * zf
            t = jnp.tanh(zf * (GELU_C + (GELU_A * GELU_C) * z2))
            slope = (1.0 + t) * (0.5 + (1.0 - t) * (zf * (0.5 * GELU_C + (1.5 * GELU_A * GELU_C) * z2)))
            up_ref[0, rows, cols] = (da * slope).astype(BF16)
    for rows in ROWS:
        acc_ref[rows, :] += nn(up_ref[0, rows, :], w1_ref[...])

    @pl.when(j == pl.num_programs(0) - 1)
    def _():
        for copy in late:
            copy.wait()
        for rows in ROWS:
            dn = acc_ref[rows, :].astype(BF16).astype(F32)
            hf = h_ref[rows, :].astype(F32)
            inv = lax.rsqrt(jnp.mean(hf * hf, axis=-1, keepdims=True) + EPS_NORM)
            proj = jnp.mean(hf * dn, axis=-1, keepdims=True)
            mid = (d_ref[rows, :].astype(F32) + inv * dn - hf * (inv * inv * inv * proj)).astype(BF16)
            mid_ref[0, 0, rows, :] = mid
            dctx_ref[rows, :] = nt(mid, wo_ref[...]).astype(BF16)


def mlp_bwd(d_next, h, z, wo, w1t, w2, layer, layers, um_hist, hist):
    t, dim = h.shape
    hidden = w2.shape[0]
    whole = pl.BlockSpec((t, dim), lambda j: (0, 0))
    hbm = pl.BlockSpec(memory_space=pl.ANY)
    wblk = pl.BlockSpec((BLOCK_B, dim), lambda j: (j, 0))
    extra = [um_hist] if hist is None else [um_hist, hist]
    return pl.pallas_call(
        mlp_bwd_body,
        grid=(hidden // BLOCK_B,),
        in_specs=[whole, hbm, pl.BlockSpec((t, BLOCK_B), lambda j: (0, j)), hbm, wblk, wblk]
        + [pl.BlockSpec(memory_space=pl.ANY)] * len(extra),
        out_specs=[pl.BlockSpec((1, t, BLOCK_B), lambda j: (layer, 0, j)), pl.BlockSpec((1, 1, t, dim), lambda j: (1, layer, 0, 0)), whole],
        out_shape=[jax.ShapeDtypeStruct((layers, t, hidden), BF16), jax.ShapeDtypeStruct((2, layers, t, dim), BF16),
                   jax.ShapeDtypeStruct((t, dim), BF16)],
        scratch_shapes=[pltpu.VMEM((t, dim), F32), pltpu.VMEM((t, dim), BF16), pltpu.VMEM((dim, dim), BF16),
                        pltpu.SemaphoreType.DMA((2,))],
        input_output_aliases={6: 1} if hist is None else {6: 1, 7: 0},
        compiler_params=pltpu.CompilerParams(dimension_semantics=('arbitrary',), vmem_limit_bytes=VMEM_ALL),
        cost_estimate=pl.CostEstimate(flops=4 * t * dim * hidden, bytes_accessed=4 * dim * hidden + 4 * t * hidden,
                                      transcendentals=t * hidden),
        name='mlp_bwd',
    )(d_next, h, z, wo, w1t, w2, *extra)


def join_body(count, core_ref, *refs):
    for n in range(count):
        own, other, out = refs[n], refs[count + n], refs[2 * count + n]
        for i, src in enumerate((own, other)):
            @pl.when(pl.program_id(0) == i)
            def _():
                out[...] = src[...]


def join_call(core, body, grid, own, other, in_specs, out_specs, out_shape):
    size = sum(v.size for v in own)
    return pl.pallas_call(
        body,
        grid_spec=pltpu.PrefetchScalarGridSpec(num_scalar_prefetch=1, grid=grid, in_specs=in_specs, out_specs=out_specs),
        out_shape=out_shape,
        compiler_params=pltpu.CompilerParams(dimension_semantics=('arbitrary', 'arbitrary'), vmem_limit_bytes=VMEM_ALL),
        cost_estimate=pl.CostEstimate(flops=8 * size, bytes_accessed=16 * size, transcendentals=0),
    )(core.reshape(1), *own, *other)


def join(core, own, other):
    rows, cols = own.shape[0] // 4, own.shape[1]
    first = pl.BlockSpec((rows, cols), lambda i, j, c: (jnp.where(i == 0, j, 3), 0))
    then = pl.BlockSpec((rows, cols), lambda i, j, c: (jnp.where(i == 0, 0, j), 0))
    return join_call(core, functools.partial(join_body, 1), (2, 4), [own], [other], [first, then],
                     pl.BlockSpec((rows, cols), lambda i, j, c: (4 * ((c[0] + i) % 2) + j, 0)),
                     jax.ShapeDtypeStruct((8 * rows, cols), F32))


def join_attn_body(core_ref, own_a, own_b, sib_a, sib_b, q_ref, k_ref, v_ref, o_ref):
    for i, (a_ref, b_ref) in enumerate(((own_a, own_b), (sib_a, sib_b))):
        @pl.when(pl.program_id(0) == i)
        def _():
            q_ref[...] = a_ref[0].T
            k_ref[...] = a_ref[1].T
            v_ref[...] = b_ref[0].T
            o_ref[...] = b_ref[1]


def join_attn(core, own, other):
    _, hid, half_d = own[0].shape
    block = pl.BlockSpec((2, hid, half_d), lambda i, j, c: (0, 0, 0))
    tall = pl.BlockSpec((half_d, hid), lambda i, j, c: ((c[0] + i) % 2, 0))
    wide = pl.BlockSpec((hid, half_d), lambda i, j, c: (0, (c[0] + i) % 2))
    return join_call(core, join_attn_body, (2, 1), list(own), list(other), [block] * 4, [tall] * 3 + [wide],
                     [jax.ShapeDtypeStruct((2 * half_d, hid), F32)] * 3 + [jax.ShapeDtypeStruct((hid, 2 * half_d), F32)])


def join_flip_body(core_ref, oa_ref, ob_ref, sa_ref, sb_ref, out_ref):
    for i, srcs in enumerate(((oa_ref, ob_ref), (sa_ref, sb_ref))):
        for j, src in enumerate(srcs):
            @pl.when((pl.program_id(0) == i) & (pl.program_id(1) == j))
            def _():
                out_ref[...] = src[...].T


def join_flip(core, own, other):
    rows, cols = own[0].shape
    block = pl.BlockSpec((rows, cols), lambda i, j, c: (0, 0))
    return join_call(core, join_flip_body, (2, 2), own, other, [block] * 4,
                     pl.BlockSpec((cols, rows), lambda i, j, c: (j, (c[0] + i) % 2)),
                     jax.ShapeDtypeStruct((2 * cols, 2 * rows), F32))


def gather_pieces(part_a, part_b):
    xa, xb = pp_x(part_a), pp_x(part_b)
    ya, yb = pp_y(part_a), pp_y(part_b)
    da, db = pp_y(xa), pp_x(yb)
    own = [(xa, xb), (ya, yb), (da, db)]
    return own, [(pp_d(a), pp_d(b)) for a, b in own]


def reduce_terms(total, pp_first, pp_second, first, second):
    here, there = pp_first(total[first]), pp_first(total[3])
    last = pp_second(total[second] + there)
    return total[0] + here + last


BOTH = ('model', 'data')


def solution(mesh):
    spec_col = P(None, 'model')
    spec_row = P('model', None)
    spec_act = P('data', None, None)
    spec_rep = P(None, None)

    def device_step(x_in, cot_out, step_emb, w_q, w_k, w_v, w_o, w_1, w_2):
        layer_count, dim = step_emb.shape
        core = lax.axis_index('data')
        chip = lax.axis_index('model')
        chip_x = lax.rem(chip, 2)
        chip_y = lax.div(chip, 2)
        nbr_x = chip + 1 - 2 * chip_x
        nbr_y = lax.rem(chip + 2, 4)
        diag = lax.rem(nbr_x + 2, 4)
        chips = (chip, nbr_x, nbr_y, diag)
        hid = w_q.shape[1]
        half_d = dim // 2
        half_t = x_in.shape[1] // 2

        def take(v, which, axis, size):
            return lax.dynamic_slice_in_dim(v, which * size, size, axis)

        def put(buf, v, which, axis):
            return lax.dynamic_update_slice_in_dim(buf, v, which * v.shape[axis], axis)

        def gather(v):
            return lax.all_gather(v, BOTH, axis=0, tiled=True)

        def after(v, *deps):
            return lax.optimization_barrier((v,) + deps)[0]

        def my_tokens(v):
            mine = lax.dynamic_index_in_dim(v, chip_x, 0, keepdims=False)
            half = mine.shape[0] // 2
            recv = pp_d(take(mine, 1 - core, 0, half))
            return jnp.where(core == chip_y, take(mine, core, 0, half), recv)

        def gather_permuted(local):
            own = take(local, core, 0, local.shape[0] // 2)
            rows = own.shape[0] // 2
            p_own, p_sib = gather_pieces(own[:rows], own[rows:])
            full = put(jnp.zeros((4 * local.shape[0], dim), BF16), local, chip, 0)
            for r in (1, 2, 3):
                for part in (0, 1):
                    full = put(full, p_own[r - 1][part], 4 * chips[r] + 2 * core + part, 0)
                    full = put(full, p_sib[r - 1][part], 4 * chips[r] + 2 * (1 - core) + part, 0)
            return full

        x_cur = my_tokens(x_in)
        qkv_t = jnp.concatenate([w_q, w_k, w_v], axis=1).T
        qkv_all = gather(take(qkv_t, core, 0, qkv_t.shape[0] // 2))
        o_all = gather(take(w_o, core, 0, hid // 2))
        w2 = gather_permuted(w_2)
        w1 = gather_permuted(w_1.T)
        wq = jnp.concatenate([take(qkv_all, 3 * c, 0, hid) for c in chips], axis=0)
        wkv = jnp.concatenate([take(qkv_all, 3 * c + i, 0, hid) for i in (1, 2) for c in chips], axis=0)
        wo = jnp.concatenate([take(o_all, c, 0, hid) for c in chips], axis=0)
        d_cur = my_tokens(cot_out)
        emb = step_emb.astype(F32)

        saved = []
        g_mine = []
        um_hist = m_hist = att_hist = None
        for layer in range(layer_count):
            e = emb[layer:layer + 1]
            kv, um_hist = norm_kv(x_cur, e, wkv, layer, layer_count, um_hist)
            kv_s = pp_d(kv)
            q = nt(um_hist[0, layer], wq).astype(BF16)
            att_hist, lse = attn_fwd(q, kv, kv_s, layer, layer_count, att_hist)
            z, g, x_next, h, m_hist = mlp_fwd(x_cur, e, att_hist, wo, w1, w2, layer, layer_count, m_hist)
            g_mine.append(lax.all_to_all(g.reshape(-1, g.shape[-1]), BOTH, split_axis=0, concat_axis=0, tiled=True))
            saved.append((x_cur, q, kv, kv_s, lse, h, z))
            x_cur = x_next

        def flat(v, lead):
            return v.reshape(lead, -1, v.shape[-1])

        places = [jnp.stack([w, *chips]).astype(jnp.int32) for w in (core, 1 - core)]
        up_hist = None
        next_all = [None] * layer_count
        for layer in reversed(range(layer_count)):
            x_l, q, kv, kv_s, lse, h, z = saved[layer]
            e = emb[layer:layer + 1]
            d_next = d_cur
            if layer < layer_count - 1:
                next_all[layer] = gather(d_next)
            up_hist, um_hist, d_ctx = mlp_bwd(d_next, h, z, wo, w1, w2, layer, layer_count, um_hist, up_hist)
            if layer == 0:
                total = summed_terms(flat(up_hist, 1), flat(m_hist, 1), hid, half_d, places, UP_PLAN)
                d_ctx = after(d_ctx, *[v for r in (1, 2, 3) for v in total[r]])
                own_1a = reduce_terms({r: v[0] for r, v in total.items()}, pp_x, pp_y, 1, 2)
                own_1b = reduce_terms({r: v[1] for r, v in total.items()}, pp_y, pp_x, 2, 1)
            att_hist, own_kv, sib_kv = attn_bwd(q, kv, kv_s, d_ctx, lse, layer, layer_count, att_hist)
            recv_kv = pp_d(sib_kv)
            acc0 = nn(att_hist[0, layer], wq)
            att_hist, d_cur = d_kv(acc0, x_l, e, um_hist, own_kv, recv_kv, wkv, layer, layer_count, att_hist)

        total = summed_terms(flat(att_hist, 4), flat(um_hist, 2), hid, half_d, places, ATTN_PLAN)
        own_qk = reduce_terms({r: v[0] for r, v in total.items()}, pp_x, pp_y, 1, 2)
        own_vo = reduce_terms({r: v[1] for r, v in total.items()}, pp_y, pp_x, 2, 1)

        at_home = chip_y == core
        to_row = [(2 * c + d, 2 * (c ^ 2) + d) for c in range(4) for d in range(2) if c // 2 == d]
        in_row = [(2 * c + d, 2 * (c ^ 1) + d) for c in range(4) for d in range(2) if c // 2 == d]

        def in_order(mine, other):
            return jnp.where(chip_x == 0, mine, other), jnp.where(chip_x == 0, other, mine)

        other_half = pp_d(d_cur)
        part_p = jnp.where(core == 0, d_cur, other_half)
        part_q = jnp.where(core == 0, other_half, d_cur)
        p_y = lax.ppermute(part_p, BOTH, to_row)
        q_x = lax.ppermute(part_q, BOTH, in_row)
        p_row = jnp.where(at_home, part_p, p_y)
        q_row = jnp.concatenate(in_order(part_q, q_x), axis=0)
        p_x = pp_x(p_row)
        q_y = lax.ppermute(q_row, BOTH, to_row)
        q_both = jnp.where(at_home, q_row, q_y)
        p_0, p_1 = in_order(p_row, p_x)
        d_x = jnp.concatenate([p_0, q_both[:half_t], p_1, q_both[half_t:]], axis=0).reshape(2, -1, dim)

        ready = tuple(v for ab in total.values() for v in ab)
        cot_mine = cot_out.reshape(-1, dim)
        cot_other = pp_d(cot_mine)
        grad_2 = None
        for layer in reversed(range(layer_count)):
            g_all = after(g_mine[layer], *ready)
            if layer == layer_count - 1:
                rows = g_all.shape[0] // 2
                grad_2 = tn(take(g_all, core, 0, rows), cot_mine) + tn(take(g_all, 1 - core, 0, rows), cot_other)
            else:
                grad_2 = grad_2 + tn(g_all, next_all[layer])

        grad_2 = join(core, grad_2, pp_d(grad_2))
        own_1 = [v.reshape(-1, half_d) for v in (own_1a, own_1b)]
        grad_1 = join_flip(core, own_1, [pp_d(v) for v in own_1])
        gq, gk, gv, go = join_attn(core, (own_qk, own_vo), (pp_d(own_qk), pp_d(own_vo)))
        return gq, gk, gv, go, grad_1, grad_2, d_x

    return jax.shard_map(device_step, mesh=mesh,
                         in_specs=(spec_act, spec_act, spec_rep, spec_col, spec_col, spec_col, spec_row, spec_col, spec_row),
                         out_specs=(spec_col, spec_col, spec_col, spec_row, spec_col, spec_row, spec_act),
                         check_vma=False)
```

```python
import functools

import jax
import jax.numpy as jnp
from jax import lax
from jax.experimental import pallas as pl
from jax.experimental.pallas import tpu as pltpu
from jax.sharding import PartitionSpec as P


HEAD_DIM = 64
EPS_NORM = 1e-6
F32 = jnp.float32
BF16 = jnp.bfloat16
LOG2E = 1.4426950408889634
VMEM_ALL = 60 * 1024 * 1024
SCALE = HEAD_DIM ** -0.5

SWAP_D = [(0, 1), (1, 0)]


SWAP_X = [(0, 1), (1, 0), (2, 3), (3, 2)]
SWAP_Y = [(0, 2), (2, 0), (1, 3), (3, 1)]


def pp_x(v):
    return lax.ppermute(v, 'model', SWAP_X)


def pp_y(v):
    return lax.ppermute(v, 'model', SWAP_Y)


def pp_d(v):
    return lax.ppermute(v, 'data', SWAP_D)


def dot(a, b, dims):
    return lax.dot_general(a, b, (dims, ((), ())), preferred_element_type=F32)


def nn(a, b):
    return dot(a, b, ((1,), (0,)))


def nt(a, b):
    return dot(a, b, ((1,), (1,)))


def tn(a, b):
    return dot(a, b, ((0,), (0,)))


def pair_masks(rows):
    lane = lax.broadcasted_iota(jnp.int32, (rows, 128), 1)
    return lane < HEAD_DIM


CHUNK = 256
WIDE = 256


def masked_pair(q):
    low = pair_masks(CHUNK)
    zero = jnp.zeros_like(q)
    return jnp.concatenate([jnp.where(low, q, zero), jnp.where(low, zero, q)], axis=0)


def attn_fwd_body(*refs):
    u_ref, w0_ref, wn_ref, ko_ref, ks_ref, kno_ref, kns_ref, vo_ref, vs_ref = refs[:9]
    q_ref, ctx_ref, lse_ref, qs_ref, a_ref, ma_ref = refs[-6:]
    units = [(sub, i) for sub in range(WIDE // 128) for i in range(q_ref.shape[0] // CHUNK)]

    def joined(own_ref, sib_ref, sub):
        cols = slice(sub * 128, (sub + 1) * 128)
        return jnp.concatenate([own_ref[:, cols], sib_ref[:, cols]], axis=0)

    def scores(ko, ks, q, sub, i):
        s = nt(joined(ko, ks, sub), masked_pair(q[i * CHUNK:(i + 1) * CHUNK, sub * 128:(sub + 1) * 128]))
        return s, jnp.max(s, axis=0, keepdims=True)

    @pl.when(pl.program_id(0) == 0)
    def _():
        qs_ref[...] = nt(u_ref[0, 0], w0_ref[...]).astype(BF16)
        a_ref[...], ma_ref[...] = scores(ko_ref, ks_ref, qs_ref[...], 0, 0)

    q_ref[...] = qs_ref[...]
    s, m = a_ref[...], ma_ref[...]
    for n, (sub, i) in enumerate(units):
        if n + 1 < len(units):
            ahead = scores(ko_ref, ks_ref, q_ref[...], *units[n + 1])
        else:
            ahead = scores(kno_ref, kns_ref, q_next, 0, 0)
        if n == 0:
            q_next = nt(u_ref[0, 0], wn_ref[...]).astype(BF16)
        rows, cols = slice(i * CHUNK, (i + 1) * CHUNK), slice(sub * 128, (sub + 1) * 128)
        p = jnp.exp2((s - m) * (SCALE * LOG2E))
        l = jnp.sum(p, axis=0, keepdims=True)
        pb = (p * (1.0 / l)).astype(BF16)
        lse = m * (SCALE * LOG2E) + jnp.log2(l)
        lse_ref[sub, 0:1, rows] = lse[:, :CHUNK]
        lse_ref[sub, 1:2, rows] = lse[:, CHUNK:]
        ctx_t = tn(joined(vo_ref, vs_ref, sub), pb)
        ctx_t = jnp.concatenate([ctx_t[:HEAD_DIM, :CHUNK], ctx_t[HEAD_DIM:, CHUNK:]], axis=0)
        ctx_ref[0, 0, rows, cols] = ctx_t.T.astype(BF16)
        s, m = ahead
    qs_ref[...] = q_next
    a_ref[...], ma_ref[...] = s, m


def attn_fwd(um_hist, wq, kv, kv_s, layer, layers, hist):
    tk, width = kv.shape[0], kv.shape[1] // 2
    tq = um_hist.shape[2]
    pairs = width // 128
    steps = width // WIDE

    def col(off):
        return lambda j: (0, j + off)

    def nxt(j):
        return (0, jnp.minimum(j + 1, steps - 1))

    extra = [] if hist is None else [hist]
    flops = 2 * 2 * tq * (2 * tk) * 256 * (width // HEAD_DIM)
    return pl.pallas_call(
        attn_fwd_body,
        grid=(steps,),
        in_specs=[pl.BlockSpec((1, 1, tq, width), lambda j: (0, layer, 0, 0)),
                  pl.BlockSpec((WIDE, width), lambda j: (0, 0)),
                  pl.BlockSpec((WIDE, width), lambda j: (jnp.minimum(j + 1, steps - 1), 0)),
                  pl.BlockSpec((tk, WIDE), col(0)), pl.BlockSpec((tk, WIDE), col(0)),
                  pl.BlockSpec((tk, WIDE), nxt), pl.BlockSpec((tk, WIDE), nxt),
                  pl.BlockSpec((tk, WIDE), col(steps)), pl.BlockSpec((tk, WIDE), col(steps))]
        + [pl.BlockSpec(memory_space=pl.ANY)] * len(extra),
        out_specs=[pl.BlockSpec((tq, WIDE), col(0)),
                   pl.BlockSpec((1, 1, tq, WIDE), lambda j: (3, layer, 0, j)),
                   pl.BlockSpec((WIDE // 128, 2, tq), lambda j: (j, 0, 0))],
        out_shape=[jax.ShapeDtypeStruct((tq, width), BF16),
                   jax.ShapeDtypeStruct((4, layers, tq, width), BF16),
                   jax.ShapeDtypeStruct((pairs, 2, tq), F32)],
        input_output_aliases={9: 1} if extra else {},
        scratch_shapes=[pltpu.VMEM((tq, WIDE), BF16), pltpu.VMEM((2 * tk, 2 * CHUNK), F32), pltpu.VMEM((1, 2 * CHUNK), F32)],
        compiler_params=pltpu.CompilerParams(dimension_semantics=('arbitrary',),
                                             vmem_limit_bytes=VMEM_ALL),
        cost_estimate=pl.CostEstimate(flops=flops, bytes_accessed=2 * (tq * width * 2 + 4 * tk * width),
                                      transcendentals=tq * 2 * tk * (width // HEAD_DIM)),
        name='attn_fwd',
    )(um_hist, wq, wq, kv, kv_s, kv, kv_s, kv, kv_s, *extra)


def attn_bwd_body(q_ref, ko_ref, ks_ref, vo_ref, vs_ref, do_ref, lse_ref, hist_ref, dq_ref, down_ref, dsib_ref):
    tk = ko_ref.shape[0]
    low = pair_masks(CHUNK)
    units = [(sub, i, h) for sub in range(WIDE // 128) for i in range(q_ref.shape[0] // CHUNK) for h in range(2)]

    def keys(own_ref, sib_ref, sub):
        cols = slice(sub * 128, (sub + 1) * 128)
        return jnp.concatenate([own_ref[:, cols], sib_ref[:, cols]], axis=0)

    def masked(ref, sub, i, h):
        v = ref[i * CHUNK:(i + 1) * CHUNK, sub * 128:(sub + 1) * 128]
        return jnp.where(low if h == 0 else ~low, v, jnp.zeros_like(v))

    def products(sub, i, h):
        s = nt(keys(ko_ref, ks_ref, sub), masked(q_ref, sub, i, h))
        return s, nt(keys(vo_ref, vs_ref, sub), masked(do_ref, sub, i, h)).astype(BF16)

    dqs = []
    ahead = products(*units[0])
    for n, (sub, i, h) in enumerate(units):
        s, dp = ahead
        if n + 1 < len(units):
            ahead = products(*units[n + 1])
        rows, cols = slice(i * CHUNK, (i + 1) * CHUNK), slice(sub * 128, (sub + 1) * 128)
        p = jnp.exp2(s * (SCALE * LOG2E) - lse_ref[sub, h:h + 1, rows])
        dp = dp.astype(F32)
        delta = jnp.sum(p * dp, axis=0, keepdims=True)
        ds = (p * (dp - delta)).astype(BF16)
        dv = nn(p.astype(BF16), masked(do_ref, sub, i, h))
        dk = nn(ds, masked(q_ref, sub, i, h) * jnp.asarray(SCALE, BF16))
        for m, grad in enumerate((dk, dv)):
            for ref, part in ((down_ref, grad[:tk]), (dsib_ref, grad[tk:])):
                if i == 0 and h == 0:
                    ref[m, :, cols] = part
                else:
                    ref[m, :, cols] += part
        dqs.append(tn(keys(ko_ref, ks_ref, sub), ds)[h * HEAD_DIM:(h + 1) * HEAD_DIM, :] * SCALE)
        if h == 1:
            dq_ref[0, 0, rows, cols] = jnp.concatenate(dqs, axis=0).T.astype(BF16)
            dqs = []


def attn_bwd(q, kv, kv_s, d_ctx, lse, layer, layers, hist):
    tq, width = q.shape
    tk = kv.shape[0]
    steps = width // WIDE

    def col(off):
        return lambda j: (0, j + off)

    flops = 5 * 2 * tq * (2 * tk) * 256 * (width // HEAD_DIM)
    qblk = pl.BlockSpec((tq, WIDE), col(0))
    kblk = pl.BlockSpec((tk, WIDE), col(0))
    vblk = pl.BlockSpec((tk, WIDE), col(steps))
    both = pl.BlockSpec((2, tk, WIDE), lambda j: (0, 0, j))
    return pl.pallas_call(
        attn_bwd_body,
        grid=(steps,),
        in_specs=[qblk, kblk, kblk, vblk, vblk, qblk,
                  pl.BlockSpec((WIDE // 128, 2, tq), lambda j: (j, 0, 0)), pl.BlockSpec(memory_space=pl.ANY)],
        out_specs=[pl.BlockSpec((1, 1, tq, WIDE), lambda j: (0, layer, 0, j)), both, both],
        out_shape=[jax.ShapeDtypeStruct((4, layers, tq, width), BF16)]
        + [jax.ShapeDtypeStruct((2, tk, width), F32)] * 2,
        input_output_aliases={7: 0},
        compiler_params=pltpu.CompilerParams(dimension_semantics=('arbitrary',),
                                             vmem_limit_bytes=VMEM_ALL),
        cost_estimate=pl.CostEstimate(flops=flops, bytes_accessed=2 * (2 * tq * width * 2 + 4 * tk * width) + 16 * tk * width,
                                      transcendentals=tq * 2 * tk * (width // HEAD_DIM)),
        name='attn_bwd',
    )(q, kv, kv_s, kv, kv_s, d_ctx, lse, hist)


def kv_body(*refs):
    x_ref, e_ref, w_ref = refs[:3]
    kv_ref, u_ref = refs[-2:]

    @pl.when(pl.program_id(0) == 0)
    def _():
        s = x_ref[...].astype(F32) + e_ref[...]
        u_ref[0, 0] = (s * lax.rsqrt(jnp.mean(s * s, axis=-1, keepdims=True) + EPS_NORM)).astype(BF16)

    for rows in ROWS:
        kv_ref[rows, :] = nt(u_ref[0, 0, rows, :], w_ref[...]).astype(BF16)


def norm_kv(x, e, wkv, layer, layers, hist):
    t, dim = x.shape
    width = wkv.shape[0]
    blk = 1024
    extra = [] if hist is None else [hist]
    return pl.pallas_call(
        kv_body,
        grid=(width // blk,),
        in_specs=[pl.BlockSpec((t, dim), lambda j: (0, 0)), pl.BlockSpec((1, dim), lambda j: (0, 0)),
                  pl.BlockSpec((blk, dim), lambda j: (j, 0))] + [pl.BlockSpec(memory_space=pl.ANY)] * len(extra),
        out_specs=[pl.BlockSpec((t, blk), lambda j: (0, j)), pl.BlockSpec((1, 1, t, dim), lambda j: (0, layer, 0, 0))],
        out_shape=[jax.ShapeDtypeStruct((t, width), BF16), jax.ShapeDtypeStruct((2, layers, t, dim), BF16)],
        input_output_aliases={3: 1} if extra else {},
        compiler_params=pltpu.CompilerParams(dimension_semantics=('arbitrary',), vmem_limit_bytes=VMEM_ALL),
        cost_estimate=pl.CostEstimate(flops=2 * t * dim * width, bytes_accessed=2 * (dim * width + t * width + 2 * t * dim),
                                      transcendentals=t),
        name='norm_kv',
    )(x, e, wkv, *extra)


def d_kv_body(layer, acc0_hbm, x_hbm, e_ref, um_hbm, own_ref, recv_ref, w_ref, hist_ref, dkv_ref, prev_ref,
              acc_ref, acc0_ref, x_ref, mid_ref, sems):
    j = pl.program_id(0)
    late = [pltpu.make_async_copy(src, dst, sems.at[n])
            for n, (src, dst) in enumerate(((acc0_hbm, acc0_ref), (x_hbm, x_ref), (um_hbm.at[1, layer], mid_ref)))]

    @pl.when(j == 0)
    def _():
        for copy in late:
            copy.start()
        acc_ref[...] = jnp.zeros_like(acc_ref)

    dkv_ref[0, 0] = (own_ref[0] + recv_ref[0]).astype(BF16)
    for rows in ROWS:
        acc_ref[rows, :] += nn(dkv_ref[0, 0, rows, :], w_ref[...])

    @pl.when(j == pl.num_programs(0) - 1)
    def _():
        for copy in late:
            copy.wait()
        dn = (acc_ref[...] + acc0_ref[...]).astype(BF16).astype(F32)
        s = x_ref[...].astype(F32) + e_ref[...]
        inv = lax.rsqrt(jnp.mean(s * s, axis=-1, keepdims=True) + EPS_NORM)
        proj = jnp.mean(s * dn, axis=-1, keepdims=True)
        prev_ref[...] = (mid_ref[...].astype(F32) + inv * dn - s * (inv * inv * inv * proj)).astype(BF16)


def d_kv(acc0, x, e, um_hist, own, recv, wkv, layer, layers, hist):
    t, dim = x.shape
    half = dim // 2
    hbm = pl.BlockSpec(memory_space=pl.ANY)
    gblk = pl.BlockSpec((1, t, half), lambda j: (j // 2, 0, j % 2))
    return pl.pallas_call(
        functools.partial(d_kv_body, layer),
        grid=(4,),
        in_specs=[hbm, hbm, pl.BlockSpec((1, dim), lambda j: (0, 0)), hbm, gblk, gblk,
                  pl.BlockSpec((half, dim), lambda j: (j, 0)), hbm],
        out_specs=[pl.BlockSpec((1, 1, t, half), lambda j: (1 + j // 2, layer, 0, j % 2)),
                   pl.BlockSpec((t, dim), lambda j: (0, 0))],
        out_shape=[jax.ShapeDtypeStruct((4, layers, t, dim), BF16), jax.ShapeDtypeStruct((t, dim), BF16)],
        scratch_shapes=[pltpu.VMEM((t, dim), F32), pltpu.VMEM((t, dim), F32), pltpu.VMEM((t, dim), BF16),
                        pltpu.VMEM((t, dim), BF16), pltpu.SemaphoreType.DMA((3,))],
        input_output_aliases={7: 0},
        compiler_params=pltpu.CompilerParams(dimension_semantics=('arbitrary',), vmem_limit_bytes=VMEM_ALL),
        cost_estimate=pl.CostEstimate(flops=4 * t * dim * dim, bytes_accessed=4 * dim * dim + 20 * t * dim, transcendentals=t),
        name='d_kv',
    )(acc0, x, e, um_hist, own, recv, wkv, hist)


def terms_body(added, slot_of, places_ref, lhs_ref, rhs_ref, *refs):
    recv, outs = refs[:4 * added], refs[-4:]
    step = pl.program_id(0)
    val = tn(lhs_ref[0], rhs_ref[0])
    for slot in range(4):
        @pl.when(slot_of(step) == slot)
        def _():
            outs[slot][0] = val + recv[slot][0] if added else val


def terms(lhs, rhs, rows, cols, places, plan, chips, recv):
    tokens = lhs.shape[1]
    first, second = chips
    lhs_at, rhs_at, slot_of, turns = plan

    def rel(r):
        return first + r * (second - first)

    slots = [pl.BlockSpec((1, rows, cols), lambda i, p, at=at: (jnp.clip(i - at, 0, 1), 0, 0)) for at in turns]
    out = pl.pallas_call(
        functools.partial(terms_body, len(recv) // 4, slot_of),
        grid_spec=pltpu.PrefetchScalarGridSpec(
            num_scalar_prefetch=1, grid=(8,),
            in_specs=[pl.BlockSpec((1, tokens, rows), lambda i, p: lhs_at(i, rel, p)),
                      pl.BlockSpec((1, tokens, cols), lambda i, p: rhs_at(i, p))] + slots[:len(recv)],
            out_specs=slots),
        out_shape=[jax.ShapeDtypeStruct((2, rows, cols), F32)] * 4,
        compiler_params=pltpu.CompilerParams(dimension_semantics=('arbitrary',), vmem_limit_bytes=VMEM_ALL),
        cost_estimate=pl.CostEstimate(flops=16 * tokens * rows * cols, bytes_accessed=24 * tokens * rows, transcendentals=0),
    )(places, lhs, rhs, *recv)
    return {first: out[:2], second: out[2:]}


ATTN_PLAN = (lambda i, rel, p: (jnp.where(i < 4, i % 2, i // 2), 0, rel(jnp.where(i < 4, i // 2, i % 2))),
             lambda i, p: (i // 6, 0, p[0]),
             lambda i: jnp.where(i < 4, 2 * (i // 2), 2 * (i % 2) + 1),
             (0, 5, 2, 6))
UP_PLAN = (lambda i, rel, p: (0, 0, 4 * p[1 + rel((i // 2) % 2)] + 2 * p[0] + i % 2),
           lambda i, p: (0, 0, i // 4),
           lambda i: 2 * ((i // 2) % 2) + i // 4,
           (0, 4, 2, 6))


def summed_terms(lhs, rhs, rows, cols, places, plan):
    def in_turn(where, done):
        return lax.optimization_barrier((where, done))[0] if done else where

    sent, total = {}, {}
    where, done = places[1], []
    for pair in ((3, 1), (2, 0)):
        out = terms(lhs, rhs, rows, cols, in_turn(where, done), plan, pair, [])
        done = [v for ab in out.values() for v in ab]
        sent.update({r: [pp_d(v) for v in ab] for r, ab in out.items()})
    where, done = places[0], []
    for pair in ((3, 1), (2, 0)):
        out = terms(lhs, rhs, rows, cols, in_turn(where, done), plan, pair, sent[pair[0]] + sent[pair[1]])
        done = [v for ab in out.values() for v in ab]
        total.update(out)
    return total


GELU_C = 0.7978845608028654
GELU_A = 0.044715
BLOCK_F = 768
ROWS = (slice(0, 256), slice(256, 512))


def mlp_fwd_body(*refs):
    x0_ref, e_ref, ctx_ref, wo_ref, w1_ref, w2_ref = refs[:6]
    z_ref, g_ref, x_ref, h_ref, m_ref, acc_ref = refs[-6:]
    j = pl.program_id(0)

    @pl.when(j == 0)
    def _():
        for rows in ROWS:
            s = x0_ref[rows, :].astype(F32) + e_ref[...]
            h = (s + nn(ctx_ref[0, 0, rows, :], wo_ref[...])).astype(BF16)
            h_ref[rows, :] = h
            hf = h.astype(F32)
            acc_ref[rows, :] = hf
            m_ref[0, rows, :] = (hf * lax.rsqrt(jnp.mean(hf * hf, axis=-1, keepdims=True) + EPS_NORM)).astype(BF16)

    for rows in ROWS:
        z = nt(m_ref[0, rows, :], w1_ref[...]).astype(BF16)
        z_ref[rows, :] = z
        zf = z.astype(F32)
        t = jnp.tanh(zf * (GELU_C + (GELU_A * GELU_C) * (zf * zf)))
        half = 0.5 * zf
        g_ref[0, rows, :] = (half + half * t).astype(BF16)
    for rows in ROWS:
        acc_ref[rows, :] += nn(g_ref[0, rows, :], w2_ref[...])

    @pl.when(j == pl.num_programs(0) - 1)
    def _():
        x_ref[...] = acc_ref[...].astype(BF16)


def mlp_fwd(x, e, ctx_hist, wo, w1t, w2, layer, layers, hist):
    t, dim = x.shape
    hidden = w2.shape[0]
    whole = pl.BlockSpec((t, dim), lambda j: (0, 0))
    slab = pl.BlockSpec((1, t, dim), lambda j: (layer, 0, 0))
    wblk = pl.BlockSpec((BLOCK_F, dim), lambda j: (j, 0))
    extra = [] if hist is None else [hist]
    return pl.pallas_call(
        mlp_fwd_body,
        grid=(hidden // BLOCK_F,),
        in_specs=[whole, pl.BlockSpec((1, dim), lambda j: (0, 0)), pl.BlockSpec((1, 1, t, dim), lambda j: (3, layer, 0, 0)),
                  pl.BlockSpec((dim, dim), lambda j: (0, 0)), wblk, wblk]
        + [pl.BlockSpec(memory_space=pl.ANY)] * len(extra),
        out_specs=[pl.BlockSpec((t, BLOCK_F), lambda j: (0, j)),
                   pl.BlockSpec((1, t, BLOCK_F), lambda j: (j, 0, 0)), whole, whole, slab],
        out_shape=[jax.ShapeDtypeStruct((t, hidden), BF16),
                   jax.ShapeDtypeStruct((hidden // BLOCK_F, t, BLOCK_F), BF16),
                   jax.ShapeDtypeStruct((t, dim), BF16), jax.ShapeDtypeStruct((t, dim), BF16),
                   jax.ShapeDtypeStruct((layers, t, dim), BF16)],
        scratch_shapes=[pltpu.VMEM((t, dim), F32)],
        input_output_aliases={6: 4} if extra else {},
        compiler_params=pltpu.CompilerParams(dimension_semantics=('arbitrary',), vmem_limit_bytes=VMEM_ALL),
        cost_estimate=pl.CostEstimate(flops=4 * t * dim * hidden, bytes_accessed=4 * dim * hidden + 4 * t * hidden,
                                      transcendentals=t * hidden),
        name='mlp_fwd',
    )(x, e, ctx_hist, wo, w1t, w2, *extra)


BLOCK_B = 1024
SUB_B = 512


def mlp_bwd_body(*refs):
    d_ref, h_hbm, z_ref, wo_hbm, w1_ref, w2_ref = refs[:6]
    up_ref, mid_ref, dctx_ref, acc_ref, h_ref, wo_ref, sems = refs[-7:]
    j = pl.program_id(0)
    late = [pltpu.make_async_copy(h_hbm, h_ref, sems.at[0]), pltpu.make_async_copy(wo_hbm, wo_ref, sems.at[1])]

    @pl.when(j == 0)
    def _():
        for copy in late:
            copy.start()
        acc_ref[...] = jnp.zeros_like(acc_ref)

    for i in range(0, BLOCK_B, SUB_B):
        cols = slice(i, i + SUB_B)
        for rows in ROWS:
            da = nt(d_ref[rows, :], w2_ref[cols, :]).astype(BF16).astype(F32)
            zf = z_ref[rows, cols].astype(F32)
            z2 = zf * zf
            t = jnp.tanh(zf * (GELU_C + (GELU_A * GELU_C) * z2))
            slope = (1.0 + t) * (0.5 + (1.0 - t) * (zf * (0.5 * GELU_C + (1.5 * GELU_A * GELU_C) * z2)))
            up_ref[0, rows, cols] = (da * slope).astype(BF16)
    for rows in ROWS:
        acc_ref[rows, :] += nn(up_ref[0, rows, :], w1_ref[...])

    @pl.when(j == pl.num_programs(0) - 1)
    def _():
        for copy in late:
            copy.wait()
        for rows in ROWS:
            dn = acc_ref[rows, :].astype(BF16).astype(F32)
            hf = h_ref[rows, :].astype(F32)
            inv = lax.rsqrt(jnp.mean(hf * hf, axis=-1, keepdims=True) + EPS_NORM)
            proj = jnp.mean(hf * dn, axis=-1, keepdims=True)
            mid = (d_ref[rows, :].astype(F32) + inv * dn - hf * (inv * inv * inv * proj)).astype(BF16)
            mid_ref[0, 0, rows, :] = mid
            dctx_ref[rows, :] = nt(mid, wo_ref[...]).astype(BF16)


def mlp_bwd(d_next, h, z, wo, w1t, w2, layer, layers, um_hist, hist):
    t, dim = h.shape
    hidden = w2.shape[0]
    whole = pl.BlockSpec((t, dim), lambda j: (0, 0))
    hbm = pl.BlockSpec(memory_space=pl.ANY)
    wblk = pl.BlockSpec((BLOCK_B, dim), lambda j: (j, 0))
    extra = [um_hist] if hist is None else [um_hist, hist]
    return pl.pallas_call(
        mlp_bwd_body,
        grid=(hidden // BLOCK_B,),
        in_specs=[whole, hbm, pl.BlockSpec((t, BLOCK_B), lambda j: (0, j)), hbm, wblk, wblk]
        + [pl.BlockSpec(memory_space=pl.ANY)] * len(extra),
        out_specs=[pl.BlockSpec((1, t, BLOCK_B), lambda j: (layer, 0, j)), pl.BlockSpec((1, 1, t, dim), lambda j: (1, layer, 0, 0)), whole],
        out_shape=[jax.ShapeDtypeStruct((layers, t, hidden), BF16), jax.ShapeDtypeStruct((2, layers, t, dim), BF16),
                   jax.ShapeDtypeStruct((t, dim), BF16)],
        scratch_shapes=[pltpu.VMEM((t, dim), F32), pltpu.VMEM((t, dim), BF16), pltpu.VMEM((dim, dim), BF16),
                        pltpu.SemaphoreType.DMA((2,))],
        input_output_aliases={6: 1} if hist is None else {6: 1, 7: 0},
        compiler_params=pltpu.CompilerParams(dimension_semantics=('arbitrary',), vmem_limit_bytes=VMEM_ALL),
        cost_estimate=pl.CostEstimate(flops=4 * t * dim * hidden, bytes_accessed=4 * dim * hidden + 4 * t * hidden,
                                      transcendentals=t * hidden),
        name='mlp_bwd',
    )(d_next, h, z, wo, w1t, w2, *extra)


def spread_body(chips_ref, src_ref, q_ref, kv_ref):
    @pl.when(pl.program_id(0) < 4)
    def _():
        q_ref[...] = src_ref[...]

    @pl.when(pl.program_id(0) >= 4)
    def _():
        kv_ref[...] = src_ref[...]


def spread(chips, qkv):
    rows, dim = qkv.shape[0] // 12, qkv.shape[1]
    return pl.pallas_call(
        spread_body,
        grid_spec=pltpu.PrefetchScalarGridSpec(
            num_scalar_prefetch=1, grid=(12,),
            in_specs=[pl.BlockSpec((rows, dim), lambda i, c: (3 * c[i % 4] + i // 4, 0))],
            out_specs=[pl.BlockSpec((rows, dim), lambda i, c: (jnp.minimum(i, 3), 0)),
                       pl.BlockSpec((rows, dim), lambda i, c: (jnp.maximum(i - 4, 0), 0))]),
        out_shape=[jax.ShapeDtypeStruct((4 * rows, dim), BF16), jax.ShapeDtypeStruct((8 * rows, dim), BF16)],
        compiler_params=pltpu.CompilerParams(dimension_semantics=('arbitrary',), vmem_limit_bytes=VMEM_ALL),
        cost_estimate=pl.CostEstimate(flops=qkv.size, bytes_accessed=4 * qkv.size, transcendentals=0),
        name='spread',
    )(chips, qkv)


def join_body(count, core_ref, *refs):
    for n in range(count):
        own, other, out = refs[n], refs[count + n], refs[2 * count + n]
        for i, src in enumerate((own, other)):
            @pl.when(pl.program_id(0) == i)
            def _():
                out[...] = src[...]


def join_call(core, body, grid, own, other, in_specs, out_specs, out_shape):
    size = sum(v.size for v in own)
    return pl.pallas_call(
        body,
        grid_spec=pltpu.PrefetchScalarGridSpec(num_scalar_prefetch=1, grid=grid, in_specs=in_specs, out_specs=out_specs),
        out_shape=out_shape,
        compiler_params=pltpu.CompilerParams(dimension_semantics=('arbitrary', 'arbitrary'), vmem_limit_bytes=VMEM_ALL),
        cost_estimate=pl.CostEstimate(flops=8 * size, bytes_accessed=16 * size, transcendentals=0),
    )(core.reshape(1), *own, *other)


def join(core, own, other):
    rows, cols = own.shape[0] // 4, own.shape[1]
    first = pl.BlockSpec((rows, cols), lambda i, j, c: (jnp.where(i == 0, j, 3), 0))
    then = pl.BlockSpec((rows, cols), lambda i, j, c: (jnp.where(i == 0, 0, j), 0))
    return join_call(core, functools.partial(join_body, 1), (2, 4), [own], [other], [first, then],
                     pl.BlockSpec((rows, cols), lambda i, j, c: (4 * ((c[0] + i) % 2) + j, 0)),
                     jax.ShapeDtypeStruct((8 * rows, cols), F32))


def join_attn_body(core_ref, own_a, own_b, sib_a, sib_b, q_ref, k_ref, v_ref, o_ref):
    for i, (a_ref, b_ref) in enumerate(((own_a, own_b), (sib_a, sib_b))):
        @pl.when(pl.program_id(0) == i)
        def _():
            q_ref[...] = a_ref[0].T
            k_ref[...] = a_ref[1].T
            v_ref[...] = b_ref[0].T
            o_ref[...] = b_ref[1]


def join_attn(core, own, other):
    _, hid, half_d = own[0].shape
    block = pl.BlockSpec((2, hid, half_d), lambda i, j, c: (0, 0, 0))
    tall = pl.BlockSpec((half_d, hid), lambda i, j, c: ((c[0] + i) % 2, 0))
    wide = pl.BlockSpec((hid, half_d), lambda i, j, c: (0, (c[0] + i) % 2))
    return join_call(core, join_attn_body, (2, 1), list(own), list(other), [block] * 4, [tall] * 3 + [wide],
                     [jax.ShapeDtypeStruct((2 * half_d, hid), F32)] * 3 + [jax.ShapeDtypeStruct((hid, 2 * half_d), F32)])


def join_flip_body(core_ref, oa_ref, ob_ref, sa_ref, sb_ref, out_ref):
    for i, srcs in enumerate(((oa_ref, ob_ref), (sa_ref, sb_ref))):
        for j, src in enumerate(srcs):
            @pl.when((pl.program_id(0) == i) & (pl.program_id(1) == j))
            def _():
                out_ref[...] = src[...].T


def join_flip(core, own, other):
    rows, cols = own[0].shape
    block = pl.BlockSpec((rows, cols), lambda i, j, c: (0, 0))
    return join_call(core, join_flip_body, (2, 2), own, other, [block] * 4,
                     pl.BlockSpec((cols, rows), lambda i, j, c: (j, (c[0] + i) % 2)),
                     jax.ShapeDtypeStruct((2 * cols, 2 * rows), F32))


def gather_pieces(part_a, part_b):
    xa, xb = pp_x(part_a), pp_x(part_b)
    ya, yb = pp_y(part_a), pp_y(part_b)
    da, db = pp_y(xa), pp_x(yb)
    own = [(xa, xb), (ya, yb), (da, db)]
    return own, [(pp_d(a), pp_d(b)) for a, b in own]


def reduce_terms(total, pp_first, pp_second, first, second):
    here, there = pp_first(total[first]), pp_first(total[3])
    last = pp_second(total[second] + there)
    return total[0] + here + last


BOTH = ('model', 'data')


def solution(mesh):
    spec_col = P(None, 'model')
    spec_row = P('model', None)
    spec_act = P('data', None, None)
    spec_rep = P(None, None)

    def device_step(x_in, cot_out, step_emb, w_q, w_k, w_v, w_o, w_1, w_2):
        layer_count, dim = step_emb.shape
        core = lax.axis_index('data')
        chip = lax.axis_index('model')
        chip_x = lax.rem(chip, 2)
        chip_y = lax.div(chip, 2)
        nbr_x = chip + 1 - 2 * chip_x
        nbr_y = lax.rem(chip + 2, 4)
        diag = lax.rem(nbr_x + 2, 4)
        chips = (chip, nbr_x, nbr_y, diag)
        hid = w_q.shape[1]
        half_d = dim // 2
        half_t = x_in.shape[1] // 2

        def take(v, which, axis, size):
            return lax.dynamic_slice_in_dim(v, which * size, size, axis)

        def put(buf, v, which, axis):
            return lax.dynamic_update_slice_in_dim(buf, v, which * v.shape[axis], axis)

        def gather(v):
            return lax.all_gather(v, BOTH, axis=0, tiled=True)

        def after(v, *deps):
            return lax.optimization_barrier((v,) + deps)[0]

        def my_tokens(v):
            mine = lax.dynamic_index_in_dim(v, chip_x, 0, keepdims=False)
            half = mine.shape[0] // 2
            recv = pp_d(take(mine, 1 - core, 0, half))
            return jnp.where(core == chip_y, take(mine, core, 0, half), recv)

        def gather_permuted(local):
            own = take(local, core, 0, local.shape[0] // 2)
            rows = own.shape[0] // 2
            p_own, p_sib = gather_pieces(own[:rows], own[rows:])
            full = put(jnp.zeros((4 * local.shape[0], dim), BF16), local, chip, 0)
            for r in (1, 2, 3):
                for part in (0, 1):
                    full = put(full, p_own[r - 1][part], 4 * chips[r] + 2 * core + part, 0)
                    full = put(full, p_sib[r - 1][part], 4 * chips[r] + 2 * (1 - core) + part, 0)
            return full

        x_cur = my_tokens(x_in)
        qkv_t = jnp.concatenate([w_q, w_k, w_v], axis=1).T
        qkv_all = gather(take(qkv_t, core, 0, qkv_t.shape[0] // 2))
        o_all = gather(take(w_o, core, 0, hid // 2))
        w2 = gather_permuted(w_2)
        w1 = gather_permuted(w_1.T)
        wq, wkv = spread(jnp.stack(chips).astype(jnp.int32), qkv_all)
        wo = jnp.concatenate([take(o_all, c, 0, hid) for c in chips], axis=0)
        d_cur = my_tokens(cot_out)
        emb = step_emb.astype(F32)

        saved = []
        g_mine = []
        um_hist = m_hist = att_hist = None
        for layer in range(layer_count):
            e = emb[layer:layer + 1]
            kv, um_hist = norm_kv(x_cur, e, wkv, layer, layer_count, um_hist)
            kv_s = pp_d(kv)
            q, att_hist, lse = attn_fwd(um_hist, wq, kv, kv_s, layer, layer_count, att_hist)
            z, g, x_next, h, m_hist = mlp_fwd(x_cur, e, att_hist, wo, w1, w2, layer, layer_count, m_hist)
            g_mine.append(lax.all_to_all(g.reshape(-1, g.shape[-1]), BOTH, split_axis=0, concat_axis=0, tiled=True))
            saved.append((x_cur, q, kv, kv_s, lse, h, z))
            x_cur = x_next

        def flat(v, lead):
            return v.reshape(lead, -1, v.shape[-1])

        places = [jnp.stack([w, *chips]).astype(jnp.int32) for w in (core, 1 - core)]
        up_hist = None
        next_all = [None] * layer_count
        for layer in reversed(range(layer_count)):
            x_l, q, kv, kv_s, lse, h, z = saved[layer]
            e = emb[layer:layer + 1]
            d_next = d_cur
            if layer < layer_count - 1:
                next_all[layer] = gather(d_next)
            up_hist, um_hist, d_ctx = mlp_bwd(d_next, h, z, wo, w1, w2, layer, layer_count, um_hist, up_hist)
            if layer == 0:
                total = summed_terms(flat(up_hist, 1), flat(m_hist, 1), hid, half_d, places, UP_PLAN)
                d_ctx = after(d_ctx, *[v for r in (1, 2, 3) for v in total[r]])
                own_1a = reduce_terms({r: v[0] for r, v in total.items()}, pp_x, pp_y, 1, 2)
                own_1b = reduce_terms({r: v[1] for r, v in total.items()}, pp_y, pp_x, 2, 1)
            att_hist, own_kv, sib_kv = attn_bwd(q, kv, kv_s, d_ctx, lse, layer, layer_count, att_hist)
            recv_kv = pp_d(sib_kv)
            acc0 = nn(att_hist[0, layer], wq)
            att_hist, d_cur = d_kv(acc0, x_l, e, um_hist, own_kv, recv_kv, wkv, layer, layer_count, att_hist)

        total = summed_terms(flat(att_hist, 4), flat(um_hist, 2), hid, half_d, places, ATTN_PLAN)
        own_qk = reduce_terms({r: v[0] for r, v in total.items()}, pp_x, pp_y, 1, 2)
        own_vo = reduce_terms({r: v[1] for r, v in total.items()}, pp_y, pp_x, 2, 1)

        at_home = chip_y == core
        to_row = [(2 * c + d, 2 * (c ^ 2) + d) for c in range(4) for d in range(2) if c // 2 == d]
        in_row = [(2 * c + d, 2 * (c ^ 1) + d) for c in range(4) for d in range(2) if c // 2 == d]

        def in_order(mine, other):
            return jnp.where(chip_x == 0, mine, other), jnp.where(chip_x == 0, other, mine)

        other_half = pp_d(d_cur)
        part_p = jnp.where(core == 0, d_cur, other_half)
        part_q = jnp.where(core == 0, other_half, d_cur)
        p_y = lax.ppermute(part_p, BOTH, to_row)
        q_x = lax.ppermute(part_q, BOTH, in_row)
        p_row = jnp.where(at_home, part_p, p_y)
        q_row = jnp.concatenate(in_order(part_q, q_x), axis=0)
        p_x = pp_x(p_row)
        q_y = lax.ppermute(q_row, BOTH, to_row)
        q_both = jnp.where(at_home, q_row, q_y)
        p_0, p_1 = in_order(p_row, p_x)
        d_x = jnp.concatenate([p_0, q_both[:half_t], p_1, q_both[half_t:]], axis=0).reshape(2, -1, dim)

        ready = tuple(v for ab in total.values() for v in ab)
        cot_mine = cot_out.reshape(-1, dim)
        cot_other = pp_d(cot_mine)
        grad_2 = None
        for layer in reversed(range(layer_count)):
            g_all = after(g_mine[layer], *ready)
            if layer == layer_count - 1:
                rows = g_all.shape[0] // 2
                grad_2 = tn(take(g_all, core, 0, rows), cot_mine) + tn(take(g_all, 1 - core, 0, rows), cot_other)
            else:
                grad_2 = grad_2 + tn(g_all, next_all[layer])

        grad_2 = join(core, grad_2, pp_d(grad_2))
        own_1 = [v.reshape(-1, half_d) for v in (own_1a, own_1b)]
        grad_1 = join_flip(core, own_1, [pp_d(v) for v in own_1])
        gq, gk, gv, go = join_attn(core, (own_qk, own_vo), (pp_d(own_qk), pp_d(own_vo)))
        return gq, gk, gv, go, grad_1, grad_2, d_x

    return jax.shard_map(device_step, mesh=mesh,
                         in_specs=(spec_act, spec_act, spec_rep, spec_col, spec_col, spec_col, spec_row, spec_col, spec_row),
                         out_specs=(spec_col, spec_col, spec_col, spec_row, spec_col, spec_row, spec_act),
                         check_vma=False)
```

```python
import functools

import jax
import jax.numpy as jnp
from jax import lax
from jax.experimental import pallas as pl
from jax.experimental.pallas import tpu as pltpu
from jax.sharding import PartitionSpec as P


HEAD_DIM = 64
EPS_NORM = 1e-6
F32 = jnp.float32
BF16 = jnp.bfloat16
LOG2E = 1.4426950408889634
VMEM_ALL = 60 * 1024 * 1024
SCALE = HEAD_DIM ** -0.5

SWAP_D = [(0, 1), (1, 0)]


SWAP_X = [(0, 1), (1, 0), (2, 3), (3, 2)]
SWAP_Y = [(0, 2), (2, 0), (1, 3), (3, 1)]


def pp_x(v):
    return lax.ppermute(v, 'model', SWAP_X)


def pp_y(v):
    return lax.ppermute(v, 'model', SWAP_Y)


def pp_d(v):
    return lax.ppermute(v, 'data', SWAP_D)


def dot(a, b, dims):
    return lax.dot_general(a, b, (dims, ((), ())), preferred_element_type=F32)


def nn(a, b):
    return dot(a, b, ((1,), (0,)))


def nt(a, b):
    return dot(a, b, ((1,), (1,)))


def tn(a, b):
    return dot(a, b, ((0,), (0,)))


def pair_masks(rows):
    lane = lax.broadcasted_iota(jnp.int32, (rows, 128), 1)
    return lane < HEAD_DIM


CHUNK = 256
WIDE = 256


def masked_pair(q):
    low = pair_masks(CHUNK)
    zero = jnp.zeros_like(q)
    return jnp.concatenate([jnp.where(low, q, zero), jnp.where(low, zero, q)], axis=0)


def attn_fwd_body(*refs):
    u_ref, w0_ref, wn_ref, ko_ref, ks_ref, kno_ref, kns_ref, vo_ref, vs_ref = refs[:9]
    q_ref, ctx_ref, lse_ref, qs_ref, a_ref, ma_ref = refs[-6:]
    units = [(sub, i) for sub in range(WIDE // 128) for i in range(q_ref.shape[0] // CHUNK)]

    def joined(own_ref, sib_ref, sub):
        cols = slice(sub * 128, (sub + 1) * 128)
        return jnp.concatenate([own_ref[:, cols], sib_ref[:, cols]], axis=0)

    def scores(ko, ks, q, sub, i):
        s = nt(joined(ko, ks, sub), masked_pair(q[i * CHUNK:(i + 1) * CHUNK, sub * 128:(sub + 1) * 128]))
        return s, jnp.max(s, axis=0, keepdims=True)

    @pl.when(pl.program_id(0) == 0)
    def _():
        qs_ref[...] = nt(u_ref[0, 0], w0_ref[...]).astype(BF16)
        a_ref[...], ma_ref[...] = scores(ko_ref, ks_ref, qs_ref[...], 0, 0)

    q_ref[...] = qs_ref[...]
    s, m = a_ref[...], ma_ref[...]
    for n, (sub, i) in enumerate(units):
        if n + 1 < len(units):
            ahead = scores(ko_ref, ks_ref, q_ref[...], *units[n + 1])
        else:
            ahead = scores(kno_ref, kns_ref, q_next, 0, 0)
        if n == 0:
            q_next = nt(u_ref[0, 0], wn_ref[...]).astype(BF16)
        rows, cols = slice(i * CHUNK, (i + 1) * CHUNK), slice(sub * 128, (sub + 1) * 128)
        p = jnp.exp2((s - m) * (SCALE * LOG2E))
        l = jnp.sum(p, axis=0, keepdims=True)
        pb = (p * (1.0 / l)).astype(BF16)
        lse = m * (SCALE * LOG2E) + jnp.log2(l)
        lse_ref[sub, 0:1, rows] = lse[:, :CHUNK]
        lse_ref[sub, 1:2, rows] = lse[:, CHUNK:]
        ctx_t = tn(joined(vo_ref, vs_ref, sub), pb)
        ctx_t = jnp.concatenate([ctx_t[:HEAD_DIM, :CHUNK], ctx_t[HEAD_DIM:, CHUNK:]], axis=0)
        ctx_ref[0, 0, rows, cols] = ctx_t.T.astype(BF16)
        s, m = ahead
    qs_ref[...] = q_next
    a_ref[...], ma_ref[...] = s, m


def attn_fwd(um_hist, wq, kv, kv_s, layer, layers, hist):
    tk, width = kv.shape[0], kv.shape[1] // 2
    tq = um_hist.shape[2]
    pairs = width // 128
    steps = width // WIDE

    def col(off):
        return lambda j: (0, j + off)

    def nxt(j):
        return (0, jnp.minimum(j + 1, steps - 1))

    extra = [] if hist is None else [hist]
    flops = 2 * 2 * tq * (2 * tk) * 256 * (width // HEAD_DIM)
    return pl.pallas_call(
        attn_fwd_body,
        grid=(steps,),
        in_specs=[pl.BlockSpec((1, 1, tq, width), lambda j: (0, layer, 0, 0)),
                  pl.BlockSpec((WIDE, width), lambda j: (0, 0)),
                  pl.BlockSpec((WIDE, width), lambda j: (jnp.minimum(j + 1, steps - 1), 0)),
                  pl.BlockSpec((tk, WIDE), col(0)), pl.BlockSpec((tk, WIDE), col(0)),
                  pl.BlockSpec((tk, WIDE), nxt), pl.BlockSpec((tk, WIDE), nxt),
                  pl.BlockSpec((tk, WIDE), col(steps)), pl.BlockSpec((tk, WIDE), col(steps))]
        + [pl.BlockSpec(memory_space=pl.ANY)] * len(extra),
        out_specs=[pl.BlockSpec((tq, WIDE), col(0)),
                   pl.BlockSpec((1, 1, tq, WIDE), lambda j: (3, layer, 0, j)),
                   pl.BlockSpec((WIDE // 128, 2, tq), lambda j: (j, 0, 0))],
        out_shape=[jax.ShapeDtypeStruct((tq, width), BF16),
                   jax.ShapeDtypeStruct((4, layers, tq, width), BF16),
                   jax.ShapeDtypeStruct((pairs, 2, tq), F32)],
        input_output_aliases={9: 1} if extra else {},
        scratch_shapes=[pltpu.VMEM((tq, WIDE), BF16), pltpu.VMEM((2 * tk, 2 * CHUNK), F32), pltpu.VMEM((1, 2 * CHUNK), F32)],
        compiler_params=pltpu.CompilerParams(dimension_semantics=('arbitrary',),
                                             vmem_limit_bytes=VMEM_ALL),
        cost_estimate=pl.CostEstimate(flops=flops, bytes_accessed=2 * (tq * width * 2 + 4 * tk * width),
                                      transcendentals=tq * 2 * tk * (width // HEAD_DIM)),
        name='attn_fwd',
    )(um_hist, wq, wq, kv, kv_s, kv, kv_s, kv, kv_s, *extra)


def attn_bwd_body(q_ref, ko_ref, ks_ref, vo_ref, vs_ref, do_ref, lse_ref, hist_ref, dq_ref, down_ref, dsib_ref):
    tk = ko_ref.shape[0]
    low = pair_masks(CHUNK)
    units = [(sub, i, h) for sub in range(WIDE // 128) for i in range(q_ref.shape[0] // CHUNK) for h in range(2)]

    def keys(own_ref, sib_ref, sub):
        cols = slice(sub * 128, (sub + 1) * 128)
        return jnp.concatenate([own_ref[:, cols], sib_ref[:, cols]], axis=0)

    def masked(ref, sub, i, h):
        v = ref[i * CHUNK:(i + 1) * CHUNK, sub * 128:(sub + 1) * 128]
        return jnp.where(low if h == 0 else ~low, v, jnp.zeros_like(v))

    def products(sub, i, h):
        s = nt(keys(ko_ref, ks_ref, sub), masked(q_ref, sub, i, h))
        return s, nt(keys(vo_ref, vs_ref, sub), masked(do_ref, sub, i, h)).astype(BF16)

    dqs = []
    ahead = products(*units[0])
    for n, (sub, i, h) in enumerate(units):
        s, dp = ahead
        if n + 1 < len(units):
            ahead = products(*units[n + 1])
        rows, cols = slice(i * CHUNK, (i + 1) * CHUNK), slice(sub * 128, (sub + 1) * 128)
        p = jnp.exp2(s * (SCALE * LOG2E) - lse_ref[sub, h:h + 1, rows])
        dp = dp.astype(F32)
        delta = jnp.sum(p * dp, axis=0, keepdims=True)
        ds = (p * (dp - delta)).astype(BF16)
        dv = nn(p.astype(BF16), masked(do_ref, sub, i, h))
        dk = nn(ds, masked(q_ref, sub, i, h) * jnp.asarray(SCALE, BF16))
        for m, grad in enumerate((dk, dv)):
            for ref, part in ((down_ref, grad[:tk]), (dsib_ref, grad[tk:])):
                if i == 0 and h == 0:
                    ref[m, :, cols] = part
                else:
                    ref[m, :, cols] += part
        dqs.append(tn(keys(ko_ref, ks_ref, sub), ds)[h * HEAD_DIM:(h + 1) * HEAD_DIM, :] * SCALE)
        if h == 1:
            dq_ref[0, 0, rows, cols] = jnp.concatenate(dqs, axis=0).T.astype(BF16)
            dqs = []


def attn_bwd(q, kv, kv_s, d_ctx, lse, layer, layers, hist):
    tq, width = q.shape
    tk = kv.shape[0]
    steps = width // WIDE

    def col(off):
        return lambda j: (0, j + off)

    flops = 5 * 2 * tq * (2 * tk) * 256 * (width // HEAD_DIM)
    qblk = pl.BlockSpec((tq, WIDE), col(0))
    kblk = pl.BlockSpec((tk, WIDE), col(0))
    vblk = pl.BlockSpec((tk, WIDE), col(steps))
    both = pl.BlockSpec((2, tk, WIDE), lambda j: (0, 0, j))
    return pl.pallas_call(
        attn_bwd_body,
        grid=(steps,),
        in_specs=[qblk, kblk, kblk, vblk, vblk, qblk,
                  pl.BlockSpec((WIDE // 128, 2, tq), lambda j: (j, 0, 0)), pl.BlockSpec(memory_space=pl.ANY)],
        out_specs=[pl.BlockSpec((1, 1, tq, WIDE), lambda j: (0, layer, 0, j)), both, both],
        out_shape=[jax.ShapeDtypeStruct((4, layers, tq, width), BF16)]
        + [jax.ShapeDtypeStruct((2, tk, width), F32)] * 2,
        input_output_aliases={7: 0},
        compiler_params=pltpu.CompilerParams(dimension_semantics=('arbitrary',),
                                             vmem_limit_bytes=VMEM_ALL),
        cost_estimate=pl.CostEstimate(flops=flops, bytes_accessed=2 * (2 * tq * width * 2 + 4 * tk * width) + 16 * tk * width,
                                      transcendentals=tq * 2 * tk * (width // HEAD_DIM)),
        name='attn_bwd',
    )(q, kv, kv_s, kv, kv_s, d_ctx, lse, hist)


def kv_body(*refs):
    x_ref, e_ref, w_ref = refs[:3]
    kv_ref, u_ref = refs[-2:]

    @pl.when(pl.program_id(0) == 0)
    def _():
        s = x_ref[...].astype(F32) + e_ref[...]
        u_ref[0, 0] = (s * lax.rsqrt(jnp.mean(s * s, axis=-1, keepdims=True) + EPS_NORM)).astype(BF16)

    for rows in ROWS:
        kv_ref[rows, :] = nt(u_ref[0, 0, rows, :], w_ref[...]).astype(BF16)


def norm_kv(x, e, wkv, layer, layers, hist):
    t, dim = x.shape
    width = wkv.shape[0]
    blk = 1024
    extra = [] if hist is None else [hist]
    return pl.pallas_call(
        kv_body,
        grid=(width // blk,),
        in_specs=[pl.BlockSpec((t, dim), lambda j: (0, 0)), pl.BlockSpec((1, dim), lambda j: (0, 0)),
                  pl.BlockSpec((blk, dim), lambda j: (j, 0))] + [pl.BlockSpec(memory_space=pl.ANY)] * len(extra),
        out_specs=[pl.BlockSpec((t, blk), lambda j: (0, j)), pl.BlockSpec((1, 1, t, dim), lambda j: (0, layer, 0, 0))],
        out_shape=[jax.ShapeDtypeStruct((t, width), BF16), jax.ShapeDtypeStruct((2, layers, t, dim), BF16)],
        input_output_aliases={3: 1} if extra else {},
        compiler_params=pltpu.CompilerParams(dimension_semantics=('arbitrary',), vmem_limit_bytes=VMEM_ALL),
        cost_estimate=pl.CostEstimate(flops=2 * t * dim * width, bytes_accessed=2 * (dim * width + t * width + 2 * t * dim),
                                      transcendentals=t),
        name='norm_kv',
    )(x, e, wkv, *extra)


def d_kv_body(layer, acc0_hbm, x_hbm, e_ref, um_hbm, own_ref, recv_ref, w_ref, hist_ref, dkv_ref, prev_ref,
              acc_ref, acc0_ref, x_ref, mid_ref, sems):
    j = pl.program_id(0)
    late = [pltpu.make_async_copy(src, dst, sems.at[n])
            for n, (src, dst) in enumerate(((acc0_hbm, acc0_ref), (x_hbm, x_ref), (um_hbm.at[1, layer], mid_ref)))]

    @pl.when(j == 0)
    def _():
        for copy in late:
            copy.start()
        acc_ref[...] = jnp.zeros_like(acc_ref)

    dkv_ref[0, 0] = (own_ref[0] + recv_ref[0]).astype(BF16)
    for rows in ROWS:
        acc_ref[rows, :] += nn(dkv_ref[0, 0, rows, :], w_ref[...])

    @pl.when(j == pl.num_programs(0) - 1)
    def _():
        for copy in late:
            copy.wait()
        dn = (acc_ref[...] + acc0_ref[...]).astype(BF16).astype(F32)
        s = x_ref[...].astype(F32) + e_ref[...]
        inv = lax.rsqrt(jnp.mean(s * s, axis=-1, keepdims=True) + EPS_NORM)
        proj = jnp.mean(s * dn, axis=-1, keepdims=True)
        prev_ref[...] = (mid_ref[...].astype(F32) + inv * dn - s * (inv * inv * inv * proj)).astype(BF16)


def d_kv(acc0, x, e, um_hist, own, recv, wkv, layer, layers, hist):
    t, dim = x.shape
    half = dim // 2
    hbm = pl.BlockSpec(memory_space=pl.ANY)
    gblk = pl.BlockSpec((1, t, half), lambda j: (j // 2, 0, j % 2))
    return pl.pallas_call(
        functools.partial(d_kv_body, layer),
        grid=(4,),
        in_specs=[hbm, hbm, pl.BlockSpec((1, dim), lambda j: (0, 0)), hbm, gblk, gblk,
                  pl.BlockSpec((half, dim), lambda j: (j, 0)), hbm],
        out_specs=[pl.BlockSpec((1, 1, t, half), lambda j: (1 + j // 2, layer, 0, j % 2)),
                   pl.BlockSpec((t, dim), lambda j: (0, 0))],
        out_shape=[jax.ShapeDtypeStruct((4, layers, t, dim), BF16), jax.ShapeDtypeStruct((t, dim), BF16)],
        scratch_shapes=[pltpu.VMEM((t, dim), F32), pltpu.VMEM((t, dim), F32), pltpu.VMEM((t, dim), BF16),
                        pltpu.VMEM((t, dim), BF16), pltpu.SemaphoreType.DMA((3,))],
        input_output_aliases={7: 0},
        compiler_params=pltpu.CompilerParams(dimension_semantics=('arbitrary',), vmem_limit_bytes=VMEM_ALL),
        cost_estimate=pl.CostEstimate(flops=4 * t * dim * dim, bytes_accessed=4 * dim * dim + 20 * t * dim, transcendentals=t),
        name='d_kv',
    )(acc0, x, e, um_hist, own, recv, wkv, hist)


def terms_body(added, slot_of, places_ref, lhs_ref, rhs_ref, *refs):
    count = len(refs) // (1 + added)
    recv, outs = refs[:count * added], refs[-count:]
    step = pl.program_id(0)
    val = tn(lhs_ref[0], rhs_ref[0])
    for slot in range(count):
        @pl.when(slot_of(step) == slot)
        def _():
            outs[slot][0] = val + recv[slot][0] if added else val


def terms(lhs, rhs, rows, cols, places, plans, chips, recv):
    tokens = lhs.shape[1]
    lhs_at, rhs_at, slot_of, turns = plans[len(chips) - 1]

    def rel(r):
        return chips[0] + r * (chips[-1] - chips[0])

    slots = [pl.BlockSpec((1, rows, cols), lambda i, p, at=at: (jnp.clip(i - at, 0, 1), 0, 0)) for at in turns]
    out = pl.pallas_call(
        functools.partial(terms_body, int(bool(recv)), slot_of),
        grid_spec=pltpu.PrefetchScalarGridSpec(
            num_scalar_prefetch=1, grid=(4 * len(chips),),
            in_specs=[pl.BlockSpec((1, tokens, rows), lambda i, p: lhs_at(i, rel, p)),
                      pl.BlockSpec((1, tokens, cols), lambda i, p: rhs_at(i, p))] + slots[:len(recv)],
            out_specs=slots),
        out_shape=[jax.ShapeDtypeStruct((2, rows, cols), F32)] * len(turns),
        compiler_params=pltpu.CompilerParams(dimension_semantics=('arbitrary',), vmem_limit_bytes=VMEM_ALL),
        cost_estimate=pl.CostEstimate(flops=8 * len(chips) * tokens * rows * cols, bytes_accessed=24 * tokens * rows,
                                      transcendentals=0),
    )(places, lhs, rhs, *recv)
    return {chip: out[2 * n:2 * n + 2] for n, chip in enumerate(chips)}


ATTN_PLANS = (
    (lambda i, rel, p: (i, 0, rel(0)), lambda i, p: (i // 3, 0, p[0]), lambda i: i // 2, (0, 2)),
    (lambda i, rel, p: (jnp.where(i < 4, i % 2, i // 2), 0, rel(jnp.where(i < 4, i // 2, i % 2))),
     lambda i, p: (i // 6, 0, p[0]), lambda i: jnp.where(i < 4, 2 * (i // 2), 2 * (i % 2) + 1), (0, 5, 2, 6)))
UP_PLANS = (
    (lambda i, rel, p: (0, 0, 4 * p[1 + rel(0)] + 2 * p[0] + i % 2), lambda i, p: (0, 0, i // 2), lambda i: i // 2, (0, 2)),
    (lambda i, rel, p: (0, 0, 4 * p[1 + rel((i // 2) % 2)] + 2 * p[0] + i % 2),
     lambda i, p: (0, 0, i // 4), lambda i: 2 * ((i // 2) % 2) + i // 4, (0, 4, 2, 6)))


def summed_terms(operands, places, plans, groups, done=()):
    def in_turn(where):
        return lax.optimization_barrier((where, done))[0] if done else where

    sent, total = {}, {}
    for group in groups:
        out = terms(*operands, in_turn(places[1]), plans, group, [])
        done = [v for ab in out.values() for v in ab]
        sent.update({r: [pp_d(v) for v in ab] for r, ab in out.items()})
    for group in groups:
        out = terms(*operands, in_turn(places[0]), plans, group, [v for r in group for v in sent[r]])
        done = [v for ab in out.values() for v in ab]
        total.update(out)
    return total


GELU_C = 0.7978845608028654
GELU_A = 0.044715
BLOCK_F = 768
ROWS = (slice(0, 256), slice(256, 512))


def mlp_fwd_body(*refs):
    x0_ref, e_ref, ctx_ref, wo_ref, w1_hbm, w2_hbm = refs[:6]
    z_ref, g_ref, x_ref, h_ref, m_ref, acc_ref, w1_ref, w2_ref, sems = refs[-9:]
    j = pl.program_id(0)
    last = pl.num_programs(0) - 1

    def fetch(step):
        rows = pl.ds(pl.multiple_of(step * BLOCK_F, BLOCK_F), BLOCK_F)
        slot = step % 2
        return [pltpu.make_async_copy(hbm.at[rows], ref.at[slot], sems.at[n, slot])
                for n, (hbm, ref) in enumerate(((w1_hbm, w1_ref), (w2_hbm, w2_ref)))]

    @pl.when(j == 0)
    def _():
        for copy in fetch(0):
            copy.start()
        for rows in ROWS:
            s = x0_ref[rows, :].astype(F32) + e_ref[...]
            h = (s + nn(ctx_ref[0, 0, rows, :], wo_ref[...])).astype(BF16)
            h_ref[rows, :] = h
            hf = h.astype(F32)
            acc_ref[rows, :] = hf
            m_ref[0, rows, :] = (hf * lax.rsqrt(jnp.mean(hf * hf, axis=-1, keepdims=True) + EPS_NORM)).astype(BF16)

    @pl.when(j < last)
    def _():
        for copy in fetch(j + 1):
            copy.start()

    for copy in fetch(j):
        copy.wait()
    slot = j % 2
    for rows in ROWS:
        z = nt(m_ref[0, rows, :], w1_ref[slot]).astype(BF16)
        z_ref[rows, :] = z
        zf = z.astype(F32)
        t = jnp.tanh(zf * (GELU_C + (GELU_A * GELU_C) * (zf * zf)))
        half = 0.5 * zf
        g_ref[0, rows, :] = (half + half * t).astype(BF16)
    for rows in ROWS:
        acc_ref[rows, :] += nn(g_ref[0, rows, :], w2_ref[slot])

    @pl.when(j == last)
    def _():
        x_ref[...] = acc_ref[...].astype(BF16)


def mlp_fwd(x, e, ctx_hist, wo, w1t, w2, layer, layers, hist):
    t, dim = x.shape
    hidden = w2.shape[0]
    whole = pl.BlockSpec((t, dim), lambda j: (0, 0))
    slab = pl.BlockSpec((1, t, dim), lambda j: (layer, 0, 0))
    hbm = pl.BlockSpec(memory_space=pl.ANY)
    extra = [] if hist is None else [hist]
    return pl.pallas_call(
        mlp_fwd_body,
        grid=(hidden // BLOCK_F,),
        in_specs=[whole, pl.BlockSpec((1, dim), lambda j: (0, 0)), pl.BlockSpec((1, 1, t, dim), lambda j: (3, layer, 0, 0)),
                  pl.BlockSpec((dim, dim), lambda j: (0, 0)), hbm, hbm] + [hbm] * len(extra),
        out_specs=[pl.BlockSpec((t, BLOCK_F), lambda j: (0, j)),
                   pl.BlockSpec((1, t, BLOCK_F), lambda j: (j, 0, 0)), whole, whole, slab],
        out_shape=[jax.ShapeDtypeStruct((t, hidden), BF16),
                   jax.ShapeDtypeStruct((hidden // BLOCK_F, t, BLOCK_F), BF16),
                   jax.ShapeDtypeStruct((t, dim), BF16), jax.ShapeDtypeStruct((t, dim), BF16),
                   jax.ShapeDtypeStruct((layers, t, dim), BF16)],
        scratch_shapes=[pltpu.VMEM((t, dim), F32), pltpu.VMEM((2, BLOCK_F, dim), BF16), pltpu.VMEM((2, BLOCK_F, dim), BF16),
                        pltpu.SemaphoreType.DMA((2, 2))],
        input_output_aliases={6: 4} if extra else {},
        compiler_params=pltpu.CompilerParams(dimension_semantics=('arbitrary',), vmem_limit_bytes=VMEM_ALL),
        cost_estimate=pl.CostEstimate(flops=4 * t * dim * hidden, bytes_accessed=4 * dim * hidden + 4 * t * hidden,
                                      transcendentals=t * hidden),
        name='mlp_fwd',
    )(x, e, ctx_hist, wo, w1t, w2, *extra)


BLOCK_B = 1024
SUB_B = 512


def mlp_bwd_body(*refs):
    d_ref, h_hbm, z_ref, wo_hbm, w1_ref, w2_ref = refs[:6]
    up_ref, mid_ref, dctx_ref, acc_ref, h_ref, wo_ref, sems = refs[-7:]
    j = pl.program_id(0)
    late = [pltpu.make_async_copy(h_hbm, h_ref, sems.at[0]), pltpu.make_async_copy(wo_hbm, wo_ref, sems.at[1])]

    @pl.when(j == 0)
    def _():
        for copy in late:
            copy.start()
        acc_ref[...] = jnp.zeros_like(acc_ref)

    for i in range(0, BLOCK_B, SUB_B):
        cols = slice(i, i + SUB_B)
        for rows in ROWS:
            da = nt(d_ref[rows, :], w2_ref[cols, :]).astype(BF16).astype(F32)
            zf = z_ref[rows, cols].astype(F32)
            z2 = zf * zf
            t = jnp.tanh(zf * (GELU_C + (GELU_A * GELU_C) * z2))
            slope = (1.0 + t) * (0.5 + (1.0 - t) * (zf * (0.5 * GELU_C + (1.5 * GELU_A * GELU_C) * z2)))
            up_ref[0, rows, cols] = (da * slope).astype(BF16)
    for rows in ROWS:
        acc_ref[rows, :] += nn(up_ref[0, rows, :], w1_ref[...])

    @pl.when(j == pl.num_programs(0) - 1)
    def _():
        for copy in late:
            copy.wait()
        for rows in ROWS:
            dn = acc_ref[rows, :].astype(BF16).astype(F32)
            hf = h_ref[rows, :].astype(F32)
            inv = lax.rsqrt(jnp.mean(hf * hf, axis=-1, keepdims=True) + EPS_NORM)
            proj = jnp.mean(hf * dn, axis=-1, keepdims=True)
            mid = (d_ref[rows, :].astype(F32) + inv * dn - hf * (inv * inv * inv * proj)).astype(BF16)
            mid_ref[0, 0, rows, :] = mid
            dctx_ref[rows, :] = nt(mid, wo_ref[...]).astype(BF16)


def mlp_bwd(d_next, h, z, wo, w1t, w2, layer, layers, um_hist, hist):
    t, dim = h.shape
    hidden = w2.shape[0]
    whole = pl.BlockSpec((t, dim), lambda j: (0, 0))
    hbm = pl.BlockSpec(memory_space=pl.ANY)
    wblk = pl.BlockSpec((BLOCK_B, dim), lambda j: (j, 0))
    extra = [um_hist] if hist is None else [um_hist, hist]
    return pl.pallas_call(
        mlp_bwd_body,
        grid=(hidden // BLOCK_B,),
        in_specs=[whole, hbm, pl.BlockSpec((t, BLOCK_B), lambda j: (0, j)), hbm, wblk, wblk]
        + [pl.BlockSpec(memory_space=pl.ANY)] * len(extra),
        out_specs=[pl.BlockSpec((1, t, BLOCK_B), lambda j: (layer, 0, j)), pl.BlockSpec((1, 1, t, dim), lambda j: (1, layer, 0, 0)), whole],
        out_shape=[jax.ShapeDtypeStruct((layers, t, hidden), BF16), jax.ShapeDtypeStruct((2, layers, t, dim), BF16),
                   jax.ShapeDtypeStruct((t, dim), BF16)],
        scratch_shapes=[pltpu.VMEM((t, dim), F32), pltpu.VMEM((t, dim), BF16), pltpu.VMEM((dim, dim), BF16),
                        pltpu.SemaphoreType.DMA((2,))],
        input_output_aliases={6: 1} if hist is None else {6: 1, 7: 0},
        compiler_params=pltpu.CompilerParams(dimension_semantics=('arbitrary',), vmem_limit_bytes=VMEM_ALL),
        cost_estimate=pl.CostEstimate(flops=4 * t * dim * hidden, bytes_accessed=4 * dim * hidden + 4 * t * hidden,
                                      transcendentals=t * hidden),
        name='mlp_bwd',
    )(d_next, h, z, wo, w1t, w2, *extra)


def spread_body(chips_ref, src_ref, q_ref, kv_ref):
    @pl.when(pl.program_id(0) < 4)
    def _():
        q_ref[...] = src_ref[...]

    @pl.when(pl.program_id(0) >= 4)
    def _():
        kv_ref[...] = src_ref[...]


def spread(chips, qkv):
    rows, dim = qkv.shape[0] // 12, qkv.shape[1]
    return pl.pallas_call(
        spread_body,
        grid_spec=pltpu.PrefetchScalarGridSpec(
            num_scalar_prefetch=1, grid=(12,),
            in_specs=[pl.BlockSpec((rows, dim), lambda i, c: (3 * c[i % 4] + i // 4, 0))],
            out_specs=[pl.BlockSpec((rows, dim), lambda i, c: (jnp.minimum(i, 3), 0)),
                       pl.BlockSpec((rows, dim), lambda i, c: (jnp.maximum(i - 4, 0), 0))]),
        out_shape=[jax.ShapeDtypeStruct((4 * rows, dim), BF16), jax.ShapeDtypeStruct((8 * rows, dim), BF16)],
        compiler_params=pltpu.CompilerParams(dimension_semantics=('arbitrary',), vmem_limit_bytes=VMEM_ALL),
        cost_estimate=pl.CostEstimate(flops=qkv.size, bytes_accessed=4 * qkv.size, transcendentals=0),
        name='spread',
    )(chips, qkv)


def join_body(count, core_ref, *refs):
    for n in range(count):
        own, other, out = refs[n], refs[count + n], refs[2 * count + n]
        for i, src in enumerate((own, other)):
            @pl.when(pl.program_id(0) == i)
            def _():
                out[...] = src[...]


def join_call(core, body, grid, own, other, in_specs, out_specs, out_shape):
    size = sum(v.size for v in own)
    return pl.pallas_call(
        body,
        grid_spec=pltpu.PrefetchScalarGridSpec(num_scalar_prefetch=1, grid=grid, in_specs=in_specs, out_specs=out_specs),
        out_shape=out_shape,
        compiler_params=pltpu.CompilerParams(dimension_semantics=('arbitrary', 'arbitrary'), vmem_limit_bytes=VMEM_ALL),
        cost_estimate=pl.CostEstimate(flops=8 * size, bytes_accessed=16 * size, transcendentals=0),
    )(core.reshape(1), *own, *other)


def join(core, own, other):
    rows, cols = own.shape[0] // 4, own.shape[1]
    first = pl.BlockSpec((rows, cols), lambda i, j, c: (jnp.where(i == 0, j, 3), 0))
    then = pl.BlockSpec((rows, cols), lambda i, j, c: (jnp.where(i == 0, 0, j), 0))
    return join_call(core, functools.partial(join_body, 1), (2, 4), [own], [other], [first, then],
                     pl.BlockSpec((rows, cols), lambda i, j, c: (4 * ((c[0] + i) % 2) + j, 0)),
                     jax.ShapeDtypeStruct((8 * rows, cols), F32))


def join_attn_body(core_ref, own_a, own_b, sib_a, sib_b, q_ref, k_ref, v_ref, o_ref):
    for i, (a_ref, b_ref) in enumerate(((own_a, own_b), (sib_a, sib_b))):
        @pl.when(pl.program_id(0) == i)
        def _():
            q_ref[...] = a_ref[0].T
            k_ref[...] = a_ref[1].T
            v_ref[...] = b_ref[0].T
            o_ref[...] = b_ref[1]


def join_attn(core, own, other):
    _, hid, half_d = own[0].shape
    block = pl.BlockSpec((2, hid, half_d), lambda i, j, c: (0, 0, 0))
    tall = pl.BlockSpec((half_d, hid), lambda i, j, c: ((c[0] + i) % 2, 0))
    wide = pl.BlockSpec((hid, half_d), lambda i, j, c: (0, (c[0] + i) % 2))
    return join_call(core, join_attn_body, (2, 1), list(own), list(other), [block] * 4, [tall] * 3 + [wide],
                     [jax.ShapeDtypeStruct((2 * half_d, hid), F32)] * 3 + [jax.ShapeDtypeStruct((hid, 2 * half_d), F32)])


def join_flip_body(core_ref, oa_ref, ob_ref, sa_ref, sb_ref, out_ref):
    for i, srcs in enumerate(((oa_ref, ob_ref), (sa_ref, sb_ref))):
        for j, src in enumerate(srcs):
            @pl.when((pl.program_id(0) == i) & (pl.program_id(1) == j))
            def _():
                out_ref[...] = src[...].T


def join_flip(core, own, other):
    rows, cols = own[0].shape
    block = pl.BlockSpec((rows, cols), lambda i, j, c: (0, 0))
    return join_call(core, join_flip_body, (2, 2), own, other, [block] * 4,
                     pl.BlockSpec((cols, rows), lambda i, j, c: (j, (c[0] + i) % 2)),
                     jax.ShapeDtypeStruct((2 * cols, 2 * rows), F32))


def gather_pieces(part_a, part_b):
    xa, xb = pp_x(part_a), pp_x(part_b)
    ya, yb = pp_y(part_a), pp_y(part_b)
    da, db = pp_y(xa), pp_x(yb)
    own = [(xa, xb), (ya, yb), (da, db)]
    return own, [(pp_d(a), pp_d(b)) for a, b in own]


def reduce_terms(total, pp_first, pp_second, first, second):
    here, there = pp_first(total[first]), pp_first(total[3])
    last = pp_second(total[second] + there)
    return total[0] + here + last


BOTH = ('model', 'data')


def solution(mesh):
    spec_col = P(None, 'model')
    spec_row = P('model', None)
    spec_act = P('data', None, None)
    spec_rep = P(None, None)

    def device_step(x_in, cot_out, step_emb, w_q, w_k, w_v, w_o, w_1, w_2):
        layer_count, dim = step_emb.shape
        core = lax.axis_index('data')
        chip = lax.axis_index('model')
        chip_x = lax.rem(chip, 2)
        chip_y = lax.div(chip, 2)
        nbr_x = chip + 1 - 2 * chip_x
        nbr_y = lax.rem(chip + 2, 4)
        diag = lax.rem(nbr_x + 2, 4)
        chips = (chip, nbr_x, nbr_y, diag)
        hid = w_q.shape[1]
        half_d = dim // 2
        half_t = x_in.shape[1] // 2

        def take(v, which, axis, size):
            return lax.dynamic_slice_in_dim(v, which * size, size, axis)

        def put(buf, v, which, axis):
            return lax.dynamic_update_slice_in_dim(buf, v, which * v.shape[axis], axis)

        def gather(v):
            return lax.all_gather(v, BOTH, axis=0, tiled=True)

        def after(v, *deps):
            return lax.optimization_barrier((v,) + deps)[0]

        def my_tokens(v):
            mine = lax.dynamic_index_in_dim(v, chip_x, 0, keepdims=False)
            half = mine.shape[0] // 2
            recv = pp_d(take(mine, 1 - core, 0, half))
            return jnp.where(core == chip_y, take(mine, core, 0, half), recv)

        def gather_permuted(local):
            own = take(local, core, 0, local.shape[0] // 2)
            rows = own.shape[0] // 2
            p_own, p_sib = gather_pieces(own[:rows], own[rows:])
            full = put(jnp.zeros((4 * local.shape[0], dim), BF16), local, chip, 0)
            for r in (1, 2, 3):
                for part in (0, 1):
                    full = put(full, p_own[r - 1][part], 4 * chips[r] + 2 * core + part, 0)
                    full = put(full, p_sib[r - 1][part], 4 * chips[r] + 2 * (1 - core) + part, 0)
            return full

        x_cur = my_tokens(x_in)
        qkv_t = jnp.concatenate([w_q, w_k, w_v], axis=1).T
        qkv_all = gather(take(qkv_t, core, 0, qkv_t.shape[0] // 2))
        o_all = gather(take(w_o, core, 0, hid // 2))
        w2 = gather_permuted(w_2)
        w1 = gather_permuted(w_1.T)
        wq, wkv = spread(jnp.stack(chips).astype(jnp.int32), qkv_all)
        wo = jnp.concatenate([take(o_all, c, 0, hid) for c in chips], axis=0)
        d_cur = my_tokens(cot_out)
        emb = step_emb.astype(F32)

        saved = []
        g_mine = []
        um_hist = m_hist = att_hist = None
        for layer in range(layer_count):
            e = emb[layer:layer + 1]
            kv, um_hist = norm_kv(x_cur, e, wkv, layer, layer_count, um_hist)
            kv_s = pp_d(kv)
            q, att_hist, lse = attn_fwd(um_hist, wq, kv, kv_s, layer, layer_count, att_hist)
            z, g, x_next, h, m_hist = mlp_fwd(x_cur, e, att_hist, wo, w1, w2, layer, layer_count, m_hist)
            g_mine.append(lax.all_to_all(g.reshape(-1, g.shape[-1]), BOTH, split_axis=0, concat_axis=0, tiled=True))
            saved.append((x_cur, q, kv, kv_s, lse, h, z))
            x_cur = x_next

        def flat(v, lead):
            return v.reshape(lead, -1, v.shape[-1])

        places = [jnp.stack([w, *chips]).astype(jnp.int32) for w in (core, 1 - core)]
        up_hist = None
        next_all = [None] * layer_count
        for layer in reversed(range(layer_count)):
            x_l, q, kv, kv_s, lse, h, z = saved[layer]
            e = emb[layer:layer + 1]
            d_next = d_cur
            if layer < layer_count - 1:
                next_all[layer] = gather(d_next)
            up_hist, um_hist, d_ctx = mlp_bwd(d_next, h, z, wo, w1, w2, layer, layer_count, um_hist, up_hist)
            if layer == 0:
                up_operands = (flat(up_hist, 1), flat(m_hist, 1), hid, half_d)
                up_total = summed_terms(up_operands, places, UP_PLANS, ((3, 1), (2,)))
                d_ctx = after(d_ctx, *[v for ab in up_total.values() for v in ab])
            att_hist, own_kv, sib_kv = attn_bwd(q, kv, kv_s, d_ctx, lse, layer, layer_count, att_hist)
            recv_kv = pp_d(sib_kv)
            acc0 = nn(att_hist[0, layer], wq)
            att_hist, d_cur = d_kv(acc0, x_l, e, um_hist, own_kv, recv_kv, wkv, layer, layer_count, att_hist)

        att_operands = (flat(att_hist, 4), flat(um_hist, 2), hid, half_d)
        att_total = summed_terms(att_operands, places, ATTN_PLANS, ((3, 1), (2,)))
        ready = [v for ab in att_total.values() for v in ab]
        att_total.update(summed_terms(att_operands, places, ATTN_PLANS, ((0,),), ready))
        up_total.update(summed_terms(up_operands, places, UP_PLANS, ((0,),), ready))

        def part(total, n):
            return {r: ab[n] for r, ab in total.items()}

        own_1a = reduce_terms(part(up_total, 0), pp_x, pp_y, 1, 2)
        own_1b = reduce_terms(part(up_total, 1), pp_y, pp_x, 2, 1)
        own_qk = reduce_terms(part(att_total, 0), pp_x, pp_y, 1, 2)
        own_vo = reduce_terms(part(att_total, 1), pp_y, pp_x, 2, 1)

        at_home = chip_y == core
        to_row = [(2 * c + d, 2 * (c ^ 2) + d) for c in range(4) for d in range(2) if c // 2 == d]
        in_row = [(2 * c + d, 2 * (c ^ 1) + d) for c in range(4) for d in range(2) if c // 2 == d]

        def in_order(mine, other):
            return jnp.where(chip_x == 0, mine, other), jnp.where(chip_x == 0, other, mine)

        other_half = pp_d(d_cur)
        part_p = jnp.where(core == 0, d_cur, other_half)
        part_q = jnp.where(core == 0, other_half, d_cur)
        p_y = lax.ppermute(part_p, BOTH, to_row)
        q_x = lax.ppermute(part_q, BOTH, in_row)
        p_row = jnp.where(at_home, part_p, p_y)
        q_row = jnp.concatenate(in_order(part_q, q_x), axis=0)
        p_x = pp_x(p_row)
        q_y = lax.ppermute(q_row, BOTH, to_row)
        q_both = jnp.where(at_home, q_row, q_y)
        p_0, p_1 = in_order(p_row, p_x)
        d_x = jnp.concatenate([p_0, q_both[:half_t], p_1, q_both[half_t:]], axis=0).reshape(2, -1, dim)

        cot_mine = cot_out.reshape(-1, dim)
        cot_other = pp_d(cot_mine)
        grad_2 = None
        for layer in reversed(range(layer_count)):
            g_all = after(g_mine[layer], *ready)
            if layer == layer_count - 1:
                rows = g_all.shape[0] // 2
                grad_2 = tn(take(g_all, core, 0, rows), cot_mine) + tn(take(g_all, 1 - core, 0, rows), cot_other)
            else:
                grad_2 = grad_2 + tn(g_all, next_all[layer])

        grad_2 = join(core, grad_2, pp_d(grad_2))
        own_1 = [v.reshape(-1, half_d) for v in (own_1a, own_1b)]
        grad_1 = join_flip(core, own_1, [pp_d(v) for v in own_1])
        gq, gk, gv, go = join_attn(core, (own_qk, own_vo), (pp_d(own_qk), pp_d(own_vo)))
        return gq, gk, gv, go, grad_1, grad_2, d_x

    return jax.shard_map(device_step, mesh=mesh,
                         in_specs=(spec_act, spec_act, spec_rep, spec_col, spec_col, spec_col, spec_row, spec_col, spec_row),
                         out_specs=(spec_col, spec_col, spec_col, spec_row, spec_col, spec_row, spec_act),
                         check_vma=False)
```
